32 devices in a mesh: groups: 2 (over y), space: 4 (over z), rhs: 4 (over x, core).
Axes of the slice: x: 2, y: 2, z: 4, core: 2. Of those that a mesh axis runs over, the one named last changes fastest.
Arguments:
- conductance: float32 [64, 1024], P(('groups', 'space')), parts along dimension 0, may hold values from 0.05 to 2
- nodata: int32 [64, 1024], P(('groups', 'space')), parts along dimension 0, may hold values 0 or 1
- ground_mask: int32 [64, 1024], P(('groups', 'space')), parts along dimension 0, may hold values 0 or 1
- ground_value: float32 [64, 1024], P(('groups', 'space')), parts along dimension 0, may hold values from 0.5 to 4
- source_mask: int32 [64, 1024], P(('groups', 'space')), parts along dimension 0, may hold values 0 or 1
- source_current: float32 [64, 1024], P(('groups', 'space')), parts along dimension 0, may hold values from 0.5 to 4
- tile_inverse: float32 [64, 8, 128, 128], P(('groups', 'space')), parts along dimension 0, may hold values from -0.04 to 8, as said below
- focal_cells: int32 [512, 2], P(('groups', 'rhs')), parts along dimension 0, may hold values from 0 to 32767
Outputs:
- solution: float32 [256, 64, 1024], P('rhs', ('groups', 'space')), parts along dimension 1
- residual: float32 [256, 64, 1024], P('rhs', ('groups', 'space')), parts along dimension 1
The draws below stay inside these ranges and needn't reach their ends.
There are 2 independent parts, one for each index of `groups`. The reference program is written for one: setup_inputs(seed, part) draws one part's arguments, and reference() takes and returns one part's arrays. A program takes and returns all parts, laid end to end along the dimension named above; each array names one. Nothing has to cross between parts.
Inputs may be any that keep to these rules, and one draw needn't show every extreme that they name: `tile_inverse`: each block is symmetric positive definite.
All inputs are finite; a program needn't handle non-finite values. No bound on the sum of `nodata` or of `ground_mask` or of `source_mask` on one device may be relied on, other than what follows from the above.
Results may differ from the reference program's by a relative error of at most 0.00025.
Values sent between devices are 32-bit elements; how exact they have to be, the bound alone decides.
A program may use at most 64 MiB of HBM per device.

```python
import math
import jax
import jax.numpy as jnp
from jax import lax

NC = 1024
ITERS = 2
NR = 32
PAIRS = 256


def draw_tile_inverse(key, part):
    key_off, key_diag = jax.random.split(jax.random.fold_in(key, 7))
    block_shape = (NR, NC // 128, 128, 128)
    spread_top = 0.02
    lower_end = 0.5
    upper_end = 1.5
    raw_values = jax.random.uniform(key_off, block_shape, jnp.float32, -spread_top, spread_top)
    upper_half = jnp.triu(raw_values, 1)
    off_part = upper_half + jnp.swapaxes(upper_half, -1, -2)
    base_part = jax.random.uniform(key_diag, block_shape[:-1], jnp.float32, lower_end, upper_end)
    diag_part = jnp.sum(jnp.abs(off_part), axis=-1) + base_part
    return off_part + diag_part[..., None] * jnp.eye(128, dtype=jnp.float32)


def set_ends(values, rng, least, high):
    place = [jax.random.randint(jax.random.fold_in(rng, axis), (), 0, length) for axis, length in enumerate(values.shape)]
    main_axis = values.shape.index(max(values.shape))
    neighbour = place[:main_axis] + [(place[main_axis] + 1) % values.shape[main_axis]] + place[main_axis + 1:]
    return values.at[tuple(place)].set(least).at[tuple(neighbour)].set(high)


def shard_levels(key, shape, cuts, smallest, top_value):
    gain, own = 1.0, jax.random.fold_in(key, 6)
    for dim, blocks in cuts:
        heights = jnp.exp(jax.random.uniform(jax.random.fold_in(own, dim), (blocks,), jnp.float32, smallest / len(cuts), top_value / len(cuts)))
        gain = gain * jnp.repeat(heights, shape[dim] // blocks).reshape([-1 if axis == dim else 1 for axis in range(len(shape))])
    return gain


def setup_inputs(seed: int = 0, part: int = 0) -> dict:
    keys = jax.random.split(jax.random.key(seed), 9)
    part_keys = jax.random.split(jax.random.fold_in(keys[8], part), 9)
    return {
        "conductance": jnp.clip(jnp.exp(math.log(2.0) - 3.6888794 * jax.random.uniform(part_keys[0], (NR, NC), jnp.float32) ** shard_levels(part_keys[0], (NR, NC), ((0, 4),), -0.2, 0.2)), 0.05, 2.0),
        "nodata": set_ends((jax.random.randint(part_keys[1], (NR, NC), 0, 10) < 1).astype(jnp.int32), jax.random.fold_in(part_keys[1], 1), 0, 1),
        "ground_mask": set_ends((jax.random.randint(part_keys[2], (NR, NC), 0, 20) < 1).astype(jnp.int32), jax.random.fold_in(part_keys[2], 1), 0, 1),
        "ground_value": jnp.clip(jnp.exp(math.log(4.0) - 2.0794415 * jax.random.uniform(part_keys[3], (NR, NC), jnp.float32) ** shard_levels(part_keys[3], (NR, NC), ((0, 4),), -0.2, 0.2)), 0.5, 4.0),
        "source_mask": set_ends((jax.random.randint(part_keys[4], (NR, NC), 0, 3) < 1).astype(jnp.int32), jax.random.fold_in(part_keys[4], 1), 0, 1),
        "source_current": jnp.clip(jnp.exp(math.log(4.0) - 2.0794415 * jax.random.uniform(part_keys[5], (NR, NC), jnp.float32) ** shard_levels(part_keys[5], (NR, NC), ((0, 4),), -0.2, 0.2)), 0.5, 4.0),
        "tile_inverse": draw_tile_inverse(jax.random.fold_in(jax.random.fold_in(keys[8], part), 71), part),
        "focal_cells": set_ends(jax.random.randint(part_keys[7], (PAIRS, 2), 0, NR * NC), jax.random.fold_in(part_keys[7], 1), 0, (NR * NC) - 1).astype(jnp.int32),
    }


LEAKAGE = 0.05
FOCAL_CURRENT = 16.0


def weights_from(padded_g, padded_v, valid_mask, ground_mask, ground_value):
    centre = padded_g[1:-1, 1:-1]
    north_w = 0.5 * (centre + padded_g[:-2, 1:-1]) * valid_mask * padded_v[:-2, 1:-1]
    south_w = 0.5 * (centre + padded_g[2:, 1:-1]) * valid_mask * padded_v[2:, 1:-1]
    west_w = 0.5 * (centre + padded_g[1:-1, :-2]) * valid_mask * padded_v[1:-1, :-2]
    east_w = 0.5 * (centre + padded_g[1:-1, 2:]) * valid_mask * padded_v[1:-1, 2:]
    grounded = ground_mask.astype(jnp.float32) * ground_value
    diagonal = valid_mask * (LEAKAGE + grounded) + (1.0 - valid_mask) + north_w + south_w + west_w + east_w
    return diagonal, north_w, south_w, west_w, east_w


def stencil(padded, weights):
    diagonal, north_w, south_w, west_w, east_w = weights
    centre = padded[:, 1:-1, 1:-1]
    return (diagonal * centre - north_w * padded[:, :-2, 1:-1] - south_w * padded[:, 2:, 1:-1]
            - west_w * padded[:, 1:-1, :-2] - east_w * padded[:, 1:-1, 2:])


def precondition(field_in, tile_inverse):
    pair_count, row_count, col_count = field_in.shape
    blocks = field_in.reshape(pair_count, row_count, col_count // 128, 128)
    result = jnp.einsum("rcij,prcj->prci", tile_inverse, blocks,
                        precision=lax.Precision.HIGHEST, preferred_element_type=jnp.float32)
    return result.reshape(pair_count, row_count, col_count)


def inner_sum(first, second):
    return jnp.sum(first * second, axis=(1, 2))


def reference(conductance, nodata, ground_mask, ground_value, source_mask, source_current, tile_inverse, focal_cells):
    valid_mask = (1 - nodata).astype(jnp.float32)
    active = conductance * valid_mask
    weights = weights_from(jnp.pad(active, 1), jnp.pad(valid_mask, 1), valid_mask, ground_mask, ground_value)
    row_count, col_count = conductance.shape
    cell_ids = jnp.arange(row_count * col_count, dtype=jnp.int32)
    onehot = ((cell_ids[None, :] == focal_cells[:, 0:1]).astype(jnp.float32)
              - (cell_ids[None, :] == focal_cells[:, 1:2]).astype(jnp.float32))
    onehot = onehot.reshape(focal_cells.shape[0], row_count, col_count)
    background = source_mask.astype(jnp.float32) * source_current
    right_side = background[None] + FOCAL_CURRENT * onehot
    solution = jnp.zeros_like(right_side)
    residual = right_side
    precond = precondition(residual, tile_inverse)
    direction = precond
    gamma_now = inner_sum(residual, precond)
    for iteration in range(ITERS):
        padded = jnp.pad(direction, ((0, 0), (1, 1), (1, 1)))
        image = stencil(padded, weights)
        step_len = gamma_now / inner_sum(direction, image)
        solution = solution + step_len[:, None, None] * direction
        residual = residual - step_len[:, None, None] * image
        if iteration + 1 < ITERS:
            precond = precondition(residual, tile_inverse)
            gamma_next = inner_sum(residual, precond)
            direction = precond + (gamma_next / gamma_now)[:, None, None] * direction
            gamma_now = gamma_next
    return solution, residual
```

```python
import functools

import jax
import jax.numpy as jnp
from jax import lax
from jax.experimental import pallas as pl
from jax.experimental.pallas import tpu as pltpu
from jax.sharding import PartitionSpec as P

LEAKAGE = 0.05
FOCAL_CURRENT = 16.0
LANES = 128
EXTRA = 8
F32 = jnp.float32
BF16 = jnp.bfloat16


def fold(x):
    out = x[:, :LANES]
    for c in range(1, x.shape[1] // LANES):
        out = out + x[:, c * LANES:(c + 1) * LANES]
    return out


def krylov_kernel(
    count, cond_hbm, nodata_hbm, gmask_hbm, gval_hbm, smask_hbm, scur_hbm, t_hbm, focal_hbm,
    r0_ref, q_ref, w_ref, z_ref, y_ref, coef_ref,
    cond_ref, nodata_ref, gmask_ref, gval_ref, smask_ref, scur_ref, focal_ref, t_ref,
    thl_ref, wts_ref, qhalo_ref, zhalo_ref, msg_ref, got_ref, tmsg_ref, tgot_ref, zmsg_ref, zgot_ref,
    acc_ref, stat_ref, all_ref, late_ref, lates_ref,
    send1, recv1, sendt, recvt, send2, recv2, send3, recv3, send4, recv4, sem_in, sem_t,
):
    rows, cols = cond_ref.shape
    tiles = cols // LANES
    pairs = focal_ref.shape[1]
    ext = pairs + EXTRA
    me = lax.axis_index("space")
    last = count - 1

    barrier = pltpu.get_barrier_semaphore()
    for off in range(1, count):
        pl.semaphore_signal(
            barrier, inc=1, device_id={"space": lax.rem(me + off, count)},
            device_id_type=pl.DeviceIdType.MESH,
        )

    loads = [
        pltpu.make_async_copy(src, dst, sem_in.at[i])
        for i, (src, dst) in enumerate((
            (focal_hbm, focal_ref), (smask_hbm, smask_ref), (scur_hbm, scur_ref),
            (cond_hbm, cond_ref), (nodata_hbm, nodata_ref), (gmask_hbm, gmask_ref),
            (gval_hbm, gval_ref),
        ))
    ]

    def t_load(r):
        return pltpu.make_async_copy(t_hbm.at[r], t_ref.at[r], sem_t.at[r])

    for load in loads:
        load.start()
    for r in (0, rows - 1):
        t_load(r).start()
    for load in loads:
        load.wait()
    for r in range(1, rows - 1):
        t_load(r).start()

    valid = (1 - nodata_ref[...]).astype(F32)
    active = cond_ref[...] * valid
    background = smask_ref[...].astype(F32) * scur_ref[...]

    def edge(a, b, v, u):
        return 0.5 * (a + b) * v * u

    def set_weights():
        grounded = gmask_ref[...].astype(F32) * gval_ref[...]
        lane = lax.broadcasted_iota(jnp.int32, (rows, cols), 1)
        row = lax.broadcasted_iota(jnp.int32, (rows, cols), 0)

        def shifted(x, at, by, axis, edge_at):
            return jnp.where(at == edge_at, 0.0, pltpu.roll(x, by, axis))

        nw, sw, ww, ew = (
            edge(active, shifted(active, *how), valid, shifted(valid, *how))
            for how in ((row, 1, 0, 0), (row, rows - 1, 0, rows - 1),
                        (lane, 1, 1, 0), (lane, cols - 1, 1, cols - 1))
        )
        dg = valid * (LEAKAGE + grounded) + (1.0 - valid) + nw + sw + ww + ew
        for r in range(rows):
            for i, x in enumerate((dg, nw, sw, ww, ew, 0.5 * dg)):
                wts_ref[r, i:i + 1, :] = x[r:r + 1, :]

    acc_ref[...] = jnp.zeros(acc_ref.shape, F32)
    diagonal = lax.broadcasted_iota(jnp.int32, (ext, pairs), 0) == lax.broadcasted_iota(
        jnp.int32, (ext, pairs), 1)
    is_pair = lax.broadcasted_iota(jnp.int32, (ext, 1), 0) < pairs

    def column(i):
        line = jnp.broadcast_to(focal_ref[i:i + 1, :].astype(F32), (ext, pairs))
        at = jnp.sum(jnp.where(diagonal, line, 0.0), 1, keepdims=True).astype(jnp.int32)
        return jnp.where(is_pair, at, -1)

    fa, fb = column(0), column(1)

    def right_side(r):
        ids = (me * rows + r) * cols + lax.broadcasted_iota(jnp.int32, (ext, cols), 1)
        onehot = (ids == fa).astype(F32) - (ids == fb).astype(F32)
        r0_ref[r] = background[r:r + 1, :] + FOCAL_CURRENT * onehot

    right_side(0)
    right_side(rows - 1)

    def precond_row(src, dst, r, split):
        for c in range(tiles):
            cut = slice(c * LANES, (c + 1) * LANES)
            if split:
                t = t_ref[r, c]
                thi = t.astype(BF16)
                thl_ref[r, c, :, :LANES] = thi
                thl_ref[r, c, :, LANES:] = (t - thi.astype(F32)).astype(BF16)
            x = src[r, :, cut]
            hi = x.astype(BF16).astype(F32)
            lhs = jnp.concatenate([hi, x - hi], 0).astype(BF16)
            o = jnp.dot(lhs, thl_ref[r, c], preferred_element_type=F32)
            dst[r, :, cut] = o[:ext, :LANES] + (o[:ext, LANES:] + (o[ext:, :LANES] + o[ext:, LANES:]))

    def precond_inner(src, dst, split):
        def body(r, carry):
            if split:
                t_load(r).wait()
            precond_row(src, dst, r, split)
            return carry
        lax.fori_loop(1, rows - 1, body, 0)

    def over_groups(number, body):
        def step(g, carry):
            body(pl.ds(pl.multiple_of(g * 8, 8), 8))
            return carry
        lax.fori_loop(0, number, step, 0, unroll=next(u for u in (4, 3, 2, 1) if number % u == 0))

    def apply_row(src, dst, r, north, south, number, first=None, second=None):
        def body(s):
            ce = src[r, s, :]
            out = wts_ref[r, 0:1, :] * ce
            if north is not None:
                out = out - wts_ref[r, 1:2, :] * north[0][north[1], s, :]
            if south is not None:
                out = out - wts_ref[r, 2:3, :] * south[0][south[1], s, :]
            out = (
                out
                - wts_ref[r, 3:4, :] * pltpu.roll(ce, 1, 1)
                - wts_ref[r, 4:5, :] * pltpu.roll(ce, cols - 1, 1)
            )
            dst[r, s, :] = out
            if first is not None:
                acc_ref[0, s, :] += fold(first[r, s, :] * ce)
            if second:
                acc_ref[1, s, :] += fold(ce * out)
        over_groups(number, body)

    def apply_inner(src, dst, number, first=None, second=None):
        def body(r, carry):
            apply_row(src, dst, r, (src, r - 1), (src, r + 1), number, first, second)
            return carry
        lax.fori_loop(1, rows - 1, body, 0)

    def moment_row(r, north):
        def body(s):
            z = z_ref[r, s, :]
            t = wts_ref[r, 5:6, :] * z - wts_ref[r, 3:4, :] * pltpu.roll(z, 1, 1)
            if north:
                t = t - wts_ref[r, 1:2, :] * z_ref[r - 1, s, :]
            acc_ref[2, s, :] += fold(w_ref[r, s, :] * z)
            acc_ref[3, s, :] += fold(t * z)
        over_groups(pairs // 8, body)

    def side_copy(src, dst, ssem, rsem, side):
        return pltpu.make_async_remote_copy(
            src_ref=src.at[side], dst_ref=dst.at[1 - side],
            send_sem=ssem.at[side], recv_sem=rsem.at[1 - side],
            device_id={"space": me - 1 if side == 0 else me + 1},
            device_id_type=pl.DeviceIdType.MESH,
        )

    has = (me > 0, me < last)

    def done(src, dst, ssem, rsem):
        for side in range(2):
            @pl.when(has[side])
            def _():
                side_copy(src, dst, ssem, rsem, side).wait_send()
                pltpu.make_async_remote_copy(
                    src_ref=src.at[1 - side], dst_ref=dst.at[side],
                    send_sem=ssem.at[1 - side], recv_sem=rsem.at[side],
                    device_id={"space": me - 1 if side == 0 else me + 1},
                    device_id_type=pl.DeviceIdType.MESH,
                ).wait_recv()

    for r in (0, rows - 1):
        t_load(r).wait()
        precond_row(r0_ref, q_ref, r, True)

    tile_a = lax.shift_right_logical(fa[:pairs] & (cols - 1), 7)
    tile_b = lax.shift_right_logical(fb[:pairs] & (cols - 1), 7)

    def pack(src, r, dst, side):
        va = src[r, :pairs, 0:LANES]
        vb = va
        for c in range(1, tiles):
            x = src[r, :pairs, c * LANES:(c + 1) * LANES]
            va = jnp.where(tile_a == c, x, va)
            vb = jnp.where(tile_b == c, x, vb)
        dst[side, 0:pairs, :] = va
        dst[side, pairs:2 * pairs, :] = vb
        for c in range(tiles):
            at = 2 * pairs + c
            dst[side, at:at + 1, :] = src[r, pairs:pairs + 1, c * LANES:(c + 1) * LANES]

    ends = ((0, 0), (1, rows - 1))
    for side, r in ends:
        pack(q_ref, r, msg_ref, side)
        for c in range(tiles):
            cut = slice(c * LANES, (c + 1) * LANES)
            at = 2 * pairs + c
            msg_ref[side, at + tiles:at + tiles + 1, :] = active[r:r + 1, cut]
            msg_ref[side, at + 2 * tiles:at + 2 * tiles + 1, :] = valid[r:r + 1, cut]
            tmsg_ref[side, c:c + 1, :] = t_ref[r, c, 0:1, :]
            tmsg_ref[side, tiles + c:tiles + c + 1, :] = t_ref[r, c, LANES - 1:LANES, :]

    pl.semaphore_wait(barrier, last)
    for side in range(2):
        @pl.when(has[side])
        def _():
            side_copy(msg_ref, got_ref, send1, recv1, side).start()
            side_copy(tmsg_ref, tgot_ref, sendt, recvt, side).start()

        @pl.when(jnp.logical_not(has[side]))
        def _():
            for ref in (got_ref, tgot_ref, zgot_ref):
                ref[side] = jnp.zeros(ref.shape[1:], F32)

    set_weights()
    for r in range(1, rows - 1):
        right_side(r)
    precond_inner(r0_ref, q_ref, True)
    apply_inner(q_ref, w_ref, ext // 8, r0_ref, True)
    apply_row(q_ref, w_ref, 0, None, (q_ref, 1), ext // 8, r0_ref)
    apply_row(q_ref, w_ref, rows - 1, (q_ref, rows - 2), None, ext // 8, r0_ref)

    done(msg_ref, got_ref, send1, recv1)

    def row_of(side, base):
        return jnp.concatenate([got_ref[side, base + c:base + c + 1, :] for c in range(tiles)], 1)

    halo_a = [row_of(side, 2 * pairs + tiles) for side in range(2)]
    halo_v = [row_of(side, 2 * pairs + 2 * tiles) for side in range(2)]
    for side, r in ends:
        i = 1 + side
        h = edge(active[r:r + 1, :], halo_a[side], valid[r:r + 1, :], halo_v[side])
        wts_ref[r, i:i + 1, :] = h
        wts_ref[r, 0:1, :] += h
        wts_ref[r, 5:6, :] += 0.5 * h
        va = got_ref[side, 0:pairs, :]
        vb = got_ref[side, pairs:2 * pairs, :]
        dots = jnp.zeros((pairs, LANES), F32)
        for c in range(tiles):
            cut = slice(c * LANES, (c + 1) * LANES)
            common = got_ref[side, 2 * pairs + c:2 * pairs + c + 1, :]
            qh = jnp.where(
                tile_a == c, va, jnp.where(tile_b == c, vb, jnp.broadcast_to(common, va.shape))
            )
            qhalo_ref[side, :, cut] = qh - common
            q0 = q_ref[r, :pairs, cut]
            w0 = w_ref[r, :pairs, cut] + h[:, cut] * (q0 - qh)
            w_ref[r, :pairs, cut] = w0
            w_ref[r, pairs:ext, cut] += h[:, cut] * (q_ref[r, pairs:ext, cut] - common)
            dots = dots + q0 * w0
        acc_ref[1, :pairs, :] += dots

    precond_row(w_ref, z_ref, 0, False)
    precond_row(w_ref, z_ref, rows - 1, False)
    for side, r in ends:
        pack(z_ref, r, zmsg_ref, side)
    for side in range(2):
        @pl.when(has[side])
        def _():
            side_copy(zmsg_ref, zgot_ref, send2, recv2, side).start()

    precond_inner(w_ref, z_ref, False)
    moment_row(0, False)

    def moments(r, carry):
        moment_row(r, True)
        return carry

    lax.fori_loop(1, rows, moments, 0)

    lane = lax.broadcasted_iota(jnp.int32, (LANES, LANES), 1)
    pad = jnp.zeros((LANES - pairs, 1), F32)

    def lines(sums):
        table = jnp.zeros((LANES, LANES), F32)
        for i, x in enumerate(sums):
            col = jnp.concatenate([jnp.sum(x, 1, keepdims=True), pad], 0)
            table = jnp.where(lane == i, jnp.broadcast_to(col, table.shape), table)
        return table.T[0:8, :]

    def exchange(src, dst, ssem, rsem):
        return [
            pltpu.make_async_remote_copy(
                src_ref=src, dst_ref=dst.at[k - 1],
                send_sem=ssem.at[k - 1], recv_sem=rsem.at[k - 1],
                device_id={"space": lax.rem(me + k, count)}, device_id_type=pl.DeviceIdType.MESH,
            )
            for k in range(1, count)
        ]

    early = lines([acc_ref[i, :pairs, :] for i in range(4)])
    stat_ref[...] = early
    early_copies = exchange(stat_ref, all_ref, send3, recv3)
    for copy in early_copies:
        copy.start()

    done(tmsg_ref, tgot_ref, sendt, recvt)
    for side in range(2):
        between = edge(halo_a[side][:, :-1], halo_a[side][:, 1:], halo_v[side][:, :-1], halo_v[side][:, 1:])
        for c in range(tiles):
            cut = slice(c * LANES, (c + 1) * LANES)
            near = jnp.zeros((pairs, LANES), F32)
            if c > 0:
                at = c * LANES - 1
                near = near - (between[:, at:at + 1] * qhalo_ref[side, :, at:at + 1]) * tgot_ref[side, c:c + 1, :]
            if c < tiles - 1:
                at = (c + 1) * LANES
                near = near - (between[:, at - 1:at] * qhalo_ref[side, :, at:at + 1]) * tgot_ref[
                    side, tiles + c:tiles + c + 1, :]
            zhalo_ref[side, :, cut] = near

    done(zmsg_ref, zgot_ref, send2, recv2)
    coupling = []
    for side, r in ends:
        va = zgot_ref[side, 0:pairs, :]
        vb = zgot_ref[side, pairs:2 * pairs, :]
        total = jnp.zeros((pairs, LANES), F32)
        for c in range(tiles):
            cut = slice(c * LANES, (c + 1) * LANES)
            other = zgot_ref[side, 2 * pairs + c:2 * pairs + c + 1, :] + zhalo_ref[side, :, cut]
            zh = jnp.where(tile_a == c, va, jnp.where(tile_b == c, vb, other))
            zhalo_ref[side, :, cut] = zh
            total = total + wts_ref[r, 1 + side:2 + side, cut] * z_ref[r, :pairs, cut] * zh
        coupling.append(total)
    late = lines(coupling)
    late_ref[...] = late
    late_copies = exchange(late_ref, lates_ref, send4, recv4)
    for copy in late_copies:
        copy.start()

    apply_inner(z_ref, y_ref, pairs // 8)
    apply_row(z_ref, y_ref, 0, (zhalo_ref, 0), (z_ref, 1), pairs // 8)
    apply_row(z_ref, y_ref, rows - 1, (z_ref, rows - 2), (zhalo_ref, 1), pairs // 8)

    for copy in early_copies:
        copy.wait()
    total = early
    for k in range(1, count):
        total = total + all_ref[k - 1]
    for copy in late_copies:
        copy.wait()
    joint = late[0:1, :] + late[1:2, :]
    for k in range(1, count):
        joint = joint + jnp.where(k <= me, lates_ref[k - 1, 0:1, :], lates_ref[k - 1, 1:2, :])
    gamma0, kappa, mu, half = (total[i:i + 1, :] for i in range(4))
    nu = 2.0 * (half - joint)
    a0 = gamma0 / kappa
    gamma1 = a0 * a0 * mu - gamma0
    beta = gamma1 / gamma0
    a1 = gamma1 / (kappa - 2.0 * a0 * mu + a0 * a0 * nu - beta * gamma1 / a0)
    first = a0 + a1 * (1.0 + beta)
    both = jnp.concatenate([first, a0 * a1, jnp.zeros((LANES - 2, LANES), F32)], 0).T
    lane_p = lax.broadcasted_iota(jnp.int32, (pairs, LANES), 1)
    coef_ref[...] = jnp.where(lane_p < LANES // 2, both[:pairs, 0:1], both[:pairs, 1:2])


def combine_kernel(coef_ref, r0_ref, q_ref, w_ref, z_ref, y_ref, sol_hbm, res_hbm, sol_ref, res_ref, sem):
    pairs, rows, cols = sol_ref.shape
    block = 8

    def out(i, src, dst, k):
        cut = pl.ds(pl.multiple_of(i * block, block), block)
        return pltpu.make_async_copy(src.at[cut], dst.at[cut], sem.at[k, i])

    def body(i, carry):
        cut = pl.ds(pl.multiple_of(i * block, block), block)
        one = coef_ref[cut, 0:1]
        two = coef_ref[cut, LANES - 1:LANES]
        for r in range(rows):
            sol_ref[cut, r, :] = one * q_ref[r, cut, :] - two * z_ref[r, cut, :]
            res_ref[cut, r, :] = r0_ref[r, cut, :] - one * w_ref[r, cut, :] + two * y_ref[r, cut, :]
        out(i, sol_ref, sol_hbm, 0).start()
        out(i, res_ref, res_hbm, 1).start()
        return carry

    lax.fori_loop(0, pairs // block, body, 0)

    def finish(i, carry):
        out(i, sol_ref, sol_hbm, 0).wait()
        out(i, res_ref, res_hbm, 1).wait()
        return carry

    lax.fori_loop(0, pairs // block, finish, 0)


def on_device(count, cond, nodata, gmask, gval, smask, scur, tinv, focal):
    rows, cols = cond.shape
    pairs = focal.shape[0]
    tiles = cols // LANES
    ext = pairs + EXTRA
    field = jax.ShapeDtypeStruct((rows, ext, cols), F32)
    vm = pl.BlockSpec(memory_space=pltpu.VMEM)
    hbm = pl.BlockSpec(memory_space=pltpu.HBM)
    msg = (2, 2 * pairs + 3 * tiles, LANES)
    tmsg = (2, 2 * tiles, LANES)
    zmsg = (2, 2 * pairs + tiles, LANES)
    others = count - 1
    small = (rows, cols)
    r0, q, w, z, y, coef = pl.pallas_call(
        functools.partial(krylov_kernel, count),
        out_shape=[field] * 5 + [jax.ShapeDtypeStruct((pairs, LANES), F32)],
        in_specs=[hbm] * 8,
        out_specs=[vm] * 6,
        scratch_shapes=[
            pltpu.VMEM(small, F32),
            pltpu.VMEM(small, jnp.int32),
            pltpu.VMEM(small, jnp.int32),
            pltpu.VMEM(small, F32),
            pltpu.VMEM(small, jnp.int32),
            pltpu.VMEM(small, F32),
            pltpu.VMEM((2, pairs), jnp.int32),
            pltpu.VMEM(tinv.shape, F32),
            pltpu.VMEM((rows, tiles, LANES, 2 * LANES), BF16),
            pltpu.VMEM((rows, 8, cols), F32),
            pltpu.VMEM((2, pairs, cols), F32),
            pltpu.VMEM((2, pairs, cols), F32),
            pltpu.VMEM(msg, F32),
            pltpu.VMEM(msg, F32),
            pltpu.VMEM(tmsg, F32),
            pltpu.VMEM(tmsg, F32),
            pltpu.VMEM(zmsg, F32),
            pltpu.VMEM(zmsg, F32),
            pltpu.VMEM((4, ext, LANES), F32),
            pltpu.VMEM((8, LANES), F32),
            pltpu.VMEM((others, 8, LANES), F32),
            pltpu.VMEM((8, LANES), F32),
            pltpu.VMEM((others, 8, LANES), F32),
            *[pltpu.SemaphoreType.DMA((2,))] * 6,
            *[pltpu.SemaphoreType.DMA((others,))] * 4,
            pltpu.SemaphoreType.DMA((7,)),
            pltpu.SemaphoreType.DMA((rows,)),
        ],
        compiler_params=pltpu.CompilerParams(
            collective_id=0, has_side_effects=True, vmem_limit_bytes=36 * 1024 * 1024
        ),
        name="krylov",
    )(*(
        pltpu.with_memory_space_constraint(x, pltpu.HBM)
        for x in (cond, nodata, gmask, gval, smask, scur, tinv, focal.T)
    ))

    out = jax.ShapeDtypeStruct((pairs, rows, cols), F32)
    return tuple(pl.pallas_call(
        combine_kernel,
        out_shape=[out, out],
        in_specs=[vm] * 6,
        out_specs=[hbm, hbm],
        scratch_shapes=[
            pltpu.VMEM(out.shape, F32),
            pltpu.VMEM(out.shape, F32),
            pltpu.SemaphoreType.DMA((2, pairs // 8)),
        ],
        compiler_params=pltpu.CompilerParams(vmem_limit_bytes=20 * 1024 * 1024),
        name="combine",
    )(coef, r0, q, w, z, y))


def solution(mesh):
    return jax.shard_map(
        functools.partial(on_device, mesh.shape["space"]),
        mesh=mesh,
        in_specs=(
            P(("groups", "space"), None),
            P(("groups", "space"), None),
            P(("groups", "space"), None),
            P(("groups", "space"), None),
            P(("groups", "space"), None),
            P(("groups", "space"), None),
            P(("groups", "space"), None, None, None),
            P(("groups", "rhs"), None),
        ),
        out_specs=(P("rhs", ("groups", "space"), None), P("rhs", ("groups", "space"), None)),
        check_vma=False,
    )
```

```python
import functools

import jax
import jax.numpy as jnp
from jax import lax
from jax.experimental import pallas as pl
from jax.experimental.pallas import tpu as pltpu
from jax.sharding import PartitionSpec as P

LEAKAGE = 0.05
FOCAL_CURRENT = 16.0
LANES = 128
EXTRA = 8
F32 = jnp.float32
BF16 = jnp.bfloat16


def krylov_kernel(
    count, cond_hbm, nodata_hbm, gmask_hbm, gval_hbm, smask_hbm, scur_hbm, t_hbm, focal_hbm,
    r0_ref, q_ref, w_ref, z_ref, y_ref, coef_ref,
    cond_ref, nodata_ref, gmask_ref, gval_ref, smask_ref, scur_ref, focal_ref, ids_ref, te_ref, ti_ref,
    thl_ref, wts_ref, spot_ref, qhalo_ref, zhalo_ref, msg_ref, got_ref, bmsg_ref, bgot_ref, tmsg_ref, tgot_ref,
    zmsg_ref, zgot_ref, acc_ref, stat_ref, all_ref, late_ref, lates_ref,
    send1, recv1, sendb, recvb, sendt, recvt, send2, recv2, send3, recv3, send4, recv4, sem_in, sem_t,
):
    rows, cols = cond_ref.shape
    tiles = cols // LANES
    pairs = focal_ref.shape[1]
    ext = pairs + EXTRA
    me = lax.axis_index("space")
    last = count - 1
    ends = ((0, 0), (1, rows - 1))
    inner = range(1, rows - 1)
    cuts = [slice(c * LANES, (c + 1) * LANES) for c in range(tiles)]

    barrier = pltpu.get_barrier_semaphore()
    for off in range(1, count):
        pl.semaphore_signal(
            barrier, inc=1, device_id={"space": lax.rem(me + off, count)},
            device_id_type=pl.DeviceIdType.MESH,
        )

    loads = [
        pltpu.make_async_copy(src, dst, sem_in.at[i])
        for i, (src, dst) in enumerate((
            (focal_hbm, ids_ref), (focal_hbm, focal_ref), (t_hbm.at[0], te_ref.at[pl.ds(0, cols)]),
            (t_hbm.at[rows - 1], te_ref.at[pl.ds(cols, cols)]), (smask_hbm, smask_ref), (scur_hbm, scur_ref),
            (cond_hbm, cond_ref), (nodata_hbm, nodata_ref), (gmask_hbm, gmask_ref), (gval_hbm, gval_ref),
        ))
    ]
    t_loads = [
        pltpu.make_async_copy(t_hbm.at[r], ti_ref.at[pl.ds((r - 1) * cols, cols)], sem_t.at[r]) for r in inner
    ]
    for load in loads:
        load.start()
    for load in loads:
        load.wait()
    for load in t_loads:
        load.start()

    def gather(src, at):
        for p in range(pairs):
            for i in range(2):
                spot_ref[i, p:p + 1, :] = src[pl.ds(at(ids_ref[i, p]), 1), :]
        return FOCAL_CURRENT * spot_ref[0], -FOCAL_CURRENT * spot_ref[1]

    half = (rows * cols // 2).bit_length() - 1
    near_a, near_b = gather(
        te_ref, lambda i: (i & (cols - 1)) + (lax.shift_right_logical(i, half) & 1) * cols)

    diagonal = lax.broadcasted_iota(jnp.int32, (pairs, pairs), 0) == lax.broadcasted_iota(
        jnp.int32, (pairs, pairs), 1)
    lane = lax.broadcasted_iota(jnp.int32, (pairs, LANES), 1)

    def column(i):
        line = jnp.broadcast_to(focal_ref[i:i + 1, :].astype(F32), (pairs, pairs))
        return jnp.broadcast_to(
            jnp.sum(jnp.where(diagonal, line, 0.0), 1, keepdims=True).astype(jnp.int32), (pairs, LANES))

    at_a, at_b = (column(i) - me * (rows * cols) for i in range(2))
    spot_a, spot_b = (lax.shift_right_arithmetic(x, 7) for x in (at_a, at_b))
    tile_a, tile_b = spot_a & (tiles - 1), spot_b & (tiles - 1)

    def within(spot, low, high):
        return jnp.logical_and(spot >= low * tiles, spot < high * tiles)

    for side, r in ends:
        msg_ref[side, 0:pairs, :] = jnp.where(within(spot_a, r, r + 1), near_a, 0.0)
        msg_ref[side, pairs:2 * pairs, :] = jnp.where(within(spot_b, r, r + 1), near_b, 0.0)

    def side_copy(src, dst, ssem, rsem, side):
        return pltpu.make_async_remote_copy(
            src_ref=src.at[side], dst_ref=dst.at[1 - side],
            send_sem=ssem.at[side], recv_sem=rsem.at[1 - side],
            device_id={"space": me - 1 if side == 0 else me + 1},
            device_id_type=pl.DeviceIdType.MESH,
        )

    has = (me > 0, me < last)

    def send(src, dst, ssem, rsem):
        for side in range(2):
            @pl.when(has[side])
            def _():
                side_copy(src, dst, ssem, rsem, side).start()

            @pl.when(jnp.logical_not(has[side]))
            def _():
                dst[side] = jnp.zeros(dst.shape[1:], F32)

    def done(src, dst, ssem, rsem):
        for side in range(2):
            @pl.when(has[side])
            def _():
                side_copy(src, dst, ssem, rsem, side).wait_send()
                pltpu.make_async_remote_copy(
                    src_ref=src.at[1 - side], dst_ref=dst.at[side],
                    send_sem=ssem.at[1 - side], recv_sem=rsem.at[side],
                    device_id={"space": me - 1 if side == 0 else me + 1},
                    device_id_type=pl.DeviceIdType.MESH,
                ).wait_recv()

    pl.semaphore_wait(barrier, last)
    send(msg_ref, got_ref, send1, recv1)

    valid = (1 - nodata_ref[...]).astype(F32)
    active = cond_ref[...] * valid
    background = smask_ref[...].astype(F32) * scur_ref[...]

    def tile_of(r, c):
        if r == 0 or r == rows - 1:
            return te_ref[pl.ds((cols if r else 0) + c * LANES, LANES), :]
        return ti_ref[pl.ds((r - 1) * cols + c * LANES, LANES), :]

    def product(x, r, c):
        number = x.shape[0]
        hi = x.astype(BF16).astype(F32)
        lhs = jnp.concatenate([hi, x - hi], 0).astype(BF16)
        o = jnp.dot(lhs, thl_ref[r, c], preferred_element_type=F32)
        return o[:number, :LANES] + (o[:number, LANES:] + (o[number:, :LANES] + o[number:, LANES:]))

    def shared_row(r):
        dot = jnp.zeros((EXTRA, LANES), F32)
        for c, cut in enumerate(cuts):
            t = tile_of(r, c)
            thi = t.astype(BF16)
            thl_ref[r, c, :, :LANES] = thi
            thl_ref[r, c, :, LANES:] = (t - thi.astype(F32)).astype(BF16)
            x = jnp.broadcast_to(background[r:r + 1, cut], (EXTRA, LANES))
            q = product(x, r, c)
            q_ref[r, pairs:ext, cut] = q
            dot = dot + x * q
        return dot

    shared = shared_row(0) + shared_row(rows - 1)
    for side, r in ends:
        for c, cut in enumerate(cuts):
            bmsg_ref[side, c:c + 1, :] = q_ref[r, pairs:pairs + 1, cut]
            bmsg_ref[side, tiles + c:tiles + c + 1, :] = active[r:r + 1, cut]
            bmsg_ref[side, 2 * tiles + c:2 * tiles + c + 1, :] = valid[r:r + 1, cut]
            first = r and cols
            tmsg_ref[side, c:c + 1, :] = te_ref[first + c * LANES:first + c * LANES + 1, :]
            tmsg_ref[side, tiles + c:tiles + c + 1, :] = te_ref[
                first + c * LANES + LANES - 1:first + (c + 1) * LANES, :]
    send(bmsg_ref, bgot_ref, sendb, recvb)
    send(tmsg_ref, tgot_ref, sendt, recvt)

    def edge(a, b, v, u):
        return 0.5 * (a + b) * v * u

    row_at = lax.broadcasted_iota(jnp.int32, (rows, cols), 0)
    col_at = lax.broadcasted_iota(jnp.int32, (rows, cols), 1)

    def shifted(x, by, axis):
        length = x.shape[axis]
        at = (row_at, col_at)[axis][:x.shape[0], :]
        return jnp.where(at == (0 if by == 1 else length - 1), 0.0, pltpu.roll(x, by % length, axis))

    nw, sw, ww, ew = (
        edge(active, shifted(active, *how), valid, shifted(valid, *how))
        for how in ((1, 0), (-1, 0), (1, 1), (-1, 1))
    )
    dg = valid * (LEAKAGE + gmask_ref[...].astype(F32) * gval_ref[...]) + (1.0 - valid) + nw + sw + ww + ew
    for r in range(rows):
        for i, x in enumerate((dg, nw, sw, ww, ew, 0.5 * dg, background)):
            wts_ref[r, i:i + 1, :] = x[r:r + 1, :]

    for load in t_loads:
        load.wait()
    far_a, far_b = gather(
        ti_ref, lambda i: jnp.clip((i & (rows * cols - 1)) - cols, 0, (rows - 2) * cols - 1))
    for r in inner:
        shared = shared + shared_row(r)

    def dense_row(r, a, b, dot):
        for c, cut in enumerate(cuts):
            k = r * tiles + c
            x = jnp.where(spot_a == k, a, 0.0) + jnp.where(spot_b == k, b, 0.0)
            q_ref[r, 0:pairs, cut] = q_ref[r, pairs:pairs + 1, cut] + x
            dot = dot + background[r:r + 1, cut] * x
        return dot

    dot = jnp.zeros((pairs, LANES), F32)
    for r in range(rows):
        a, b = (far_a, far_b) if r in inner else (near_a, near_b)
        dot = dense_row(r, a, b, dot)
    in_a, in_b = (
        jnp.where(within(spot, 1, rows - 1), far, jnp.where(within(spot, 0, rows), near, 0.0))
        for spot, far, near in ((spot_a, far_a, near_a), (spot_b, far_b, near_b))
    )
    same = spot_a == spot_b
    own = jnp.where(lane == (at_a & (LANES - 1)), in_a + jnp.where(same, in_b, 0.0), 0.0) - jnp.where(
        lane == (at_b & (LANES - 1)), in_b + jnp.where(same, in_a, 0.0), 0.0)
    acc_ref[0] = 2.0 * dot + FOCAL_CURRENT * own + jnp.broadcast_to(shared[0:1, :], dot.shape)
    for i in range(1, 4):
        acc_ref[i] = jnp.zeros(acc_ref.shape[1:], F32)

    parts = [slice(p, p + pairs // 2) for p in (0, pairs // 2)]
    extra = slice(pairs, ext)

    def sides(xs):
        at = lane[:xs[0].shape[0]]
        west = [pltpu.roll(x, 1, 1) for x in xs]
        east = [pltpu.roll(x, LANES - 1, 1) for x in xs]
        west = west[:1] + [jnp.where(at == 0, west[c - 1], west[c]) for c in range(1, tiles)]
        east = [jnp.where(at == LANES - 1, east[c + 1], east[c]) for c in range(tiles - 1)] + east[-1:]
        return west, east

    def apply_part(src, dst, r, s, north, south, acc=None):
        xs = [src[r, s, cut] for cut in cuts]
        west, east = sides(xs)
        dots = None
        for c, cut in enumerate(cuts):
            out = (
                wts_ref[r, 0:1, cut] * xs[c] - wts_ref[r, 3:4, cut] * west[c] - wts_ref[r, 4:5, cut] * east[c]
            )
            if north is not None:
                out = out - wts_ref[r, 1:2, cut] * north[0][north[1], s, cut]
            if south is not None:
                out = out - wts_ref[r, 2:3, cut] * south[0][south[1], s, cut]
            dst[r, s, cut] = out
            dots = xs[c] * out if dots is None else dots + xs[c] * out
        if acc is not None:
            acc_ref[acc, s, :] += dots

    def apply_inner(src, dst, both, acc=None):
        def body(r, carry):
            for s in parts:
                apply_part(src, dst, r, s, (src, r - 1), (src, r + 1), acc)
            if both:
                apply_part(src, dst, r, extra, (src, r - 1), (src, r + 1))
            return carry
        lax.fori_loop(1, rows - 1, body, 0)

    apply_inner(q_ref, w_ref, True, 1)
    for s in (*parts, extra):
        apply_part(q_ref, w_ref, 0, s, None, (q_ref, 1))
        apply_part(q_ref, w_ref, rows - 1, s, (q_ref, rows - 2), None)

    done(msg_ref, got_ref, send1, recv1)
    done(bmsg_ref, bgot_ref, sendb, recvb)

    def row_of(side, base):
        return jnp.concatenate([bgot_ref[side, base + c:base + c + 1, :] for c in range(tiles)], 1)

    halo_a = [row_of(side, tiles) for side in range(2)]
    halo_v = [row_of(side, 2 * tiles) for side in range(2)]
    for side, r in ends:
        i = 1 + side
        h = edge(active[r:r + 1, :], halo_a[side], valid[r:r + 1, :], halo_v[side])
        wts_ref[r, i:i + 1, :] = h
        wts_ref[r, 0:1, :] += h
        wts_ref[r, 5:6, :] += 0.5 * h
        va = got_ref[side, 0:pairs, :]
        vb = got_ref[side, pairs:2 * pairs, :]
        dots = jnp.zeros((pairs, LANES), F32)
        for c, cut in enumerate(cuts):
            common = bgot_ref[side, c:c + 1, :]
            qh = jnp.where(tile_a == c, va, 0.0) + jnp.where(tile_b == c, vb, 0.0)
            qhalo_ref[side, :, cut] = qh
            q0 = q_ref[r, :pairs, cut]
            w0 = w_ref[r, :pairs, cut] + h[:, cut] * (q0 - (qh + common))
            w_ref[r, :pairs, cut] = w0
            w_ref[r, extra, cut] += h[:, cut] * (q_ref[r, extra, cut] - common)
            dots = dots + q0 * w0
        acc_ref[1] += dots

    def precond_row(r):
        for c, cut in enumerate(cuts):
            z_ref[r, :, cut] = product(w_ref[r, :, cut], r, c)

    def pack(src, r, dst, side):
        va = src[r, :pairs, 0:LANES]
        vb = va
        for c in range(1, tiles):
            x = src[r, :pairs, cuts[c]]
            va = jnp.where(tile_a == c, x, va)
            vb = jnp.where(tile_b == c, x, vb)
        dst[side, 0:pairs, :] = va
        dst[side, pairs:2 * pairs, :] = vb
        for c, cut in enumerate(cuts):
            dst[side, 2 * pairs + c:2 * pairs + c + 1, :] = src[r, pairs:pairs + 1, cut]

    precond_row(0)
    precond_row(rows - 1)
    for side, r in ends:
        pack(z_ref, r, zmsg_ref, side)
    send(zmsg_ref, zgot_ref, send2, recv2)

    for r in inner:
        precond_row(r)

    def moment_part(r, s, north):
        zs = [z_ref[r, s, cut] for cut in cuts]
        west, _ = sides(zs)
        mu = nu = None
        for c, cut in enumerate(cuts):
            t = wts_ref[r, 5:6, cut] * zs[c] - wts_ref[r, 3:4, cut] * west[c]
            if north:
                t = t - wts_ref[r, 1:2, cut] * z_ref[r - 1, s, cut]
            one, two = w_ref[r, s, cut] * zs[c], t * zs[c]
            mu, nu = (one, two) if mu is None else (mu + one, nu + two)
        acc_ref[2, s, :] += mu
        acc_ref[3, s, :] += nu

    def moments(r, carry):
        for s in parts:
            moment_part(r, s, True)
        return carry

    for s in parts:
        moment_part(0, s, False)
    lax.fori_loop(1, rows, moments, 0)

    square = lax.broadcasted_iota(jnp.int32, (LANES, LANES), 1)
    pad = jnp.zeros((LANES - pairs, 1), F32)

    def lines(sums):
        table = jnp.zeros((LANES, LANES), F32)
        for i, x in enumerate(sums):
            col = jnp.concatenate([jnp.sum(x, 1, keepdims=True), pad], 0)
            table = jnp.where(square == i, jnp.broadcast_to(col, table.shape), table)
        return table.T[0:8, :]

    def exchange(src, dst, ssem, rsem):
        return [
            pltpu.make_async_remote_copy(
                src_ref=src, dst_ref=dst.at[k - 1],
                send_sem=ssem.at[k - 1], recv_sem=rsem.at[k - 1],
                device_id={"space": lax.rem(me + k, count)}, device_id_type=pl.DeviceIdType.MESH,
            )
            for k in range(1, count)
        ]

    early = lines([acc_ref[i] for i in range(4)])
    stat_ref[...] = early
    early_copies = exchange(stat_ref, all_ref, send3, recv3)
    for copy in early_copies:
        copy.start()

    done(tmsg_ref, tgot_ref, sendt, recvt)
    for side in range(2):
        halo_w, halo_e = (
            edge(halo_a[side], shifted(halo_a[side], by, 1), halo_v[side], shifted(halo_v[side], by, 1))
            for by in (1, -1)
        )
        near = [jnp.zeros((pairs, LANES), F32)] * tiles
        for c, cut in enumerate(cuts):
            qh = qhalo_ref[side, :, cut]
            if c > 0:
                gone = (halo_w[:, cut] * qh)[:, 0:1]
                near[c - 1] = near[c - 1] - gone * tgot_ref[side, tiles + c - 1:tiles + c, :]
            if c < tiles - 1:
                gone = (halo_e[:, cut] * qh)[:, LANES - 1:LANES]
                near[c + 1] = near[c + 1] - gone * tgot_ref[side, c + 1:c + 2, :]
        for c, cut in enumerate(cuts):
            zhalo_ref[side, :, cut] = near[c]

    done(zmsg_ref, zgot_ref, send2, recv2)
    coupling = []
    for side, r in ends:
        va = zgot_ref[side, 0:pairs, :]
        vb = zgot_ref[side, pairs:2 * pairs, :]
        total = jnp.zeros((pairs, LANES), F32)
        for c, cut in enumerate(cuts):
            other = zgot_ref[side, 2 * pairs + c:2 * pairs + c + 1, :] + zhalo_ref[side, :, cut]
            zh = jnp.where(tile_a == c, va, jnp.where(tile_b == c, vb, other))
            zhalo_ref[side, :, cut] = zh
            total = total + wts_ref[r, 1 + side:2 + side, cut] * z_ref[r, :pairs, cut] * zh
        coupling.append(total)
    late = lines(coupling)
    late_ref[...] = late
    late_copies = exchange(late_ref, lates_ref, send4, recv4)
    for copy in late_copies:
        copy.start()

    apply_inner(z_ref, y_ref, False)
    for s in parts:
        apply_part(z_ref, y_ref, 0, s, (zhalo_ref, 0), (z_ref, 1))
        apply_part(z_ref, y_ref, rows - 1, s, (z_ref, rows - 2), (zhalo_ref, 1))

    def right_side(r, carry):
        for c, cut in enumerate(cuts):
            local = r * cols + c * LANES + lane
            x = jnp.where(local == at_a, FOCAL_CURRENT, 0.0) - jnp.where(local == at_b, FOCAL_CURRENT, 0.0)
            r0_ref[r, 0:pairs, cut] = wts_ref[r, 6:7, cut] + x
        return carry

    lax.fori_loop(0, rows, right_side, 0)

    for copy in early_copies:
        copy.wait()
    total = early
    for k in range(1, count):
        total = total + all_ref[k - 1]
    for copy in late_copies:
        copy.wait()
    joint = late[0:1, :] + late[1:2, :]
    for k in range(1, count):
        joint = joint + jnp.where(k <= me, lates_ref[k - 1, 0:1, :], lates_ref[k - 1, 1:2, :])
    gamma0, kappa, mu, part = (total[i:i + 1, :] for i in range(4))
    nu = 2.0 * (part - joint)
    a0 = gamma0 / kappa
    gamma1 = a0 * a0 * mu - gamma0
    beta = gamma1 / gamma0
    a1 = gamma1 / (kappa - 2.0 * a0 * mu + a0 * a0 * nu - beta * gamma1 / a0)
    first = a0 + a1 * (1.0 + beta)
    both = jnp.concatenate([first, a0 * a1, jnp.zeros((LANES - 2, LANES), F32)], 0).T
    coef_ref[...] = jnp.where(lane < LANES // 2, both[:pairs, 0:1], both[:pairs, 1:2])


def combine_kernel(coef_ref, r0_ref, q_ref, w_ref, z_ref, y_ref, sol_hbm, res_hbm, sol_ref, res_ref, sem):
    pairs, rows, cols = sol_ref.shape
    block = 8

    def out(i, src, dst, k):
        cut = pl.ds(pl.multiple_of(i * block, block), block)
        return pltpu.make_async_copy(src.at[cut], dst.at[cut], sem.at[k, i])

    def body(i, carry):
        cut = pl.ds(pl.multiple_of(i * block, block), block)
        one = coef_ref[cut, 0:1]
        two = coef_ref[cut, LANES - 1:LANES]
        for r in range(rows):
            sol_ref[cut, r, :] = one * q_ref[r, cut, :] - two * z_ref[r, cut, :]
            res_ref[cut, r, :] = r0_ref[r, cut, :] - one * w_ref[r, cut, :] + two * y_ref[r, cut, :]
        out(i, sol_ref, sol_hbm, 0).start()
        out(i, res_ref, res_hbm, 1).start()
        return carry

    lax.fori_loop(0, pairs // block, body, 0)

    def finish(i, carry):
        out(i, sol_ref, sol_hbm, 0).wait()
        out(i, res_ref, res_hbm, 1).wait()
        return carry

    lax.fori_loop(0, pairs // block, finish, 0)


def on_device(count, cond, nodata, gmask, gval, smask, scur, tinv, focal):
    rows, cols = cond.shape
    pairs = focal.shape[0]
    tiles = cols // LANES
    ext = pairs + EXTRA
    field = jax.ShapeDtypeStruct((rows, ext, cols), F32)
    vm = pl.BlockSpec(memory_space=pltpu.VMEM)
    hbm = pl.BlockSpec(memory_space=pltpu.HBM)
    msg = (2, 2 * pairs, LANES)
    bmsg = (2, 3 * tiles, LANES)
    tmsg = (2, 2 * tiles, LANES)
    zmsg = (2, 2 * pairs + tiles, LANES)
    others = count - 1
    small = (rows, cols)
    r0, q, w, z, y, coef = pl.pallas_call(
        functools.partial(krylov_kernel, count),
        out_shape=[field] * 5 + [jax.ShapeDtypeStruct((pairs, LANES), F32)],
        in_specs=[hbm] * 8,
        out_specs=[vm] * 6,
        scratch_shapes=[
            pltpu.VMEM(small, F32),
            pltpu.VMEM(small, jnp.int32),
            pltpu.VMEM(small, jnp.int32),
            pltpu.VMEM(small, F32),
            pltpu.VMEM(small, jnp.int32),
            pltpu.VMEM(small, F32),
            pltpu.VMEM((2, pairs), jnp.int32),
            pltpu.SMEM((2, pairs), jnp.int32),
            pltpu.VMEM((2 * cols, LANES), F32),
            pltpu.VMEM(((rows - 2) * cols, LANES), F32),
            pltpu.VMEM((rows, tiles, LANES, 2 * LANES), BF16),
            pltpu.VMEM((rows, 8, cols), F32),
            pltpu.VMEM((2, pairs, LANES), F32),
            pltpu.VMEM((2, pairs, cols), F32),
            pltpu.VMEM((2, pairs, cols), F32),
            *[pltpu.VMEM(shape, F32) for shape in (msg, bmsg, tmsg, zmsg) for _ in range(2)],
            pltpu.VMEM((4, pairs, LANES), F32),
            *[pltpu.VMEM(shape, F32) for _ in range(2) for shape in ((8, LANES), (others, 8, LANES))],
            *[pltpu.SemaphoreType.DMA((2,))] * 8,
            *[pltpu.SemaphoreType.DMA((others,))] * 4,
            pltpu.SemaphoreType.DMA((10,)),
            pltpu.SemaphoreType.DMA((rows,)),
        ],
        compiler_params=pltpu.CompilerParams(
            collective_id=0, has_side_effects=True, vmem_limit_bytes=36 * 1024 * 1024
        ),
        name="krylov",
    )(*(
        pltpu.with_memory_space_constraint(x, pltpu.HBM)
        for x in (cond, nodata, gmask, gval, smask, scur, tinv.reshape(rows, cols, LANES), focal.T)
    ))

    out = jax.ShapeDtypeStruct((pairs, rows, cols), F32)
    return tuple(pl.pallas_call(
        combine_kernel,
        out_shape=[out, out],
        in_specs=[vm] * 6,
        out_specs=[hbm, hbm],
        scratch_shapes=[
            pltpu.VMEM(out.shape, F32),
            pltpu.VMEM(out.shape, F32),
            pltpu.SemaphoreType.DMA((2, pairs // 8)),
        ],
        compiler_params=pltpu.CompilerParams(vmem_limit_bytes=20 * 1024 * 1024),
        name="combine",
    )(coef, r0, q, w, z, y))


def solution(mesh):
    return jax.shard_map(
        functools.partial(on_device, mesh.shape["space"]),
        mesh=mesh,
        in_specs=(
            P(("groups", "space"), None),
            P(("groups", "space"), None),
            P(("groups", "space"), None),
            P(("groups", "space"), None),
            P(("groups", "space"), None),
            P(("groups", "space"), None),
            P(("groups", "space"), None, None, None),
            P(("groups", "rhs"), None),
        ),
        out_specs=(P("rhs", ("groups", "space"), None), P("rhs", ("groups", "space"), None)),
        check_vma=False,
    )
```

```python
import functools

import jax
import jax.numpy as jnp
from jax import lax
from jax.experimental import pallas as pl
from jax.experimental.pallas import tpu as pltpu
from jax.sharding import PartitionSpec as P

LEAKAGE = 0.05
FOCAL_CURRENT = 16.0
LANES = 128
EXTRA = 8
F32 = jnp.float32
BF16 = jnp.bfloat16


def krylov_kernel(
    count, cond_hbm, nodata_hbm, gmask_hbm, gval_hbm, smask_hbm, scur_hbm, t_hbm, focal_hbm,
    r0_ref, q_ref, w_ref, z_ref, y_ref, coef_ref,
    cond_ref, nodata_ref, gmask_ref, gval_ref, smask_ref, scur_ref, focal_ref, ids_ref, te_ref, ti_ref,
    thl_ref, wts_ref, spot_ref, qhalo_ref, zhalo_ref, msg_ref, got_ref, bmsg_ref, bgot_ref, tmsg_ref, tgot_ref,
    zmsg_ref, zgot_ref, acc_ref, stat_ref, all_ref, late_ref, lates_ref,
    send1, recv1, sendb, recvb, sendt, recvt, send2, recv2, send3, recv3, send4, recv4, sem_in, sem_t,
):
    rows, cols = cond_ref.shape
    tiles = cols // LANES
    pairs = focal_ref.shape[1]
    ext = pairs + EXTRA
    me = lax.axis_index("space")
    last = count - 1
    ends = ((0, 0), (1, rows - 1))
    inner = range(1, rows - 1)
    cuts = [slice(c * LANES, (c + 1) * LANES) for c in range(tiles)]

    barrier = pltpu.get_barrier_semaphore()
    for off in range(1, count):
        pl.semaphore_signal(
            barrier, inc=1, device_id={"space": lax.rem(me + off, count)},
            device_id_type=pl.DeviceIdType.MESH,
        )

    loads = [
        pltpu.make_async_copy(src, dst, sem_in.at[i])
        for i, (src, dst) in enumerate((
            (focal_hbm, ids_ref), (focal_hbm, focal_ref), (t_hbm.at[0], te_ref.at[pl.ds(0, cols)]),
            (t_hbm.at[rows - 1], te_ref.at[pl.ds(cols, cols)]), (smask_hbm, smask_ref), (scur_hbm, scur_ref),
            (cond_hbm, cond_ref), (nodata_hbm, nodata_ref), (gmask_hbm, gmask_ref), (gval_hbm, gval_ref),
        ))
    ]
    t_loads = [
        pltpu.make_async_copy(t_hbm.at[r], ti_ref.at[pl.ds((r - 1) * cols, cols)], sem_t.at[r]) for r in inner
    ]
    for load in loads:
        load.start()
    loads[0].wait()
    for load in t_loads:
        load.start()
    for load in loads[1:]:
        load.wait()

    def gather(src, at):
        for p in range(pairs):
            for i in range(2):
                spot_ref[i, p:p + 1, :] = src[pl.ds(at(ids_ref[i, p]), 1), :]
        return FOCAL_CURRENT * spot_ref[0], -FOCAL_CURRENT * spot_ref[1]

    half = (rows * cols // 2).bit_length() - 1
    near_a, near_b = gather(
        te_ref, lambda i: (i & (cols - 1)) + (lax.shift_right_logical(i, half) & 1) * cols)

    diagonal = lax.broadcasted_iota(jnp.int32, (pairs, pairs), 0) == lax.broadcasted_iota(
        jnp.int32, (pairs, pairs), 1)
    lane = lax.broadcasted_iota(jnp.int32, (pairs, LANES), 1)

    def column(i):
        line = jnp.broadcast_to(focal_ref[i:i + 1, :].astype(F32), (pairs, pairs))
        return jnp.broadcast_to(
            jnp.sum(jnp.where(diagonal, line, 0.0), 1, keepdims=True).astype(jnp.int32), (pairs, LANES))

    at_a, at_b = (column(i) - me * (rows * cols) for i in range(2))
    spot_a, spot_b = (lax.shift_right_arithmetic(x, 7) for x in (at_a, at_b))
    tile_a, tile_b = spot_a & (tiles - 1), spot_b & (tiles - 1)

    def within(spot, low, high):
        return jnp.logical_and(spot >= low * tiles, spot < high * tiles)

    for side, r in ends:
        msg_ref[side, 0:pairs, :] = jnp.where(within(spot_a, r, r + 1), near_a, 0.0)
        msg_ref[side, pairs:2 * pairs, :] = jnp.where(within(spot_b, r, r + 1), near_b, 0.0)

    def side_copy(src, dst, ssem, rsem, side):
        return pltpu.make_async_remote_copy(
            src_ref=src.at[side], dst_ref=dst.at[1 - side],
            send_sem=ssem.at[side], recv_sem=rsem.at[1 - side],
            device_id={"space": me - 1 if side == 0 else me + 1},
            device_id_type=pl.DeviceIdType.MESH,
        )

    has = (me > 0, me < last)

    def send(src, dst, ssem, rsem):
        for side in range(2):
            @pl.when(has[side])
            def _():
                side_copy(src, dst, ssem, rsem, side).start()

            @pl.when(jnp.logical_not(has[side]))
            def _():
                dst[side] = jnp.zeros(dst.shape[1:], F32)

    def done(src, dst, ssem, rsem):
        for side in range(2):
            @pl.when(has[side])
            def _():
                side_copy(src, dst, ssem, rsem, side).wait_send()
                pltpu.make_async_remote_copy(
                    src_ref=src.at[1 - side], dst_ref=dst.at[side],
                    send_sem=ssem.at[1 - side], recv_sem=rsem.at[side],
                    device_id={"space": me - 1 if side == 0 else me + 1},
                    device_id_type=pl.DeviceIdType.MESH,
                ).wait_recv()

    pl.semaphore_wait(barrier, last)
    send(msg_ref, got_ref, send1, recv1)

    valid = (1 - nodata_ref[...]).astype(F32)
    active = cond_ref[...] * valid
    background = smask_ref[...].astype(F32) * scur_ref[...]

    def tile_of(r, c):
        if r == 0 or r == rows - 1:
            return te_ref[pl.ds((cols if r else 0) + c * LANES, LANES), :]
        return ti_ref[pl.ds((r - 1) * cols + c * LANES, LANES), :]

    def product(x, r, c):
        number = x.shape[0]
        hi = x.astype(BF16).astype(F32)
        lhs = jnp.concatenate([hi, x - hi], 0).astype(BF16)
        o = jnp.dot(lhs, thl_ref[r, c], preferred_element_type=F32)
        return o[:number, :LANES] + (o[:number, LANES:] + (o[number:, :LANES] + o[number:, LANES:]))

    def shared_row(r):
        dot = jnp.zeros((EXTRA, LANES), F32)
        for c, cut in enumerate(cuts):
            t = tile_of(r, c)
            thi = t.astype(BF16)
            thl_ref[r, c, :, :LANES] = thi
            thl_ref[r, c, :, LANES:] = (t - thi.astype(F32)).astype(BF16)
            x = jnp.broadcast_to(background[r:r + 1, cut], (EXTRA, LANES))
            q = product(x, r, c)
            q_ref[r, pairs:ext, cut] = q
            dot = dot + x * q
        return dot

    shared = shared_row(0) + shared_row(rows - 1)
    for side, r in ends:
        for c, cut in enumerate(cuts):
            bmsg_ref[side, c:c + 1, :] = q_ref[r, pairs:pairs + 1, cut]
            bmsg_ref[side, tiles + c:tiles + c + 1, :] = active[r:r + 1, cut]
            bmsg_ref[side, 2 * tiles + c:2 * tiles + c + 1, :] = valid[r:r + 1, cut]
            first = r and cols
            tmsg_ref[side, c:c + 1, :] = te_ref[first + c * LANES:first + c * LANES + 1, :]
            tmsg_ref[side, tiles + c:tiles + c + 1, :] = te_ref[
                first + c * LANES + LANES - 1:first + (c + 1) * LANES, :]
    send(bmsg_ref, bgot_ref, sendb, recvb)
    send(tmsg_ref, tgot_ref, sendt, recvt)

    def edge(a, b, v, u):
        return 0.5 * (a + b) * v * u

    row_at = lax.broadcasted_iota(jnp.int32, (rows, cols), 0)
    col_at = lax.broadcasted_iota(jnp.int32, (rows, cols), 1)

    def shifted(x, by, axis):
        length = x.shape[axis]
        at = (row_at, col_at)[axis][:x.shape[0], :]
        return jnp.where(at == (0 if by == 1 else length - 1), 0.0, pltpu.roll(x, by % length, axis))

    nw, sw, ww, ew = (
        edge(active, shifted(active, *how), valid, shifted(valid, *how))
        for how in ((1, 0), (-1, 0), (1, 1), (-1, 1))
    )
    dg = valid * (LEAKAGE + gmask_ref[...].astype(F32) * gval_ref[...]) + (1.0 - valid) + nw + sw + ww + ew
    for r in range(rows):
        for i, x in enumerate((dg, nw, sw, ww, ew, 0.5 * dg, background)):
            wts_ref[r, i:i + 1, :] = x[r:r + 1, :]

    for load in t_loads:
        load.wait()
    far_a, far_b = gather(
        ti_ref, lambda i: jnp.clip((i & (rows * cols - 1)) - cols, 0, (rows - 2) * cols - 1))
    for r in inner:
        shared = shared + shared_row(r)

    def dense_row(r, a, b, dot):
        for c, cut in enumerate(cuts):
            k = r * tiles + c
            x = jnp.where(spot_a == k, a, 0.0) + jnp.where(spot_b == k, b, 0.0)
            q_ref[r, 0:pairs, cut] = q_ref[r, pairs:pairs + 1, cut] + x
            dot = dot + background[r:r + 1, cut] * x
        return dot

    dot = jnp.zeros((pairs, LANES), F32)
    for r in range(rows):
        a, b = (far_a, far_b) if r in inner else (near_a, near_b)
        dot = dense_row(r, a, b, dot)
    in_a, in_b = (
        jnp.where(within(spot, 1, rows - 1), far, jnp.where(within(spot, 0, rows), near, 0.0))
        for spot, far, near in ((spot_a, far_a, near_a), (spot_b, far_b, near_b))
    )
    same = spot_a == spot_b
    own = jnp.where(lane == (at_a & (LANES - 1)), in_a + jnp.where(same, in_b, 0.0), 0.0) - jnp.where(
        lane == (at_b & (LANES - 1)), in_b + jnp.where(same, in_a, 0.0), 0.0)
    acc_ref[0] = 2.0 * dot + FOCAL_CURRENT * own + jnp.broadcast_to(shared[0:1, :], dot.shape)
    for i in range(1, 4):
        acc_ref[i] = jnp.zeros(acc_ref.shape[1:], F32)

    parts = [slice(p, p + pairs // 2) for p in (0, pairs // 2)]
    extra = slice(pairs, ext)

    def sides(xs):
        at = lane[:xs[0].shape[0]]
        west = [pltpu.roll(x, 1, 1) for x in xs]
        east = [pltpu.roll(x, LANES - 1, 1) for x in xs]
        west = west[:1] + [jnp.where(at == 0, west[c - 1], west[c]) for c in range(1, tiles)]
        east = [jnp.where(at == LANES - 1, east[c + 1], east[c]) for c in range(tiles - 1)] + east[-1:]
        return west, east

    def apply_part(src, dst, r, s, north, south, acc=None):
        xs = [src[r, s, cut] for cut in cuts]
        west, east = sides(xs)
        dots = None
        for c, cut in enumerate(cuts):
            out = (
                wts_ref[r, 0:1, cut] * xs[c] - wts_ref[r, 3:4, cut] * west[c] - wts_ref[r, 4:5, cut] * east[c]
            )
            if north is not None:
                out = out - wts_ref[r, 1:2, cut] * north[0][north[1], s, cut]
            if south is not None:
                out = out - wts_ref[r, 2:3, cut] * south[0][south[1], s, cut]
            dst[r, s, cut] = out
            dots = xs[c] * out if dots is None else dots + xs[c] * out
        if acc is not None:
            acc_ref[acc, s, :] += dots

    def apply_inner(src, dst, both, acc=None):
        def body(r, carry):
            for s in parts:
                apply_part(src, dst, r, s, (src, r - 1), (src, r + 1), acc)
            if both:
                apply_part(src, dst, r, extra, (src, r - 1), (src, r + 1))
            return carry
        lax.fori_loop(1, rows - 1, body, 0)

    apply_inner(q_ref, w_ref, True, 1)
    for s in (*parts, extra):
        apply_part(q_ref, w_ref, 0, s, None, (q_ref, 1))
        apply_part(q_ref, w_ref, rows - 1, s, (q_ref, rows - 2), None)

    done(msg_ref, got_ref, send1, recv1)
    done(bmsg_ref, bgot_ref, sendb, recvb)

    def row_of(side, base):
        return jnp.concatenate([bgot_ref[side, base + c:base + c + 1, :] for c in range(tiles)], 1)

    halo_a = [row_of(side, tiles) for side in range(2)]
    halo_v = [row_of(side, 2 * tiles) for side in range(2)]
    for side, r in ends:
        i = 1 + side
        h = edge(active[r:r + 1, :], halo_a[side], valid[r:r + 1, :], halo_v[side])
        wts_ref[r, i:i + 1, :] = h
        wts_ref[r, 0:1, :] += h
        wts_ref[r, 5:6, :] += 0.5 * h
        va = got_ref[side, 0:pairs, :]
        vb = got_ref[side, pairs:2 * pairs, :]
        dots = jnp.zeros((pairs, LANES), F32)
        for c, cut in enumerate(cuts):
            common = bgot_ref[side, c:c + 1, :]
            qh = jnp.where(tile_a == c, va, 0.0) + jnp.where(tile_b == c, vb, 0.0)
            qhalo_ref[side, :, cut] = qh
            q0 = q_ref[r, :pairs, cut]
            w0 = w_ref[r, :pairs, cut] + h[:, cut] * (q0 - (qh + common))
            w_ref[r, :pairs, cut] = w0
            w_ref[r, extra, cut] += h[:, cut] * (q_ref[r, extra, cut] - common)
            dots = dots + q0 * w0
        acc_ref[1] += dots

    def precond_row(r):
        for c, cut in enumerate(cuts):
            z_ref[r, :, cut] = product(w_ref[r, :, cut], r, c)

    def pack(src, r, dst, side):
        va = src[r, :pairs, 0:LANES]
        vb = va
        for c in range(1, tiles):
            x = src[r, :pairs, cuts[c]]
            va = jnp.where(tile_a == c, x, va)
            vb = jnp.where(tile_b == c, x, vb)
        dst[side, 0:pairs, :] = va
        dst[side, pairs:2 * pairs, :] = vb
        for c, cut in enumerate(cuts):
            dst[side, 2 * pairs + c:2 * pairs + c + 1, :] = src[r, pairs:pairs + 1, cut]

    precond_row(0)
    precond_row(rows - 1)
    for side, r in ends:
        pack(z_ref, r, zmsg_ref, side)
    send(zmsg_ref, zgot_ref, send2, recv2)

    for r in inner:
        precond_row(r)

    def moment_part(r, s, north):
        zs = [z_ref[r, s, cut] for cut in cuts]
        west, _ = sides(zs)
        mu = nu = None
        for c, cut in enumerate(cuts):
            t = wts_ref[r, 5:6, cut] * zs[c] - wts_ref[r, 3:4, cut] * west[c]
            if north:
                t = t - wts_ref[r, 1:2, cut] * z_ref[r - 1, s, cut]
            one, two = w_ref[r, s, cut] * zs[c], t * zs[c]
            mu, nu = (one, two) if mu is None else (mu + one, nu + two)
        acc_ref[2, s, :] += mu
        acc_ref[3, s, :] += nu

    def moments(r, carry):
        for s in parts:
            moment_part(r, s, True)
        return carry

    for s in parts:
        moment_part(0, s, False)
    lax.fori_loop(1, rows, moments, 0)

    square = lax.broadcasted_iota(jnp.int32, (LANES, LANES), 1)
    pad = jnp.zeros((LANES - pairs, 1), F32)

    def lines(sums):
        table = jnp.zeros((LANES, LANES), F32)
        for i, x in enumerate(sums):
            col = jnp.concatenate([jnp.sum(x, 1, keepdims=True), pad], 0)
            table = jnp.where(square == i, jnp.broadcast_to(col, table.shape), table)
        return table.T[0:8, :]

    def exchange(src, dst, ssem, rsem):
        return [
            pltpu.make_async_remote_copy(
                src_ref=src, dst_ref=dst.at[k - 1],
                send_sem=ssem.at[k - 1], recv_sem=rsem.at[k - 1],
                device_id={"space": lax.rem(me + k, count)}, device_id_type=pl.DeviceIdType.MESH,
            )
            for k in range(1, count)
        ]

    early = lines([acc_ref[i] for i in range(4)])
    stat_ref[...] = early
    early_copies = exchange(stat_ref, all_ref, send3, recv3)
    for copy in early_copies:
        copy.start()

    done(tmsg_ref, tgot_ref, sendt, recvt)
    for side in range(2):
        halo_w, halo_e = (
            edge(halo_a[side], shifted(halo_a[side], by, 1), halo_v[side], shifted(halo_v[side], by, 1))
            for by in (1, -1)
        )
        near = [jnp.zeros((pairs, LANES), F32)] * tiles
        for c, cut in enumerate(cuts):
            qh = qhalo_ref[side, :, cut]
            if c > 0:
                gone = (halo_w[:, cut] * qh)[:, 0:1]
                near[c - 1] = near[c - 1] - gone * tgot_ref[side, tiles + c - 1:tiles + c, :]
            if c < tiles - 1:
                gone = (halo_e[:, cut] * qh)[:, LANES - 1:LANES]
                near[c + 1] = near[c + 1] - gone * tgot_ref[side, c + 1:c + 2, :]
        for c, cut in enumerate(cuts):
            zhalo_ref[side, :, cut] = near[c]

    done(zmsg_ref, zgot_ref, send2, recv2)
    coupling = []
    for side, r in ends:
        va = zgot_ref[side, 0:pairs, :]
        vb = zgot_ref[side, pairs:2 * pairs, :]
        total = jnp.zeros((pairs, LANES), F32)
        for c, cut in enumerate(cuts):
            other = zgot_ref[side, 2 * pairs + c:2 * pairs + c + 1, :] + zhalo_ref[side, :, cut]
            zh = jnp.where(tile_a == c, va, jnp.where(tile_b == c, vb, other))
            zhalo_ref[side, :, cut] = zh
            total = total + wts_ref[r, 1 + side:2 + side, cut] * z_ref[r, :pairs, cut] * zh
        coupling.append(total)
    late = lines(coupling)
    late_ref[...] = late
    late_copies = exchange(late_ref, lates_ref, send4, recv4)
    for copy in late_copies:
        copy.start()

    apply_inner(z_ref, y_ref, False)
    for s in parts:
        apply_part(z_ref, y_ref, 0, s, (zhalo_ref, 0), (z_ref, 1))
        apply_part(z_ref, y_ref, rows - 1, s, (z_ref, rows - 2), (zhalo_ref, 1))

    def right_side(r, carry):
        for c, cut in enumerate(cuts):
            local = r * cols + c * LANES + lane
            x = jnp.where(local == at_a, FOCAL_CURRENT, 0.0) - jnp.where(local == at_b, FOCAL_CURRENT, 0.0)
            r0_ref[r, 0:pairs, cut] = wts_ref[r, 6:7, cut] + x
        return carry

    lax.fori_loop(0, rows, right_side, 0)

    for copy in early_copies:
        copy.wait()
    total = early
    for k in range(1, count):
        total = total + all_ref[k - 1]
    gamma0, kappa, mu, part = (total[i:i + 1, :] for i in range(4))
    a0 = gamma0 / kappa
    gamma1 = a0 * a0 * mu - gamma0
    beta = gamma1 / gamma0
    known = kappa - 2.0 * a0 * mu - beta * gamma1 / a0 + 2.0 * a0 * a0 * part
    scale = 2.0 * a0 * a0
    joint = late[0:1, :] + late[1:2, :]
    for copy in late_copies:
        copy.wait()
    for k in range(1, count):
        joint = joint + jnp.where(k <= me, lates_ref[k - 1, 0:1, :], lates_ref[k - 1, 1:2, :])
    a1 = gamma1 / (known - scale * joint)
    first = a0 + a1 * (1.0 + beta)
    both = jnp.concatenate([first, a0 * a1, jnp.zeros((6, LANES), F32)], 0).T
    for i in range(2):
        coef_ref[i] = jnp.broadcast_to(both[:pairs, i:i + 1], (pairs, LANES))


def combine_kernel(coef_ref, r0_ref, q_ref, w_ref, z_ref, y_ref, sol_hbm, res_hbm, sol_ref, res_ref, sem):
    rows, pairs, cols = sol_ref.shape
    mine = pl.ds(0, pairs)

    def out(r, src, dst, k):
        return pltpu.make_async_copy(src.at[r], dst.at[mine, r], sem.at[k, r])

    def body(r, carry):
        one, two = coef_ref[0], coef_ref[1]
        for c in range(cols // LANES):
            cut = slice(c * LANES, (c + 1) * LANES)
            sol_ref[r, :, cut] = one * q_ref[r, mine, cut] - two * z_ref[r, mine, cut]
            res_ref[r, :, cut] = r0_ref[r, mine, cut] - one * w_ref[r, mine, cut] + two * y_ref[r, mine, cut]
        out(r, sol_ref, sol_hbm, 0).start()
        out(r, res_ref, res_hbm, 1).start()
        return carry

    lax.fori_loop(0, rows, body, 0)

    def finish(r, carry):
        out(r, sol_ref, sol_hbm, 0).wait()
        out(r, res_ref, res_hbm, 1).wait()
        return carry

    lax.fori_loop(0, rows, finish, 0)


def on_device(count, cond, nodata, gmask, gval, smask, scur, tinv, focal):
    rows, cols = cond.shape
    pairs = focal.shape[0]
    tiles = cols // LANES
    ext = pairs + EXTRA
    field = jax.ShapeDtypeStruct((rows, ext, cols), F32)
    vm = pl.BlockSpec(memory_space=pltpu.VMEM)
    hbm = pl.BlockSpec(memory_space=pltpu.HBM)
    msg = (2, 2 * pairs, LANES)
    bmsg = (2, 3 * tiles, LANES)
    tmsg = (2, 2 * tiles, LANES)
    zmsg = (2, 2 * pairs + tiles, LANES)
    others = count - 1
    small = (rows, cols)
    r0, q, w, z, y, coef = pl.pallas_call(
        functools.partial(krylov_kernel, count),
        out_shape=[field] * 5 + [jax.ShapeDtypeStruct((2, pairs, LANES), F32)],
        in_specs=[hbm] * 8,
        out_specs=[vm] * 6,
        scratch_shapes=[
            pltpu.VMEM(small, F32),
            pltpu.VMEM(small, jnp.int32),
            pltpu.VMEM(small, jnp.int32),
            pltpu.VMEM(small, F32),
            pltpu.VMEM(small, jnp.int32),
            pltpu.VMEM(small, F32),
            pltpu.VMEM((2, pairs), jnp.int32),
            pltpu.SMEM((2, pairs), jnp.int32),
            pltpu.VMEM((2 * cols, LANES), F32),
            pltpu.VMEM(((rows - 2) * cols, LANES), F32),
            pltpu.VMEM((rows, tiles, LANES, 2 * LANES), BF16),
            pltpu.VMEM((rows, 8, cols), F32),
            pltpu.VMEM((2, pairs, LANES), F32),
            pltpu.VMEM((2, pairs, cols), F32),
            pltpu.VMEM((2, pairs, cols), F32),
            *[pltpu.VMEM(shape, F32) for shape in (msg, bmsg, tmsg, zmsg) for _ in range(2)],
            pltpu.VMEM((4, pairs, LANES), F32),
            *[pltpu.VMEM(shape, F32) for _ in range(2) for shape in ((8, LANES), (others, 8, LANES))],
            *[pltpu.SemaphoreType.DMA((2,))] * 8,
            *[pltpu.SemaphoreType.DMA((others,))] * 4,
            pltpu.SemaphoreType.DMA((10,)),
            pltpu.SemaphoreType.DMA((rows,)),
        ],
        compiler_params=pltpu.CompilerParams(
            collective_id=0, has_side_effects=True, vmem_limit_bytes=36 * 1024 * 1024
        ),
        name="krylov",
    )(*(
        pltpu.with_memory_space_constraint(x, pltpu.HBM)
        for x in (cond, nodata, gmask, gval, smask, scur, tinv.reshape(rows, cols, LANES), focal.T)
    ))

    out = jax.ShapeDtypeStruct((pairs, rows, cols), F32)
    return tuple(pl.pallas_call(
        combine_kernel,
        out_shape=[out, out],
        in_specs=[vm] * 6,
        out_specs=[hbm, hbm],
        scratch_shapes=[
            pltpu.VMEM((rows, pairs, cols), F32),
            pltpu.VMEM((rows, pairs, cols), F32),
            pltpu.SemaphoreType.DMA((2, rows)),
        ],
        compiler_params=pltpu.CompilerParams(vmem_limit_bytes=20 * 1024 * 1024),
        name="combine",
    )(coef, r0, q, w, z, y))


def solution(mesh):
    return jax.shard_map(
        functools.partial(on_device, mesh.shape["space"]),
        mesh=mesh,
        in_specs=(
            P(("groups", "space"), None),
            P(("groups", "space"), None),
            P(("groups", "space"), None),
            P(("groups", "space"), None),
            P(("groups", "space"), None),
            P(("groups", "space"), None),
            P(("groups", "space"), None, None, None),
            P(("groups", "rhs"), None),
        ),
        out_specs=(P("rhs", ("groups", "space"), None), P("rhs", ("groups", "space"), None)),
        check_vma=False,
    )
```

```python
import functools

import jax
import jax.numpy as jnp
from jax import lax
from jax.experimental import pallas as pl
from jax.experimental.pallas import tpu as pltpu
from jax.sharding import PartitionSpec as P

LEAKAGE = 0.05
FOCAL_CURRENT = 16.0
LANES = 128
EXTRA = 8
F32 = jnp.float32
BF16 = jnp.bfloat16


def krylov_kernel(
    count, cond_hbm, nodata_hbm, gmask_hbm, gval_hbm, smask_hbm, scur_hbm, t_hbm, focal_hbm,
    r0_ref, q_ref, w_ref, z_ref, y_ref, coef_ref,
    reals_ref, flags_ref, focal_ref, ids_ref, te_ref, ti_ref,
    thl_ref, wts_ref, spot_ref, qhalo_ref, zhalo_ref, msg_ref, got_ref, bmsg_ref, bgot_ref, tmsg_ref, tgot_ref,
    zmsg_ref, zgot_ref, acc_ref, stat_ref, all_ref, late_ref, lates_ref,
    send1, recv1, sendb, recvb, sendt, recvt, send2, recv2, send3, recv3, send4, recv4, sem_in,
):
    rows, cols = reals_ref.shape[1:]
    tiles = cols // LANES
    pairs = focal_ref.shape[1]
    ext = pairs + EXTRA
    me = lax.axis_index("space")
    last = count - 1
    ends = ((0, 0), (1, rows - 1))
    inner = range(1, rows - 1)
    cuts = [slice(c * LANES, (c + 1) * LANES) for c in range(tiles)]

    barrier = pltpu.get_barrier_semaphore()
    for off in range(1, count):
        pl.semaphore_signal(
            barrier, inc=1, device_id={"space": lax.rem(me + off, count)},
            device_id_type=pl.DeviceIdType.MESH,
        )

    def whole(ref, i):
        return pltpu.make_async_copy(ref, ref, sem_in.at[i])

    ids_load = pltpu.make_async_copy(focal_hbm, ids_ref, sem_in.at[0])
    focal_load = pltpu.make_async_copy(focal_hbm, focal_ref, sem_in.at[1])
    inner_load = pltpu.make_async_copy(t_hbm.at[pl.ds(1, rows - 2)], ti_ref, sem_in.at[5])
    ids_load.start()
    focal_load.start()
    for side, r in ends:
        for cut in cuts:
            pltpu.make_async_copy(
                t_hbm.at[r, pl.ds(cut.start, LANES)], te_ref.at[side, pl.ds(cut.start, LANES)], sem_in.at[2]).start()
    for i, group in ((3, (cond_hbm, gval_hbm, scur_hbm)), (4, (nodata_hbm, gmask_hbm, smask_hbm))):
        for k, src in enumerate(group):
            pltpu.make_async_copy(src, (reals_ref, flags_ref)[i - 3].at[k], sem_in.at[i]).start()
    inner_load.start()
    ids_load.wait()
    focal_load.wait()
    whole(te_ref, 2).wait()

    def gather(src, at):
        for p in range(pairs):
            for i in range(2):
                r, k = at(ids_ref[i, p])
                spot_ref[i, p:p + 1, :] = src[r, pl.ds(k, 1), :]
        return FOCAL_CURRENT * spot_ref[0], -FOCAL_CURRENT * spot_ref[1]

    half, high = (rows * cols // 2).bit_length() - 1, cols.bit_length() - 1
    near_a, near_b = gather(
        te_ref, lambda i: (lax.shift_right_logical(i, half) & 1, i & (cols - 1)))

    diagonal = lax.broadcasted_iota(jnp.int32, (pairs, pairs), 0) == lax.broadcasted_iota(
        jnp.int32, (pairs, pairs), 1)
    lane = lax.broadcasted_iota(jnp.int32, (pairs, LANES), 1)

    def column(i):
        line = jnp.broadcast_to(focal_ref[i:i + 1, :].astype(F32), (pairs, pairs))
        return jnp.broadcast_to(
            jnp.sum(jnp.where(diagonal, line, 0.0), 1, keepdims=True).astype(jnp.int32), (pairs, LANES))

    at_a, at_b = (column(i) - me * (rows * cols) for i in range(2))
    spot_a, spot_b = (lax.shift_right_arithmetic(x, 7) for x in (at_a, at_b))
    tile_a, tile_b = spot_a & (tiles - 1), spot_b & (tiles - 1)

    def within(spot, low, high):
        return jnp.logical_and(spot >= low * tiles, spot < high * tiles)

    for side, r in ends:
        msg_ref[side, 0:pairs, :] = jnp.where(within(spot_a, r, r + 1), near_a, 0.0)
        msg_ref[side, pairs:2 * pairs, :] = jnp.where(within(spot_b, r, r + 1), near_b, 0.0)

    def side_copy(src, dst, ssem, rsem, side):
        return pltpu.make_async_remote_copy(
            src_ref=src.at[side], dst_ref=dst.at[1 - side],
            send_sem=ssem.at[side], recv_sem=rsem.at[1 - side],
            device_id={"space": me - 1 if side == 0 else me + 1},
            device_id_type=pl.DeviceIdType.MESH,
        )

    has = (me > 0, me < last)

    def send(src, dst, ssem, rsem):
        for side in range(2):
            @pl.when(has[side])
            def _():
                side_copy(src, dst, ssem, rsem, side).start()

            @pl.when(jnp.logical_not(has[side]))
            def _():
                dst[side] = jnp.zeros(dst.shape[1:], F32)

    def done(src, dst, ssem, rsem):
        for side in range(2):
            @pl.when(has[side])
            def _():
                side_copy(src, dst, ssem, rsem, side).wait_send()
                pltpu.make_async_remote_copy(
                    src_ref=src.at[1 - side], dst_ref=dst.at[side],
                    send_sem=ssem.at[1 - side], recv_sem=rsem.at[side],
                    device_id={"space": me - 1 if side == 0 else me + 1},
                    device_id_type=pl.DeviceIdType.MESH,
                ).wait_recv()

    pl.semaphore_wait(barrier, last)
    send(msg_ref, got_ref, send1, recv1)

    whole(reals_ref, 3).wait()
    whole(flags_ref, 4).wait()
    valid = (1 - flags_ref[0]).astype(F32)
    active = reals_ref[0] * valid
    background = flags_ref[2].astype(F32) * reals_ref[2]

    def tile_of(r, c):
        if r == 0 or r == rows - 1:
            return te_ref[min(r, 1), cuts[c], :]
        return ti_ref[r - 1, cuts[c], :]

    def product(x, r, c):
        number = x.shape[0]
        hi = x.astype(BF16).astype(F32)
        lhs = jnp.concatenate([hi, x - hi], 0).astype(BF16)
        o = jnp.dot(lhs, thl_ref[r, c], preferred_element_type=F32)
        return o[:number, :LANES] + (o[:number, LANES:] + (o[number:, :LANES] + o[number:, LANES:]))

    def shared_row(r):
        dot = jnp.zeros((EXTRA, LANES), F32)
        for c, cut in enumerate(cuts):
            t = tile_of(r, c)
            thi = t.astype(BF16)
            thl_ref[r, c, :, :LANES] = thi
            thl_ref[r, c, :, LANES:] = (t - thi.astype(F32)).astype(BF16)
            x = jnp.broadcast_to(background[r:r + 1, cut], (EXTRA, LANES))
            q = product(x, r, c)
            q_ref[r, pairs:ext, cut] = q
            dot = dot + x * q
        return dot

    shared = shared_row(0) + shared_row(rows - 1)
    for side, r in ends:
        for c, cut in enumerate(cuts):
            bmsg_ref[side, c:c + 1, :] = q_ref[r, pairs:pairs + 1, cut]
            bmsg_ref[side, tiles + c:tiles + c + 1, :] = active[r:r + 1, cut]
            bmsg_ref[side, 2 * tiles + c:2 * tiles + c + 1, :] = valid[r:r + 1, cut]
            tmsg_ref[side, c:c + 1, :] = te_ref[side, cut.start:cut.start + 1, :]
            tmsg_ref[side, tiles + c:tiles + c + 1, :] = te_ref[side, cut.stop - 1:cut.stop, :]
    send(bmsg_ref, bgot_ref, sendb, recvb)
    send(tmsg_ref, tgot_ref, sendt, recvt)

    def edge(a, b, v, u):
        return 0.5 * (a + b) * v * u

    row_at = lax.broadcasted_iota(jnp.int32, (rows, cols), 0)
    col_at = lax.broadcasted_iota(jnp.int32, (rows, cols), 1)

    def shifted(x, by, axis):
        length = x.shape[axis]
        at = (row_at, col_at)[axis][:x.shape[0], :]
        return jnp.where(at == (0 if by == 1 else length - 1), 0.0, pltpu.roll(x, by % length, axis))

    nw, sw, ww, ew = (
        edge(active, shifted(active, *how), valid, shifted(valid, *how))
        for how in ((1, 0), (-1, 0), (1, 1), (-1, 1))
    )
    dg = valid * (LEAKAGE + flags_ref[1].astype(F32) * reals_ref[1]) + (1.0 - valid) + nw + sw + ww + ew
    for r in range(rows):
        for i, x in enumerate((dg, nw, sw, ww, ew, 0.5 * dg, background)):
            wts_ref[r, i:i + 1, :] = x[r:r + 1, :]

    inner_load.wait()
    far_a, far_b = gather(
        ti_ref, lambda i: (
            jnp.clip((lax.shift_right_logical(i, high) & (rows - 1)) - 1, 0, rows - 3), i & (cols - 1)))
    for r in inner:
        shared = shared + shared_row(r)

    def dense_row(r, a, b, dot):
        for c, cut in enumerate(cuts):
            k = r * tiles + c
            x = jnp.where(spot_a == k, a, 0.0) + jnp.where(spot_b == k, b, 0.0)
            q_ref[r, 0:pairs, cut] = q_ref[r, pairs:pairs + 1, cut] + x
            dot = dot + background[r:r + 1, cut] * x
        return dot

    dot = jnp.zeros((pairs, LANES), F32)
    for r in range(rows):
        a, b = (far_a, far_b) if r in inner else (near_a, near_b)
        dot = dense_row(r, a, b, dot)
    in_a, in_b = (
        jnp.where(within(spot, 1, rows - 1), far, jnp.where(within(spot, 0, rows), near, 0.0))
        for spot, far, near in ((spot_a, far_a, near_a), (spot_b, far_b, near_b))
    )
    same = spot_a == spot_b
    own = jnp.where(lane == (at_a & (LANES - 1)), in_a + jnp.where(same, in_b, 0.0), 0.0) - jnp.where(
        lane == (at_b & (LANES - 1)), in_b + jnp.where(same, in_a, 0.0), 0.0)
    acc_ref[0] = 2.0 * dot + FOCAL_CURRENT * own + jnp.broadcast_to(shared[0:1, :], dot.shape)
    for i in range(1, 4):
        acc_ref[i] = jnp.zeros(acc_ref.shape[1:], F32)

    parts = [slice(p, p + 16) for p in range(0, pairs, 16)]
    extra = slice(pairs, ext)

    def stream(src, r, s, east=True):
        at = lane[:s.stop - s.start]
        x = src[r, s, cuts[0]]
        gone, west, ahead = None, pltpu.roll(x, 1, 1), east and pltpu.roll(x, LANES - 1, 1)
        for c in range(tiles):
            more = c + 1 < tiles
            if more:
                y = src[r, s, cuts[c + 1]]
                after = east and pltpu.roll(y, LANES - 1, 1)
            yield (
                c, cuts[c], x, west if gone is None else jnp.where(at == 0, gone, west),
                jnp.where(at == LANES - 1, after, ahead) if east and more else ahead,
            )
            if more:
                x, gone, west, ahead = y, west, pltpu.roll(y, 1, 1), after

    def apply_part(src, dst, r, s, north, south, acc=None):
        dots = None
        for c, cut, x, west, east in stream(src, r, s):
            out = wts_ref[r, 0:1, cut] * x - wts_ref[r, 3:4, cut] * west - wts_ref[r, 4:5, cut] * east
            if north is not None:
                out = out - wts_ref[r, 1:2, cut] * north[0][north[1], s, cut]
            if south is not None:
                out = out - wts_ref[r, 2:3, cut] * south[0][south[1], s, cut]
            dst[r, s, cut] = out
            dots = x * out if dots is None else dots + x * out
        if acc is not None:
            acc_ref[acc, s, :] += dots

    def apply_inner(src, dst, both, acc=None):
        def body(r, carry):
            for s in parts:
                apply_part(src, dst, r, s, (src, r - 1), (src, r + 1), acc)
            if both:
                apply_part(src, dst, r, extra, (src, r - 1), (src, r + 1))
            return carry
        lax.fori_loop(1, rows - 1, body, 0)

    for s in (*parts, extra):
        apply_part(q_ref, w_ref, 0, s, None, (q_ref, 1))
        apply_part(q_ref, w_ref, rows - 1, s, (q_ref, rows - 2), None)

    done(msg_ref, got_ref, send1, recv1)
    done(bmsg_ref, bgot_ref, sendb, recvb)

    def row_of(side, base):
        return jnp.concatenate([bgot_ref[side, base + c:base + c + 1, :] for c in range(tiles)], 1)

    halo_a = [row_of(side, tiles) for side in range(2)]
    halo_v = [row_of(side, 2 * tiles) for side in range(2)]
    for side, r in ends:
        i = 1 + side
        h = edge(active[r:r + 1, :], halo_a[side], valid[r:r + 1, :], halo_v[side])
        wts_ref[r, i:i + 1, :] = h
        wts_ref[r, 0:1, :] += h
        wts_ref[r, 5:6, :] += 0.5 * h
        va = got_ref[side, 0:pairs, :]
        vb = got_ref[side, pairs:2 * pairs, :]
        dots = jnp.zeros((pairs, LANES), F32)
        for c, cut in enumerate(cuts):
            common = bgot_ref[side, c:c + 1, :]
            qh = jnp.where(tile_a == c, va, 0.0) + jnp.where(tile_b == c, vb, 0.0)
            qhalo_ref[side, :, cut] = qh
            q0 = q_ref[r, :pairs, cut]
            w0 = w_ref[r, :pairs, cut] + h[:, cut] * (q0 - (qh + common))
            w_ref[r, :pairs, cut] = w0
            w_ref[r, extra, cut] += h[:, cut] * (q_ref[r, extra, cut] - common)
            dots = dots + q0 * w0
        acc_ref[1] += dots

    def precond_row(r):
        for c, cut in enumerate(cuts):
            z_ref[r, :, cut] = product(w_ref[r, :, cut], r, c)

    def pack(src, r, dst, side):
        va = src[r, :pairs, 0:LANES]
        vb = va
        for c in range(1, tiles):
            x = src[r, :pairs, cuts[c]]
            va = jnp.where(tile_a == c, x, va)
            vb = jnp.where(tile_b == c, x, vb)
        dst[side, 0:pairs, :] = va
        dst[side, pairs:2 * pairs, :] = vb
        for c, cut in enumerate(cuts):
            dst[side, 2 * pairs + c:2 * pairs + c + 1, :] = src[r, pairs:pairs + 1, cut]

    precond_row(0)
    precond_row(rows - 1)
    for side, r in ends:
        pack(z_ref, r, zmsg_ref, side)
    send(zmsg_ref, zgot_ref, send2, recv2)

    apply_inner(q_ref, w_ref, True, 1)
    for r in inner:
        precond_row(r)

    def moment_part(r, s, north):
        mu = nu = None
        for c, cut, z, west, _ in stream(z_ref, r, s, False):
            t = wts_ref[r, 5:6, cut] * z - wts_ref[r, 3:4, cut] * west
            if north:
                t = t - wts_ref[r, 1:2, cut] * z_ref[r - 1, s, cut]
            one, two = w_ref[r, s, cut] * z, t * z
            mu, nu = (one, two) if mu is None else (mu + one, nu + two)
        acc_ref[2, s, :] += mu
        acc_ref[3, s, :] += nu

    def moments(r, carry):
        for s in parts:
            moment_part(r, s, True)
        return carry

    for s in parts:
        moment_part(0, s, False)
    lax.fori_loop(1, rows, moments, 0)

    pad = jnp.zeros((8, LANES - pairs), F32)

    def lines(sums):
        table = jnp.zeros((pairs, LANES), F32)
        for i, x in enumerate(sums):
            table = jnp.where(lane == i, jnp.sum(x, 1, keepdims=True), table)
        return jnp.concatenate([table.T[0:8, :], pad], 1)

    def exchange(src, dst, ssem, rsem):
        for k in range(1, count):
            pltpu.make_async_remote_copy(
                src_ref=src, dst_ref=dst.at[k - 1], send_sem=ssem, recv_sem=rsem,
                device_id={"space": lax.rem(me + k, count)}, device_id_type=pl.DeviceIdType.MESH,
            ).start()

    def arrived(dst, ssem, rsem):
        for sem in (ssem, rsem):
            pltpu.make_async_copy(dst, dst, sem).wait()

    early = lines([acc_ref[i] for i in range(4)])
    stat_ref[...] = early
    exchange(stat_ref, all_ref, send3, recv3)

    done(tmsg_ref, tgot_ref, sendt, recvt)
    for side in range(2):
        halo_w, halo_e = (
            edge(halo_a[side], shifted(halo_a[side], by, 1), halo_v[side], shifted(halo_v[side], by, 1))
            for by in (1, -1)
        )
        near = [jnp.zeros((pairs, LANES), F32)] * tiles
        for c, cut in enumerate(cuts):
            qh = qhalo_ref[side, :, cut]
            if c > 0:
                gone = (halo_w[:, cut] * qh)[:, 0:1]
                near[c - 1] = near[c - 1] - gone * tgot_ref[side, tiles + c - 1:tiles + c, :]
            if c < tiles - 1:
                gone = (halo_e[:, cut] * qh)[:, LANES - 1:LANES]
                near[c + 1] = near[c + 1] - gone * tgot_ref[side, c + 1:c + 2, :]
        for c, cut in enumerate(cuts):
            zhalo_ref[side, :, cut] = near[c]

    done(zmsg_ref, zgot_ref, send2, recv2)
    coupling = []
    for side, r in ends:
        va = zgot_ref[side, 0:pairs, :]
        vb = zgot_ref[side, pairs:2 * pairs, :]
        total = jnp.zeros((pairs, LANES), F32)
        for c, cut in enumerate(cuts):
            other = zgot_ref[side, 2 * pairs + c:2 * pairs + c + 1, :] + zhalo_ref[side, :, cut]
            zh = jnp.where(tile_a == c, va, jnp.where(tile_b == c, vb, other))
            zhalo_ref[side, :, cut] = zh
            total = total + wts_ref[r, 1 + side:2 + side, cut] * z_ref[r, :pairs, cut] * zh
        coupling.append(total)
    late = lines(coupling)
    late_ref[...] = late
    exchange(late_ref, lates_ref, send4, recv4)

    apply_inner(z_ref, y_ref, False)
    for s in parts:
        apply_part(z_ref, y_ref, 0, s, (zhalo_ref, 0), (z_ref, 1))
        apply_part(z_ref, y_ref, rows - 1, s, (z_ref, rows - 2), (zhalo_ref, 1))

    def right_side(r, carry):
        for c, cut in enumerate(cuts):
            local = r * cols + c * LANES + lane
            x = jnp.where(local == at_a, FOCAL_CURRENT, 0.0) - jnp.where(local == at_b, FOCAL_CURRENT, 0.0)
            r0_ref[r, 0:pairs, cut] = wts_ref[r, 6:7, cut] + x
        return carry

    lax.fori_loop(0, rows, right_side, 0)

    arrived(all_ref, send3, recv3)
    total = early
    for k in range(1, count):
        total = total + all_ref[k - 1]
    gamma0, kappa, mu, part = (total[i:i + 1, :] for i in range(4))
    a0 = gamma0 / kappa
    gamma1 = a0 * a0 * mu - gamma0
    beta = gamma1 / gamma0
    known = kappa - 2.0 * a0 * mu - beta * gamma1 / a0 + 2.0 * a0 * a0 * part
    scale = 2.0 * a0 * a0
    joint = late[0:1, :] + late[1:2, :]
    arrived(lates_ref, send4, recv4)
    for k in range(1, count):
        joint = joint + jnp.where(k <= me, lates_ref[k - 1, 0:1, :], lates_ref[k - 1, 1:2, :])
    a1 = gamma1 / (known - scale * joint)
    first = a0 + a1 * (1.0 + beta)
    both = jnp.concatenate([first, a0 * a1, jnp.zeros((6, LANES), F32)], 0).T
    for i in range(2):
        coef_ref[i] = jnp.broadcast_to(both[:pairs, i:i + 1], (pairs, LANES))


def combine_kernel(coef_ref, r0_ref, q_ref, w_ref, z_ref, y_ref, sol_hbm, res_hbm, sol_ref, res_ref, sem):
    rows, pairs, cols = sol_ref.shape
    mine = pl.ds(0, pairs)

    def out(r, src, dst, k):
        return pltpu.make_async_copy(src.at[r], dst.at[mine, r], sem.at[k, r])

    def body(r, carry):
        one, two = coef_ref[0], coef_ref[1]
        for c in range(cols // LANES):
            cut = slice(c * LANES, (c + 1) * LANES)
            sol_ref[r, :, cut] = one * q_ref[r, mine, cut] - two * z_ref[r, mine, cut]
            res_ref[r, :, cut] = r0_ref[r, mine, cut] - one * w_ref[r, mine, cut] + two * y_ref[r, mine, cut]
        out(r, sol_ref, sol_hbm, 0).start()
        out(r, res_ref, res_hbm, 1).start()
        return carry

    lax.fori_loop(0, rows, body, 0)

    def finish(r, carry):
        out(r, sol_ref, sol_hbm, 0).wait()
        out(r, res_ref, res_hbm, 1).wait()
        return carry

    lax.fori_loop(0, rows, finish, 0)


def on_device(count, cond, nodata, gmask, gval, smask, scur, tinv, focal):
    rows, cols = cond.shape
    pairs = focal.shape[0]
    tiles = cols // LANES
    ext = pairs + EXTRA
    field = jax.ShapeDtypeStruct((rows, ext, cols), F32)
    vm = pl.BlockSpec(memory_space=pltpu.VMEM)
    hbm = pl.BlockSpec(memory_space=pltpu.HBM)
    msg = (2, 2 * pairs, LANES)
    bmsg = (2, 3 * tiles, LANES)
    tmsg = (2, 2 * tiles, LANES)
    zmsg = (2, 2 * pairs + tiles, LANES)
    others = count - 1
    r0, q, w, z, y, coef = pl.pallas_call(
        functools.partial(krylov_kernel, count),
        out_shape=[field] * 5 + [jax.ShapeDtypeStruct((2, pairs, LANES), F32)],
        in_specs=[hbm] * 8,
        out_specs=[vm] * 6,
        scratch_shapes=[
            pltpu.VMEM((3, rows, cols), F32),
            pltpu.VMEM((3, rows, cols), jnp.int32),
            pltpu.VMEM((2, pairs), jnp.int32),
            pltpu.SMEM((2, pairs), jnp.int32),
            pltpu.VMEM((2, cols, LANES), F32),
            pltpu.VMEM((rows - 2, cols, LANES), F32),
            pltpu.VMEM((rows, tiles, LANES, 2 * LANES), BF16),
            pltpu.VMEM((rows, 8, cols), F32),
            pltpu.VMEM((2, pairs, LANES), F32),
            pltpu.VMEM((2, pairs, cols), F32),
            pltpu.VMEM((2, pairs, cols), F32),
            *[pltpu.VMEM(shape, F32) for shape in (msg, bmsg, tmsg, zmsg) for _ in range(2)],
            pltpu.VMEM((4, pairs, LANES), F32),
            *[pltpu.VMEM(shape, F32) for _ in range(2) for shape in ((8, LANES), (others, 8, LANES))],
            *[pltpu.SemaphoreType.DMA((2,))] * 8,
            *[pltpu.SemaphoreType.DMA] * 4,
            pltpu.SemaphoreType.DMA((6,)),
        ],
        compiler_params=pltpu.CompilerParams(
            collective_id=0, has_side_effects=True, vmem_limit_bytes=36 * 1024 * 1024
        ),
        name="krylov",
    )(*(
        pltpu.with_memory_space_constraint(x, pltpu.HBM)
        for x in (cond, nodata, gmask, gval, smask, scur, tinv.reshape(rows, cols, LANES), focal.T)
    ))

    out = jax.ShapeDtypeStruct((pairs, rows, cols), F32)
    return tuple(pl.pallas_call(
        combine_kernel,
        out_shape=[out, out],
        in_specs=[vm] * 6,
        out_specs=[hbm, hbm],
        scratch_shapes=[
            pltpu.VMEM((rows, pairs, cols), F32),
            pltpu.VMEM((rows, pairs, cols), F32),
            pltpu.SemaphoreType.DMA((2, rows)),
        ],
        compiler_params=pltpu.CompilerParams(vmem_limit_bytes=20 * 1024 * 1024),
        name="combine",
    )(coef, r0, q, w, z, y))


def solution(mesh):
    return jax.shard_map(
        functools.partial(on_device, mesh.shape["space"]),
        mesh=mesh,
        in_specs=(
            P(("groups", "space"), None),
            P(("groups", "space"), None),
            P(("groups", "space"), None),
            P(("groups", "space"), None),
            P(("groups", "space"), None),
            P(("groups", "space"), None),
            P(("groups", "space"), None, None, None),
            P(("groups", "rhs"), None),
        ),
        out_specs=(P("rhs", ("groups", "space"), None), P("rhs", ("groups", "space"), None)),
        check_vma=False,
    )
```

```python
import functools

import jax
import jax.numpy as jnp
from jax import lax
from jax.experimental import pallas as pl
from jax.experimental.pallas import tpu as pltpu
from jax.sharding import PartitionSpec as P

LEAKAGE = 0.05
FOCAL_CURRENT = 16.0
LANES = 128
EXTRA = 8
F32 = jnp.float32
BF16 = jnp.bfloat16


def krylov_kernel(
    count, cond_hbm, nodata_hbm, gmask_hbm, gval_hbm, smask_hbm, scur_hbm, t_hbm, focal_hbm,
    r0_ref, q_ref, w_ref, z_ref, y_ref, coef_ref,
    reals_ref, flags_ref, focal_ref, ids_ref, te_ref, ti_ref,
    thl_ref, wts_ref, spot_ref, qhalo_ref, zhalo_ref, msg_ref, got_ref, bmsg_ref, bgot_ref, tmsg_ref, tgot_ref,
    zmsg_ref, zgot_ref, acc_ref, stat_ref, all_ref, late_ref, lates_ref,
    send1, recv1, sendb, recvb, sendt, recvt, send2, recv2, send3, recv3, send4, recv4, sem_in, hello,
):
    rows, cols = reals_ref.shape[1:]
    tiles = cols // LANES
    pairs = focal_ref.shape[1]
    ext = pairs + EXTRA
    me = lax.axis_index("space")
    last = count - 1
    ends = ((0, 0), (1, rows - 1))
    inner = range(1, rows - 1)
    cuts = [slice(c * LANES, (c + 1) * LANES) for c in range(tiles)]

    has = (me > 0, me < last)
    few = count <= 4
    barrier = pltpu.get_barrier_semaphore()

    def greet(sem):
        for side in range(2):
            @pl.when(has[side])
            def _():
                pl.semaphore_signal(
                    sem, inc=1, device_id={"space": me - 1 if side == 0 else me + 1},
                    device_id_type=pl.DeviceIdType.MESH,
                )

    def greeted(sem):
        pl.semaphore_wait(sem, jnp.minimum(me, 1) + jnp.minimum(last - me, 1))

    if few:
        greet(barrier)
    else:
        for off in range(1, count):
            pl.semaphore_signal(
                barrier, inc=1, device_id={"space": lax.rem(me + off, count)},
                device_id_type=pl.DeviceIdType.MESH,
            )

    def whole(ref, i):
        return pltpu.make_async_copy(ref, ref, sem_in.at[i])

    ids_load = pltpu.make_async_copy(focal_hbm, ids_ref, sem_in.at[0])
    focal_load = pltpu.make_async_copy(focal_hbm, focal_ref, sem_in.at[1])
    inner_load = pltpu.make_async_copy(t_hbm.at[pl.ds(1, rows - 2)], ti_ref, sem_in.at[5])
    ids_load.start()
    focal_load.start()
    for side, r in ends:
        for cut in cuts:
            pltpu.make_async_copy(
                t_hbm.at[r, pl.ds(cut.start, LANES)], te_ref.at[side, pl.ds(cut.start, LANES)], sem_in.at[2]).start()
    for i, group in ((3, (cond_hbm, gval_hbm, scur_hbm)), (4, (nodata_hbm, gmask_hbm, smask_hbm))):
        for k, src in enumerate(group):
            pltpu.make_async_copy(src, (reals_ref, flags_ref)[i - 3].at[k], sem_in.at[i]).start()
    inner_load.start()
    ids_load.wait()
    focal_load.wait()
    whole(te_ref, 2).wait()

    def gather(src, at):
        for p in range(pairs):
            for i in range(2):
                r, k = at(ids_ref[i, p])
                spot_ref[i, p:p + 1, :] = src[r, pl.ds(k, 1), :]
        return FOCAL_CURRENT * spot_ref[0], -FOCAL_CURRENT * spot_ref[1]

    half, high = (rows * cols // 2).bit_length() - 1, cols.bit_length() - 1
    near_a, near_b = gather(
        te_ref, lambda i: (lax.shift_right_logical(i, half) & 1, i & (cols - 1)))

    diagonal = lax.broadcasted_iota(jnp.int32, (pairs, pairs), 0) == lax.broadcasted_iota(
        jnp.int32, (pairs, pairs), 1)
    lane = lax.broadcasted_iota(jnp.int32, (pairs, LANES), 1)

    def column(i):
        line = jnp.broadcast_to(focal_ref[i:i + 1, :].astype(F32), (pairs, pairs))
        return jnp.broadcast_to(
            jnp.sum(jnp.where(diagonal, line, 0.0), 1, keepdims=True).astype(jnp.int32), (pairs, LANES))

    at_a, at_b = (column(i) - me * (rows * cols) for i in range(2))
    spot_a, spot_b = (lax.shift_right_arithmetic(x, 7) for x in (at_a, at_b))
    tile_a, tile_b = spot_a & (tiles - 1), spot_b & (tiles - 1)

    def within(spot, low, high):
        return jnp.logical_and(spot >= low * tiles, spot < high * tiles)

    for side, r in ends:
        msg_ref[side, 0:pairs, :] = jnp.where(within(spot_a, r, r + 1), near_a, 0.0)
        msg_ref[side, pairs:2 * pairs, :] = jnp.where(within(spot_b, r, r + 1), near_b, 0.0)

    def side_copy(src, dst, ssem, rsem, side):
        return pltpu.make_async_remote_copy(
            src_ref=src.at[side], dst_ref=dst.at[1 - side],
            send_sem=ssem.at[side], recv_sem=rsem.at[1 - side],
            device_id={"space": me - 1 if side == 0 else me + 1},
            device_id_type=pl.DeviceIdType.MESH,
        )

    def send(src, dst, ssem, rsem):
        for side in range(2):
            @pl.when(has[side])
            def _():
                side_copy(src, dst, ssem, rsem, side).start()

            @pl.when(jnp.logical_not(has[side]))
            def _():
                dst[side] = jnp.zeros(dst.shape[1:], F32)

    def done(src, dst, ssem, rsem):
        for side in range(2):
            @pl.when(has[side])
            def _():
                side_copy(src, dst, ssem, rsem, side).wait_send()
                pltpu.make_async_remote_copy(
                    src_ref=src.at[1 - side], dst_ref=dst.at[side],
                    send_sem=ssem.at[1 - side], recv_sem=rsem.at[side],
                    device_id={"space": me - 1 if side == 0 else me + 1},
                    device_id_type=pl.DeviceIdType.MESH,
                ).wait_recv()

    if few:
        greeted(barrier)
    else:
        pl.semaphore_wait(barrier, last)
    send(msg_ref, got_ref, send1, recv1)

    whole(reals_ref, 3).wait()
    whole(flags_ref, 4).wait()
    valid = (1 - flags_ref[0]).astype(F32)
    active = reals_ref[0] * valid
    background = flags_ref[2].astype(F32) * reals_ref[2]

    def tile_of(r, c):
        if r == 0 or r == rows - 1:
            return te_ref[min(r, 1), cuts[c], :]
        return ti_ref[r - 1, cuts[c], :]

    def product(x, r, c):
        number = x.shape[0]
        hi = x.astype(BF16).astype(F32)
        lhs = jnp.concatenate([hi, x - hi], 0).astype(BF16)
        o = jnp.dot(lhs, thl_ref[r, c], preferred_element_type=F32)
        return o[:number, :LANES] + (o[:number, LANES:] + (o[number:, :LANES] + o[number:, LANES:]))

    def shared_row(r):
        dot = jnp.zeros((EXTRA, LANES), F32)
        for c, cut in enumerate(cuts):
            t = tile_of(r, c)
            thi = t.astype(BF16)
            thl_ref[r, c, :, :LANES] = thi
            thl_ref[r, c, :, LANES:] = (t - thi.astype(F32)).astype(BF16)
            x = jnp.broadcast_to(background[r:r + 1, cut], (EXTRA, LANES))
            q = product(x, r, c)
            q_ref[r, pairs:ext, cut] = q
            dot = dot + x * q
        return dot

    shared = shared_row(0) + shared_row(rows - 1)
    for side, r in ends:
        for c, cut in enumerate(cuts):
            bmsg_ref[side, c:c + 1, :] = q_ref[r, pairs:pairs + 1, cut]
            bmsg_ref[side, tiles + c:tiles + c + 1, :] = active[r:r + 1, cut]
            bmsg_ref[side, 2 * tiles + c:2 * tiles + c + 1, :] = valid[r:r + 1, cut]
            tmsg_ref[side, c:c + 1, :] = te_ref[side, cut.start:cut.start + 1, :]
            tmsg_ref[side, tiles + c:tiles + c + 1, :] = te_ref[side, cut.stop - 1:cut.stop, :]
    send(bmsg_ref, bgot_ref, sendb, recvb)
    send(tmsg_ref, tgot_ref, sendt, recvt)

    def edge(a, b, v, u):
        return 0.5 * (a + b) * v * u

    row_at = lax.broadcasted_iota(jnp.int32, (rows, cols), 0)
    col_at = lax.broadcasted_iota(jnp.int32, (rows, cols), 1)

    def shifted(x, by, axis):
        length = x.shape[axis]
        at = (row_at, col_at)[axis][:x.shape[0], :]
        return jnp.where(at == (0 if by == 1 else length - 1), 0.0, pltpu.roll(x, by % length, axis))

    nw, sw, ww, ew = (
        edge(active, shifted(active, *how), valid, shifted(valid, *how))
        for how in ((1, 0), (-1, 0), (1, 1), (-1, 1))
    )
    dg = valid * (LEAKAGE + flags_ref[1].astype(F32) * reals_ref[1]) + (1.0 - valid) + nw + sw + ww + ew
    for r in range(rows):
        for i, x in enumerate((dg, nw, sw, ww, ew, 0.5 * dg, background)):
            wts_ref[r, i:i + 1, :] = x[r:r + 1, :]

    inner_load.wait()
    far_a, far_b = gather(
        ti_ref, lambda i: (
            jnp.clip((lax.shift_right_logical(i, high) & (rows - 1)) - 1, 0, rows - 3), i & (cols - 1)))
    for r in inner:
        shared = shared + shared_row(r)

    def dense_row(r, a, b, dot):
        for c, cut in enumerate(cuts):
            k = r * tiles + c
            x = jnp.where(spot_a == k, a, 0.0) + jnp.where(spot_b == k, b, 0.0)
            q_ref[r, 0:pairs, cut] = q_ref[r, pairs:pairs + 1, cut] + x
            dot = dot + background[r:r + 1, cut] * x
        return dot

    dot = jnp.zeros((pairs, LANES), F32)
    for r in range(rows):
        a, b = (far_a, far_b) if r in inner else (near_a, near_b)
        dot = dense_row(r, a, b, dot)
    in_a, in_b = (
        jnp.where(within(spot, 1, rows - 1), far, jnp.where(within(spot, 0, rows), near, 0.0))
        for spot, far, near in ((spot_a, far_a, near_a), (spot_b, far_b, near_b))
    )
    same = spot_a == spot_b
    own = jnp.where(lane == (at_a & (LANES - 1)), in_a + jnp.where(same, in_b, 0.0), 0.0) - jnp.where(
        lane == (at_b & (LANES - 1)), in_b + jnp.where(same, in_a, 0.0), 0.0)
    acc_ref[0] = 2.0 * dot + FOCAL_CURRENT * own + jnp.broadcast_to(shared[0:1, :], dot.shape)
    for i in range(1, 4):
        acc_ref[i] = jnp.zeros(acc_ref.shape[1:], F32)

    parts = [slice(p, p + 16) for p in range(0, pairs, 16)]
    extra = slice(pairs, ext)

    def stream(src, r, s, east=True):
        at = lane[:s.stop - s.start]
        x = src[r, s, cuts[0]]
        gone, west, ahead = None, pltpu.roll(x, 1, 1), east and pltpu.roll(x, LANES - 1, 1)
        for c in range(tiles):
            more = c + 1 < tiles
            if more:
                y = src[r, s, cuts[c + 1]]
                after = east and pltpu.roll(y, LANES - 1, 1)
            yield (
                c, cuts[c], x, west if gone is None else jnp.where(at == 0, gone, west),
                jnp.where(at == LANES - 1, after, ahead) if east and more else ahead,
            )
            if more:
                x, gone, west, ahead = y, west, pltpu.roll(y, 1, 1), after

    def apply_part(src, dst, r, s, north, south, acc=None):
        dots = None
        for c, cut, x, west, east in stream(src, r, s):
            out = wts_ref[r, 0:1, cut] * x - wts_ref[r, 3:4, cut] * west - wts_ref[r, 4:5, cut] * east
            if north is not None:
                out = out - wts_ref[r, 1:2, cut] * north[0][north[1], s, cut]
            if south is not None:
                out = out - wts_ref[r, 2:3, cut] * south[0][south[1], s, cut]
            dst[r, s, cut] = out
            dots = x * out if dots is None else dots + x * out
        if acc is not None:
            acc_ref[acc, s, :] += dots

    def apply_inner(src, dst, both, acc=None):
        def body(r, carry):
            for s in parts:
                apply_part(src, dst, r, s, (src, r - 1), (src, r + 1), acc)
            if both:
                apply_part(src, dst, r, extra, (src, r - 1), (src, r + 1))
            return carry
        lax.fori_loop(1, rows - 1, body, 0)

    for s in (*parts, extra):
        apply_part(q_ref, w_ref, 0, s, None, (q_ref, 1))
        apply_part(q_ref, w_ref, rows - 1, s, (q_ref, rows - 2), None)

    done(msg_ref, got_ref, send1, recv1)
    if few:
        greet(hello)
    done(bmsg_ref, bgot_ref, sendb, recvb)

    def row_of(side, base):
        return jnp.concatenate([bgot_ref[side, base + c:base + c + 1, :] for c in range(tiles)], 1)

    halo_a = [row_of(side, tiles) for side in range(2)]
    halo_v = [row_of(side, 2 * tiles) for side in range(2)]
    for side, r in ends:
        i = 1 + side
        h = edge(active[r:r + 1, :], halo_a[side], valid[r:r + 1, :], halo_v[side])
        wts_ref[r, i:i + 1, :] = h
        wts_ref[r, 0:1, :] += h
        wts_ref[r, 5:6, :] += 0.5 * h
        va = got_ref[side, 0:pairs, :]
        vb = got_ref[side, pairs:2 * pairs, :]
        dots = jnp.zeros((pairs, LANES), F32)
        for c, cut in enumerate(cuts):
            common = bgot_ref[side, c:c + 1, :]
            qh = jnp.where(tile_a == c, va, 0.0) + jnp.where(tile_b == c, vb, 0.0)
            qhalo_ref[side, :, cut] = qh
            q0 = q_ref[r, :pairs, cut]
            w0 = w_ref[r, :pairs, cut] + h[:, cut] * (q0 - (qh + common))
            w_ref[r, :pairs, cut] = w0
            w_ref[r, extra, cut] += h[:, cut] * (q_ref[r, extra, cut] - common)
            dots = dots + q0 * w0
        acc_ref[1] += dots

    def precond_row(r):
        for c, cut in enumerate(cuts):
            z_ref[r, :, cut] = product(w_ref[r, :, cut], r, c)

    def pack(src, r, dst, side):
        va = src[r, :pairs, 0:LANES]
        vb = va
        for c in range(1, tiles):
            x = src[r, :pairs, cuts[c]]
            va = jnp.where(tile_a == c, x, va)
            vb = jnp.where(tile_b == c, x, vb)
        dst[side, 0:pairs, :] = va
        dst[side, pairs:2 * pairs, :] = vb
        for c, cut in enumerate(cuts):
            dst[side, 2 * pairs + c:2 * pairs + c + 1, :] = src[r, pairs:pairs + 1, cut]

    precond_row(0)
    precond_row(rows - 1)
    for side, r in ends:
        pack(z_ref, r, zmsg_ref, side)
    send(zmsg_ref, zgot_ref, send2, recv2)

    apply_inner(q_ref, w_ref, True, 1)
    for r in inner:
        precond_row(r)

    def moment_part(r, s, north):
        mu = nu = None
        for c, cut, z, west, _ in stream(z_ref, r, s, False):
            t = wts_ref[r, 5:6, cut] * z - wts_ref[r, 3:4, cut] * west
            if north:
                t = t - wts_ref[r, 1:2, cut] * z_ref[r - 1, s, cut]
            one, two = w_ref[r, s, cut] * z, t * z
            mu, nu = (one, two) if mu is None else (mu + one, nu + two)
        acc_ref[2, s, :] += mu
        acc_ref[3, s, :] += nu

    def moments(r, carry):
        for s in parts:
            moment_part(r, s, True)
        return carry

    for s in parts:
        moment_part(0, s, False)
    lax.fori_loop(1, rows, moments, 0)

    pad = jnp.zeros((8, LANES - pairs), F32)

    def lines(sums):
        table = jnp.zeros((pairs, LANES), F32)
        for i, x in enumerate(sums):
            table = jnp.where(lane == i, jnp.sum(x, 1, keepdims=True), table)
        return jnp.concatenate([table.T[0:8, :], pad], 1)

    def exchange(src, dst, ssem, rsem):
        for k in range(1, count):
            pltpu.make_async_remote_copy(
                src_ref=src, dst_ref=dst.at[k - 1], send_sem=ssem, recv_sem=rsem,
                device_id={"space": lax.rem(me + k, count)}, device_id_type=pl.DeviceIdType.MESH,
            ).start()

    def arrived(dst, ssem, rsem):
        for sem in (ssem, rsem):
            pltpu.make_async_copy(dst, dst, sem).wait()

    early = lines([acc_ref[i] for i in range(4)])
    stat_ref[...] = early
    if few:
        greeted(hello)
    exchange(stat_ref, all_ref, send3, recv3)

    done(tmsg_ref, tgot_ref, sendt, recvt)
    for side in range(2):
        halo_w, halo_e = (
            edge(halo_a[side], shifted(halo_a[side], by, 1), halo_v[side], shifted(halo_v[side], by, 1))
            for by in (1, -1)
        )
        near = [jnp.zeros((pairs, LANES), F32)] * tiles
        for c, cut in enumerate(cuts):
            qh = qhalo_ref[side, :, cut]
            if c > 0:
                gone = (halo_w[:, cut] * qh)[:, 0:1]
                near[c - 1] = near[c - 1] - gone * tgot_ref[side, tiles + c - 1:tiles + c, :]
            if c < tiles - 1:
                gone = (halo_e[:, cut] * qh)[:, LANES - 1:LANES]
                near[c + 1] = near[c + 1] - gone * tgot_ref[side, c + 1:c + 2, :]
        for c, cut in enumerate(cuts):
            zhalo_ref[side, :, cut] = near[c]

    done(zmsg_ref, zgot_ref, send2, recv2)
    coupling = []
    for side, r in ends:
        va = zgot_ref[side, 0:pairs, :]
        vb = zgot_ref[side, pairs:2 * pairs, :]
        total = jnp.zeros((pairs, LANES), F32)
        for c, cut in enumerate(cuts):
            other = zgot_ref[side, 2 * pairs + c:2 * pairs + c + 1, :] + zhalo_ref[side, :, cut]
            zh = jnp.where(tile_a == c, va, jnp.where(tile_b == c, vb, other))
            zhalo_ref[side, :, cut] = zh
            total = total + wts_ref[r, 1 + side:2 + side, cut] * z_ref[r, :pairs, cut] * zh
        coupling.append(total)
    late = lines(coupling)
    late_ref[...] = late
    exchange(late_ref, lates_ref, send4, recv4)

    apply_inner(z_ref, y_ref, False)
    for s in parts:
        apply_part(z_ref, y_ref, 0, s, (zhalo_ref, 0), (z_ref, 1))
        apply_part(z_ref, y_ref, rows - 1, s, (z_ref, rows - 2), (zhalo_ref, 1))

    def right_side(r, carry):
        for c, cut in enumerate(cuts):
            local = r * cols + c * LANES + lane
            x = jnp.where(local == at_a, FOCAL_CURRENT, 0.0) - jnp.where(local == at_b, FOCAL_CURRENT, 0.0)
            r0_ref[r, 0:pairs, cut] = wts_ref[r, 6:7, cut] + x
        return carry

    lax.fori_loop(0, rows, right_side, 0)

    arrived(all_ref, send3, recv3)
    total = early
    for k in range(1, count):
        total = total + all_ref[k - 1]
    gamma0, kappa, mu, part = (total[i:i + 1, :] for i in range(4))
    a0 = gamma0 / kappa
    gamma1 = a0 * a0 * mu - gamma0
    beta = gamma1 / gamma0
    known = kappa - 2.0 * a0 * mu - beta * gamma1 / a0 + 2.0 * a0 * a0 * part
    scale = 2.0 * a0 * a0
    joint = late[0:1, :] + late[1:2, :]
    arrived(lates_ref, send4, recv4)
    for k in range(1, count):
        joint = joint + jnp.where(k <= me, lates_ref[k - 1, 0:1, :], lates_ref[k - 1, 1:2, :])
    a1 = gamma1 / (known - scale * joint)
    first = a0 + a1 * (1.0 + beta)
    both = jnp.concatenate([first, a0 * a1, jnp.zeros((6, LANES), F32)], 0).T
    for i in range(2):
        coef_ref[i] = jnp.broadcast_to(both[:pairs, i:i + 1], (pairs, LANES))


def combine_kernel(coef_ref, r0_ref, q_ref, w_ref, z_ref, y_ref, sol_hbm, res_hbm, sol_ref, res_ref, sem):
    rows, pairs, cols = sol_ref.shape
    mine = pl.ds(0, pairs)

    def out(r, src, dst, k):
        return pltpu.make_async_copy(src.at[r], dst.at[mine, r], sem.at[k, r])

    def body(r, carry):
        one, two = coef_ref[0], coef_ref[1]
        for c in range(cols // LANES):
            cut = slice(c * LANES, (c + 1) * LANES)
            sol_ref[r, :, cut] = one * q_ref[r, mine, cut] - two * z_ref[r, mine, cut]
            res_ref[r, :, cut] = r0_ref[r, mine, cut] - one * w_ref[r, mine, cut] + two * y_ref[r, mine, cut]
        out(r, sol_ref, sol_hbm, 0).start()
        out(r, res_ref, res_hbm, 1).start()
        return carry

    lax.fori_loop(0, rows, body, 0)

    def finish(r, carry):
        out(r, sol_ref, sol_hbm, 0).wait()
        out(r, res_ref, res_hbm, 1).wait()
        return carry

    lax.fori_loop(0, rows, finish, 0)


def on_device(count, cond, nodata, gmask, gval, smask, scur, tinv, focal):
    rows, cols = cond.shape
    pairs = focal.shape[0]
    tiles = cols // LANES
    ext = pairs + EXTRA
    field = jax.ShapeDtypeStruct((rows, ext, cols), F32)
    vm = pl.BlockSpec(memory_space=pltpu.VMEM)
    hbm = pl.BlockSpec(memory_space=pltpu.HBM)
    msg = (2, 2 * pairs, LANES)
    bmsg = (2, 3 * tiles, LANES)
    tmsg = (2, 2 * tiles, LANES)
    zmsg = (2, 2 * pairs + tiles, LANES)
    others = count - 1
    r0, q, w, z, y, coef = pl.pallas_call(
        functools.partial(krylov_kernel, count),
        out_shape=[field] * 5 + [jax.ShapeDtypeStruct((2, pairs, LANES), F32)],
        in_specs=[hbm] * 8,
        out_specs=[vm] * 6,
        scratch_shapes=[
            pltpu.VMEM((3, rows, cols), F32),
            pltpu.VMEM((3, rows, cols), jnp.int32),
            pltpu.VMEM((2, pairs), jnp.int32),
            pltpu.SMEM((2, pairs), jnp.int32),
            pltpu.VMEM((2, cols, LANES), F32),
            pltpu.VMEM((rows - 2, cols, LANES), F32),
            pltpu.VMEM((rows, tiles, LANES, 2 * LANES), BF16),
            pltpu.VMEM((rows, 8, cols), F32),
            pltpu.VMEM((2, pairs, LANES), F32),
            pltpu.VMEM((2, pairs, cols), F32),
            pltpu.VMEM((2, pairs, cols), F32),
            *[pltpu.VMEM(shape, F32) for shape in (msg, bmsg, tmsg, zmsg) for _ in range(2)],
            pltpu.VMEM((4, pairs, LANES), F32),
            *[pltpu.VMEM(shape, F32) for _ in range(2) for shape in ((8, LANES), (others, 8, LANES))],
            *[pltpu.SemaphoreType.DMA((2,))] * 8,
            *[pltpu.SemaphoreType.DMA] * 4,
            pltpu.SemaphoreType.DMA((6,)),
            pltpu.SemaphoreType.REGULAR,
        ],
        compiler_params=pltpu.CompilerParams(
            collective_id=0, has_side_effects=True, vmem_limit_bytes=36 * 1024 * 1024
        ),
        name="krylov",
    )(*(
        pltpu.with_memory_space_constraint(x, pltpu.HBM)
        for x in (cond, nodata, gmask, gval, smask, scur, tinv.reshape(rows, cols, LANES), focal.T)
    ))

    out = jax.ShapeDtypeStruct((pairs, rows, cols), F32)
    return tuple(pl.pallas_call(
        combine_kernel,
        out_shape=[out, out],
        in_specs=[vm] * 6,
        out_specs=[hbm, hbm],
        scratch_shapes=[
            pltpu.VMEM((rows, pairs, cols), F32),
            pltpu.VMEM((rows, pairs, cols), F32),
            pltpu.SemaphoreType.DMA((2, rows)),
        ],
        compiler_params=pltpu.CompilerParams(vmem_limit_bytes=20 * 1024 * 1024),
        name="combine",
    )(coef, r0, q, w, z, y))


def solution(mesh):
    return jax.shard_map(
        functools.partial(on_device, mesh.shape["space"]),
        mesh=mesh,
        in_specs=(
            P(("groups", "space"), None),
            P(("groups", "space"), None),
            P(("groups", "space"), None),
            P(("groups", "space"), None),
            P(("groups", "space"), None),
            P(("groups", "space"), None),
            P(("groups", "space"), None, None, None),
            P(("groups", "rhs"), None),
        ),
        out_specs=(P("rhs", ("groups", "space"), None), P("rhs", ("groups", "space"), None)),
        check_vma=False,
    )
```

```python
import functools

import jax
import jax.numpy as jnp
from jax import lax
from jax.experimental import pallas as pl
from jax.experimental.pallas import tpu as pltpu
from jax.sharding import PartitionSpec as P

LEAKAGE = 0.05
FOCAL_CURRENT = 16.0
LANES = 128
EXTRA = 8
F32 = jnp.float32
BF16 = jnp.bfloat16


def krylov_kernel(
    count, cond_hbm, nodata_hbm, gmask_hbm, gval_hbm, smask_hbm, scur_hbm, t_hbm, focal_hbm,
    r0_ref, q_ref, w_ref, z_ref, y_ref, coef_ref,
    reals_ref, flags_ref, focal_ref, ids_ref, te_ref, ti_ref,
    thl_ref, wts_ref, spot_ref, qhalo_ref, zhalo_ref, msg_ref, got_ref, bmsg_ref, bgot_ref, tmsg_ref, tgot_ref,
    zmsg_ref, zgot_ref, acc_ref, stat_ref, all_ref, late_ref, lates_ref,
    send1, recv1, sendb, recvb, sendt, recvt, send2, recv2, send3, recv3, send4, recv4, sem_in, hello,
):
    rows, cols = reals_ref.shape[1:]
    tiles = cols // LANES
    pairs = focal_ref.shape[1]
    ext = pairs + EXTRA
    me = lax.axis_index("space")
    last = count - 1
    ends = ((0, 0), (1, rows - 1))
    inner = range(1, rows - 1)
    cuts = [slice(c * LANES, (c + 1) * LANES) for c in range(tiles)]

    has = (me > 0, me < last)
    few = count <= 4
    barrier = pltpu.get_barrier_semaphore()

    def greet(sem):
        for side in range(2):
            @pl.when(has[side])
            def _():
                pl.semaphore_signal(
                    sem, inc=1, device_id={"space": me - 1 if side == 0 else me + 1},
                    device_id_type=pl.DeviceIdType.MESH,
                )

    def greeted(sem):
        pl.semaphore_wait(sem, jnp.minimum(me, 1) + jnp.minimum(last - me, 1))

    if few:
        greet(barrier)
    else:
        for off in range(1, count):
            pl.semaphore_signal(
                barrier, inc=1, device_id={"space": lax.rem(me + off, count)},
                device_id_type=pl.DeviceIdType.MESH,
            )

    def whole(ref, i):
        return pltpu.make_async_copy(ref, ref, sem_in.at[i])

    ids_load = pltpu.make_async_copy(focal_hbm, ids_ref, sem_in.at[0])
    focal_load = pltpu.make_async_copy(focal_hbm, focal_ref, sem_in.at[1])
    inner_load = pltpu.make_async_copy(t_hbm.at[pl.ds(1, rows - 2)], ti_ref, sem_in.at[5])
    ids_load.start()
    focal_load.start()
    for side, r in ends:
        for cut in cuts:
            pltpu.make_async_copy(
                t_hbm.at[r, pl.ds(cut.start, LANES)], te_ref.at[side, pl.ds(cut.start, LANES)], sem_in.at[2]).start()
    for i, group in ((3, (cond_hbm, gval_hbm, scur_hbm)), (4, (nodata_hbm, gmask_hbm, smask_hbm))):
        for k, src in enumerate(group):
            pltpu.make_async_copy(src, (reals_ref, flags_ref)[i - 3].at[k], sem_in.at[i]).start()
    inner_load.start()
    ids_load.wait()
    focal_load.wait()
    whole(te_ref, 2).wait()

    def gather(src, at):
        for p in range(pairs):
            for i in range(2):
                r, k = at(ids_ref[i, p])
                spot_ref[i, p:p + 1, :] = src[r, pl.ds(k, 1), :]
        return FOCAL_CURRENT * spot_ref[0], -FOCAL_CURRENT * spot_ref[1]

    half, high = (rows * cols // 2).bit_length() - 1, cols.bit_length() - 1
    near_a, near_b = gather(
        te_ref, lambda i: (lax.shift_right_logical(i, half) & 1, i & (cols - 1)))

    diagonal = lax.broadcasted_iota(jnp.int32, (pairs, pairs), 0) == lax.broadcasted_iota(
        jnp.int32, (pairs, pairs), 1)
    lane = lax.broadcasted_iota(jnp.int32, (pairs, LANES), 1)

    def column(i):
        line = jnp.broadcast_to(focal_ref[i:i + 1, :].astype(F32), (pairs, pairs))
        return jnp.broadcast_to(
            jnp.sum(jnp.where(diagonal, line, 0.0), 1, keepdims=True).astype(jnp.int32), (pairs, LANES))

    at_a, at_b = (column(i) - me * (rows * cols) for i in range(2))
    spot_a, spot_b = (lax.shift_right_arithmetic(x, 7) for x in (at_a, at_b))
    tile_a, tile_b = spot_a & (tiles - 1), spot_b & (tiles - 1)

    def within(spot, low, high):
        return jnp.logical_and(spot >= low * tiles, spot < high * tiles)

    for side, r in ends:
        msg_ref[side, 0:pairs, :] = jnp.where(within(spot_a, r, r + 1), near_a, 0.0)
        msg_ref[side, pairs:2 * pairs, :] = jnp.where(within(spot_b, r, r + 1), near_b, 0.0)

    def side_copy(src, dst, ssem, rsem, side):
        return pltpu.make_async_remote_copy(
            src_ref=src.at[side], dst_ref=dst.at[1 - side],
            send_sem=ssem.at[side], recv_sem=rsem.at[1 - side],
            device_id={"space": me - 1 if side == 0 else me + 1},
            device_id_type=pl.DeviceIdType.MESH,
        )

    def send(src, dst, ssem, rsem):
        for side in range(2):
            @pl.when(has[side])
            def _():
                side_copy(src, dst, ssem, rsem, side).start()

            @pl.when(jnp.logical_not(has[side]))
            def _():
                dst[side] = jnp.zeros(dst.shape[1:], F32)

    def done(src, dst, ssem, rsem):
        for side in range(2):
            @pl.when(has[side])
            def _():
                side_copy(src, dst, ssem, rsem, side).wait_send()
                pltpu.make_async_remote_copy(
                    src_ref=src.at[1 - side], dst_ref=dst.at[side],
                    send_sem=ssem.at[1 - side], recv_sem=rsem.at[side],
                    device_id={"space": me - 1 if side == 0 else me + 1},
                    device_id_type=pl.DeviceIdType.MESH,
                ).wait_recv()

    if few:
        greeted(barrier)
    else:
        pl.semaphore_wait(barrier, last)
    send(msg_ref, got_ref, send1, recv1)

    whole(reals_ref, 3).wait()
    whole(flags_ref, 4).wait()
    valid = (1 - flags_ref[0]).astype(F32)
    active = reals_ref[0] * valid
    background = flags_ref[2].astype(F32) * reals_ref[2]

    def tile_of(r, c):
        if r == 0 or r == rows - 1:
            return te_ref[min(r, 1), cuts[c], :]
        return ti_ref[r - 1, cuts[c], :]

    def product(x, r, c):
        number = x.shape[0]
        hi = x.astype(BF16).astype(F32)
        lhs = jnp.concatenate([hi, x - hi], 0).astype(BF16)
        o = jnp.dot(lhs, thl_ref[r, c], preferred_element_type=F32)
        return o[:number, :LANES] + (o[:number, LANES:] + (o[number:, :LANES] + o[number:, LANES:]))

    def shared_row(r):
        dot = jnp.zeros((EXTRA, LANES), F32)
        for c, cut in enumerate(cuts):
            t = tile_of(r, c)
            thi = t.astype(BF16)
            thl_ref[r, c, :, :LANES] = thi
            thl_ref[r, c, :, LANES:] = (t - thi.astype(F32)).astype(BF16)
            x = jnp.broadcast_to(background[r:r + 1, cut], (EXTRA, LANES))
            q = product(x, r, c)
            q_ref[r, pairs:ext, cut] = q
            dot = dot + x * q
        return dot

    shared = shared_row(0) + shared_row(rows - 1)
    for side, r in ends:
        for c, cut in enumerate(cuts):
            bmsg_ref[side, c:c + 1, :] = q_ref[r, pairs:pairs + 1, cut]
            bmsg_ref[side, tiles + c:tiles + c + 1, :] = active[r:r + 1, cut]
            bmsg_ref[side, 2 * tiles + c:2 * tiles + c + 1, :] = valid[r:r + 1, cut]
            tmsg_ref[side, c:c + 1, :] = te_ref[side, cut.start:cut.start + 1, :]
            tmsg_ref[side, tiles + c:tiles + c + 1, :] = te_ref[side, cut.stop - 1:cut.stop, :]
    send(bmsg_ref, bgot_ref, sendb, recvb)
    send(tmsg_ref, tgot_ref, sendt, recvt)

    def edge(a, b, v, u):
        return 0.5 * (a + b) * v * u

    row_at = lax.broadcasted_iota(jnp.int32, (rows, cols), 0)
    col_at = lax.broadcasted_iota(jnp.int32, (rows, cols), 1)

    def shifted(x, by, axis):
        length = x.shape[axis]
        at = (row_at, col_at)[axis][:x.shape[0], :]
        return jnp.where(at == (0 if by == 1 else length - 1), 0.0, pltpu.roll(x, by % length, axis))

    nw, sw, ww, ew = (
        edge(active, shifted(active, *how), valid, shifted(valid, *how))
        for how in ((1, 0), (-1, 0), (1, 1), (-1, 1))
    )
    dg = valid * (LEAKAGE + flags_ref[1].astype(F32) * reals_ref[1]) + (1.0 - valid) + nw + sw + ww + ew
    for r in range(rows):
        for i, x in enumerate((dg, nw, sw, ww, ew, 0.5 * dg, background)):
            wts_ref[r, i:i + 1, :] = x[r:r + 1, :]

    inner_load.wait()
    far_a, far_b = gather(
        ti_ref, lambda i: (
            jnp.clip((lax.shift_right_logical(i, high) & (rows - 1)) - 1, 0, rows - 3), i & (cols - 1)))
    for r in inner:
        shared = shared + shared_row(r)

    def dense_row(r, a, b, dot):
        for c, cut in enumerate(cuts):
            k = r * tiles + c
            x = jnp.where(spot_a == k, a, 0.0) + jnp.where(spot_b == k, b, 0.0)
            q_ref[r, 0:pairs, cut] = q_ref[r, pairs:pairs + 1, cut] + x
            dot = dot + background[r:r + 1, cut] * x
        return dot

    dot = jnp.zeros((pairs, LANES), F32)
    for r in range(rows):
        a, b = (far_a, far_b) if r in inner else (near_a, near_b)
        dot = dense_row(r, a, b, dot)
    in_a, in_b = (
        jnp.where(within(spot, 1, rows - 1), far, jnp.where(within(spot, 0, rows), near, 0.0))
        for spot, far, near in ((spot_a, far_a, near_a), (spot_b, far_b, near_b))
    )
    same = spot_a == spot_b
    own = jnp.where(lane == (at_a & (LANES - 1)), in_a + jnp.where(same, in_b, 0.0), 0.0) - jnp.where(
        lane == (at_b & (LANES - 1)), in_b + jnp.where(same, in_a, 0.0), 0.0)
    acc_ref[0] = 2.0 * dot + FOCAL_CURRENT * own + jnp.broadcast_to(shared[0:1, :], dot.shape)
    for i in range(1, 4):
        acc_ref[i] = jnp.zeros(acc_ref.shape[1:], F32)

    parts = [slice(p, p + 16) for p in range(0, pairs, 16)]
    extra = slice(pairs, ext)

    def stream(src, r, s, east=True):
        at = lane[:s.stop - s.start]
        x = src[r, s, cuts[0]]
        gone, west, ahead = None, pltpu.roll(x, 1, 1), east and pltpu.roll(x, LANES - 1, 1)
        for c in range(tiles):
            more = c + 1 < tiles
            if more:
                y = src[r, s, cuts[c + 1]]
                after = east and pltpu.roll(y, LANES - 1, 1)
            yield (
                c, cuts[c], x, west if gone is None else jnp.where(at == 0, gone, west),
                jnp.where(at == LANES - 1, after, ahead) if east and more else ahead,
            )
            if more:
                x, gone, west, ahead = y, west, pltpu.roll(y, 1, 1), after

    def apply_part(src, dst, r, s, north, south, acc=None):
        dots = None
        for c, cut, x, west, east in stream(src, r, s):
            out = wts_ref[r, 0:1, cut] * x - wts_ref[r, 3:4, cut] * west - wts_ref[r, 4:5, cut] * east
            if north is not None:
                out = out - wts_ref[r, 1:2, cut] * north[0][north[1], s, cut]
            if south is not None:
                out = out - wts_ref[r, 2:3, cut] * south[0][south[1], s, cut]
            dst[r, s, cut] = out
            dots = x * out if dots is None else dots + x * out
        if acc is not None:
            acc_ref[acc, s, :] += dots

    def apply_inner(src, dst):
        def body(r, carry):
            for s in parts:
                apply_part(src, dst, r, s, (src, r - 1), (src, r + 1))
            return carry
        lax.fori_loop(1, rows - 1, body, 0)

    for s in (*parts, extra):
        apply_part(q_ref, w_ref, 0, s, None, (q_ref, 1))
        apply_part(q_ref, w_ref, rows - 1, s, (q_ref, rows - 2), None)

    done(msg_ref, got_ref, send1, recv1)
    if few:
        greet(hello)
    done(bmsg_ref, bgot_ref, sendb, recvb)

    def row_of(side, base):
        return jnp.concatenate([bgot_ref[side, base + c:base + c + 1, :] for c in range(tiles)], 1)

    halo_a = [row_of(side, tiles) for side in range(2)]
    halo_v = [row_of(side, 2 * tiles) for side in range(2)]
    for side, r in ends:
        i = 1 + side
        h = edge(active[r:r + 1, :], halo_a[side], valid[r:r + 1, :], halo_v[side])
        wts_ref[r, i:i + 1, :] = h
        wts_ref[r, 0:1, :] += h
        wts_ref[r, 5:6, :] += 0.5 * h
        va = got_ref[side, 0:pairs, :]
        vb = got_ref[side, pairs:2 * pairs, :]
        dots = jnp.zeros((pairs, LANES), F32)
        for c, cut in enumerate(cuts):
            common = bgot_ref[side, c:c + 1, :]
            qh = jnp.where(tile_a == c, va, 0.0) + jnp.where(tile_b == c, vb, 0.0)
            qhalo_ref[side, :, cut] = qh
            q0 = q_ref[r, :pairs, cut]
            w0 = w_ref[r, :pairs, cut] + h[:, cut] * (q0 - (qh + common))
            w_ref[r, :pairs, cut] = w0
            w_ref[r, extra, cut] += h[:, cut] * (q_ref[r, extra, cut] - common)
            dots = dots + q0 * w0
        acc_ref[1] += dots

    def precond_row(r):
        for c, cut in enumerate(cuts):
            z_ref[r, :, cut] = product(w_ref[r, :, cut], r, c)

    def pack(src, r, dst, side):
        va = src[r, :pairs, 0:LANES]
        vb = va
        for c in range(1, tiles):
            x = src[r, :pairs, cuts[c]]
            va = jnp.where(tile_a == c, x, va)
            vb = jnp.where(tile_b == c, x, vb)
        dst[side, 0:pairs, :] = va
        dst[side, pairs:2 * pairs, :] = vb
        for c, cut in enumerate(cuts):
            dst[side, 2 * pairs + c:2 * pairs + c + 1, :] = src[r, pairs:pairs + 1, cut]

    precond_row(0)
    precond_row(rows - 1)
    for side, r in ends:
        pack(z_ref, r, zmsg_ref, side)
    send(zmsg_ref, zgot_ref, send2, recv2)


    def moment_part(r, s, north):
        mu = nu = None
        for c, cut, z, west, _ in stream(z_ref, r, s, False):
            t = wts_ref[r, 5:6, cut] * z - wts_ref[r, 3:4, cut] * west
            if north:
                t = t - wts_ref[r, 1:2, cut] * z_ref[r - 1, s, cut]
            one, two = w_ref[r, s, cut] * z, t * z
            mu, nu = (one, two) if mu is None else (mu + one, nu + two)
        acc_ref[2, s, :] += mu
        acc_ref[3, s, :] += nu

    def image_row(r):
        for s in parts:
            apply_part(q_ref, w_ref, r, s, (q_ref, r - 1), (q_ref, r + 1), 1)
        apply_part(q_ref, w_ref, r, extra, (q_ref, r - 1), (q_ref, r + 1))

    def moment_row(r):
        for s in parts:
            moment_part(r, s, r > 0)

    image_row(1)
    for r in inner:
        if r + 1 in inner:
            image_row(r + 1)
        precond_row(r)
        moment_row(r - 1)
    moment_row(rows - 2)
    moment_row(rows - 1)

    pad = jnp.zeros((8, LANES - pairs), F32)

    def lines(sums):
        table = jnp.zeros((pairs, LANES), F32)
        for i, x in enumerate(sums):
            table = jnp.where(lane == i, jnp.sum(x, 1, keepdims=True), table)
        return jnp.concatenate([table.T[0:8, :], pad], 1)

    def exchange(src, dst, ssem, rsem):
        for k in range(1, count):
            pltpu.make_async_remote_copy(
                src_ref=src, dst_ref=dst.at[k - 1], send_sem=ssem, recv_sem=rsem,
                device_id={"space": lax.rem(me + k, count)}, device_id_type=pl.DeviceIdType.MESH,
            ).start()

    def arrived(dst, ssem, rsem):
        for sem in (ssem, rsem):
            pltpu.make_async_copy(dst, dst, sem).wait()

    early = lines([acc_ref[i] for i in range(4)])
    stat_ref[...] = early
    if few:
        greeted(hello)
    exchange(stat_ref, all_ref, send3, recv3)

    done(tmsg_ref, tgot_ref, sendt, recvt)
    for side in range(2):
        halo_w, halo_e = (
            edge(halo_a[side], shifted(halo_a[side], by, 1), halo_v[side], shifted(halo_v[side], by, 1))
            for by in (1, -1)
        )
        near = [jnp.zeros((pairs, LANES), F32)] * tiles
        for c, cut in enumerate(cuts):
            qh = qhalo_ref[side, :, cut]
            if c > 0:
                gone = (halo_w[:, cut] * qh)[:, 0:1]
                near[c - 1] = near[c - 1] - gone * tgot_ref[side, tiles + c - 1:tiles + c, :]
            if c < tiles - 1:
                gone = (halo_e[:, cut] * qh)[:, LANES - 1:LANES]
                near[c + 1] = near[c + 1] - gone * tgot_ref[side, c + 1:c + 2, :]
        for c, cut in enumerate(cuts):
            zhalo_ref[side, :, cut] = near[c]

    done(zmsg_ref, zgot_ref, send2, recv2)
    coupling = []
    for side, r in ends:
        va = zgot_ref[side, 0:pairs, :]
        vb = zgot_ref[side, pairs:2 * pairs, :]
        total = jnp.zeros((pairs, LANES), F32)
        for c, cut in enumerate(cuts):
            other = zgot_ref[side, 2 * pairs + c:2 * pairs + c + 1, :] + zhalo_ref[side, :, cut]
            zh = jnp.where(tile_a == c, va, jnp.where(tile_b == c, vb, other))
            zhalo_ref[side, :, cut] = zh
            total = total + wts_ref[r, 1 + side:2 + side, cut] * z_ref[r, :pairs, cut] * zh
        coupling.append(total)
    late = lines(coupling)
    late_ref[...] = late
    exchange(late_ref, lates_ref, send4, recv4)

    apply_inner(z_ref, y_ref)
    for s in parts:
        apply_part(z_ref, y_ref, 0, s, (zhalo_ref, 0), (z_ref, 1))
        apply_part(z_ref, y_ref, rows - 1, s, (z_ref, rows - 2), (zhalo_ref, 1))

    def right_side(r, carry):
        for c, cut in enumerate(cuts):
            local = r * cols + c * LANES + lane
            x = jnp.where(local == at_a, FOCAL_CURRENT, 0.0) - jnp.where(local == at_b, FOCAL_CURRENT, 0.0)
            r0_ref[r, 0:pairs, cut] = wts_ref[r, 6:7, cut] + x
        return carry

    lax.fori_loop(0, rows, right_side, 0)

    arrived(all_ref, send3, recv3)
    total = early
    for k in range(1, count):
        total = total + all_ref[k - 1]
    gamma0, kappa, mu, part = (total[i:i + 1, :] for i in range(4))
    a0 = gamma0 / kappa
    gamma1 = a0 * a0 * mu - gamma0
    beta = gamma1 / gamma0
    known = kappa - 2.0 * a0 * mu - beta * gamma1 / a0 + 2.0 * a0 * a0 * part
    scale = 2.0 * a0 * a0
    joint = late[0:1, :] + late[1:2, :]
    arrived(lates_ref, send4, recv4)
    for k in range(1, count):
        joint = joint + jnp.where(k <= me, lates_ref[k - 1, 0:1, :], lates_ref[k - 1, 1:2, :])
    a1 = gamma1 / (known - scale * joint)
    first = a0 + a1 * (1.0 + beta)
    both = jnp.concatenate([first, a0 * a1, jnp.zeros((6, LANES), F32)], 0).T
    for i in range(2):
        coef_ref[i] = jnp.broadcast_to(both[:pairs, i:i + 1], (pairs, LANES))


def combine_kernel(coef_ref, r0_ref, q_ref, w_ref, z_ref, y_ref, sol_hbm, res_hbm, sol_ref, res_ref, sem):
    rows, pairs, cols = sol_ref.shape
    mine = pl.ds(0, pairs)

    def out(r, src, dst, k):
        return pltpu.make_async_copy(src.at[r], dst.at[mine, r], sem.at[k, r])

    def body(r, carry):
        one, two = coef_ref[0], coef_ref[1]
        for c in range(cols // LANES):
            cut = slice(c * LANES, (c + 1) * LANES)
            sol_ref[r, :, cut] = one * q_ref[r, mine, cut] - two * z_ref[r, mine, cut]
            res_ref[r, :, cut] = r0_ref[r, mine, cut] - one * w_ref[r, mine, cut] + two * y_ref[r, mine, cut]
        out(r, sol_ref, sol_hbm, 0).start()
        out(r, res_ref, res_hbm, 1).start()
        return carry

    lax.fori_loop(0, rows, body, 0)

    def finish(r, carry):
        out(r, sol_ref, sol_hbm, 0).wait()
        out(r, res_ref, res_hbm, 1).wait()
        return carry

    lax.fori_loop(0, rows, finish, 0)


def on_device(count, cond, nodata, gmask, gval, smask, scur, tinv, focal):
    rows, cols = cond.shape
    pairs = focal.shape[0]
    tiles = cols // LANES
    ext = pairs + EXTRA
    field = jax.ShapeDtypeStruct((rows, ext, cols), F32)
    vm = pl.BlockSpec(memory_space=pltpu.VMEM)
    hbm = pl.BlockSpec(memory_space=pltpu.HBM)
    msg = (2, 2 * pairs, LANES)
    bmsg = (2, 3 * tiles, LANES)
    tmsg = (2, 2 * tiles, LANES)
    zmsg = (2, 2 * pairs + tiles, LANES)
    others = count - 1
    r0, q, w, z, y, coef = pl.pallas_call(
        functools.partial(krylov_kernel, count),
        out_shape=[field] * 5 + [jax.ShapeDtypeStruct((2, pairs, LANES), F32)],
        in_specs=[hbm] * 8,
        out_specs=[vm] * 6,
        scratch_shapes=[
            pltpu.VMEM((3, rows, cols), F32),
            pltpu.VMEM((3, rows, cols), jnp.int32),
            pltpu.VMEM((2, pairs), jnp.int32),
            pltpu.SMEM((2, pairs), jnp.int32),
            pltpu.VMEM((2, cols, LANES), F32),
            pltpu.VMEM((rows - 2, cols, LANES), F32),
            pltpu.VMEM((rows, tiles, LANES, 2 * LANES), BF16),
            pltpu.VMEM((rows, 8, cols), F32),
            pltpu.VMEM((2, pairs, LANES), F32),
            pltpu.VMEM((2, pairs, cols), F32),
            pltpu.VMEM((2, pairs, cols), F32),
            *[pltpu.VMEM(shape, F32) for shape in (msg, bmsg, tmsg, zmsg) for _ in range(2)],
            pltpu.VMEM((4, pairs, LANES), F32),
            *[pltpu.VMEM(shape, F32) for _ in range(2) for shape in ((8, LANES), (others, 8, LANES))],
            *[pltpu.SemaphoreType.DMA((2,))] * 8,
            *[pltpu.SemaphoreType.DMA] * 4,
            pltpu.SemaphoreType.DMA((6,)),
            pltpu.SemaphoreType.REGULAR,
        ],
        compiler_params=pltpu.CompilerParams(
            collective_id=0, has_side_effects=True, vmem_limit_bytes=36 * 1024 * 1024
        ),
        name="krylov",
    )(*(
        pltpu.with_memory_space_constraint(x, pltpu.HBM)
        for x in (cond, nodata, gmask, gval, smask, scur, tinv.reshape(rows, cols, LANES), focal.T)
    ))

    out = jax.ShapeDtypeStruct((pairs, rows, cols), F32)
    return tuple(pl.pallas_call(
        combine_kernel,
        out_shape=[out, out],
        in_specs=[vm] * 6,
        out_specs=[hbm, hbm],
        scratch_shapes=[
            pltpu.VMEM((rows, pairs, cols), F32),
            pltpu.VMEM((rows, pairs, cols), F32),
            pltpu.SemaphoreType.DMA((2, rows)),
        ],
        compiler_params=pltpu.CompilerParams(vmem_limit_bytes=20 * 1024 * 1024),
        name="combine",
    )(coef, r0, q, w, z, y))


def solution(mesh):
    return jax.shard_map(
        functools.partial(on_device, mesh.shape["space"]),
        mesh=mesh,
        in_specs=(
            P(("groups", "space"), None),
            P(("groups", "space"), None),
            P(("groups", "space"), None),
            P(("groups", "space"), None),
            P(("groups", "space"), None),
            P(("groups", "space"), None),
            P(("groups", "space"), None, None, None),
            P(("groups", "rhs"), None),
        ),
        out_specs=(P("rhs", ("groups", "space"), None), P("rhs", ("groups", "space"), None)),
        check_vma=False,
    )
```

```python
import functools

import jax
import jax.numpy as jnp
from jax import lax
from jax.experimental import pallas as pl
from jax.experimental.pallas import tpu as pltpu
from jax.sharding import PartitionSpec as P

LEAKAGE = 0.05
FOCAL_CURRENT = 16.0
LANES = 128
EXTRA = 8
F32 = jnp.float32
BF16 = jnp.bfloat16


def krylov_kernel(
    count, cond_hbm, nodata_hbm, gmask_hbm, gval_hbm, smask_hbm, scur_hbm, t_hbm, focal_hbm,
    r0_ref, q_ref, w_ref, z_ref, y_ref, coef_ref,
    reals_ref, flags_ref, focal_ref, ids_ref, te_ref, ti_ref,
    thl_ref, wts_ref, spot_ref, qhalo_ref, zhalo_ref, msg_ref, got_ref, bmsg_ref, bgot_ref, tmsg_ref, tgot_ref,
    zmsg_ref, zgot_ref, acc_ref, stat_ref, all_ref, late_ref, lates_ref,
    send1, recv1, sendb, recvb, sendt, recvt, send2, recv2, send3, recv3, send4, recv4, sem_in, hello,
):
    rows, cols = reals_ref.shape[1:]
    tiles = cols // LANES
    pairs = focal_ref.shape[1]
    ext = pairs + EXTRA
    me = lax.axis_index("space")
    last = count - 1
    ends = ((0, 0), (1, rows - 1))
    inner = range(1, rows - 1)
    cuts = [slice(c * LANES, (c + 1) * LANES) for c in range(tiles)]

    has = (me > 0, me < last)
    few = count <= 4
    barrier = pltpu.get_barrier_semaphore()
    lates_ref[...] = jnp.zeros(lates_ref.shape, F32)

    def greet(sem):
        for side in range(2):
            @pl.when(has[side])
            def _():
                pl.semaphore_signal(
                    sem, inc=1, device_id={"space": me - 1 if side == 0 else me + 1},
                    device_id_type=pl.DeviceIdType.MESH,
                )

    def greeted(sem):
        pl.semaphore_wait(sem, jnp.minimum(me, 1) + jnp.minimum(last - me, 1))

    if few:
        greet(barrier)
    else:
        for off in range(1, count):
            pl.semaphore_signal(
                barrier, inc=1, device_id={"space": lax.rem(me + off, count)},
                device_id_type=pl.DeviceIdType.MESH,
            )

    def whole(ref, i):
        return pltpu.make_async_copy(ref, ref, sem_in.at[i])

    ids_load = pltpu.make_async_copy(focal_hbm, ids_ref, sem_in.at[0])
    focal_load = pltpu.make_async_copy(focal_hbm, focal_ref, sem_in.at[1])
    inner_load = pltpu.make_async_copy(t_hbm.at[pl.ds(1, rows - 2)], ti_ref, sem_in.at[5])
    ids_load.start()
    focal_load.start()
    for side, r in ends:
        for cut in cuts:
            pltpu.make_async_copy(
                t_hbm.at[r, pl.ds(cut.start, LANES)], te_ref.at[side, pl.ds(cut.start, LANES)], sem_in.at[2]).start()
    for i, group in ((3, (cond_hbm, gval_hbm, scur_hbm)), (4, (nodata_hbm, gmask_hbm, smask_hbm))):
        for k, src in enumerate(group):
            pltpu.make_async_copy(src, (reals_ref, flags_ref)[i - 3].at[k], sem_in.at[i]).start()
    inner_load.start()
    ids_load.wait()
    focal_load.wait()
    whole(te_ref, 2).wait()

    def gather(src, at):
        for p in range(pairs):
            for i in range(2):
                r, k = at(ids_ref[i, p])
                spot_ref[i, p:p + 1, :] = src[r, pl.ds(k, 1), :]
        return FOCAL_CURRENT * spot_ref[0], -FOCAL_CURRENT * spot_ref[1]

    half, high = (rows * cols // 2).bit_length() - 1, cols.bit_length() - 1
    near_a, near_b = gather(
        te_ref, lambda i: (lax.shift_right_logical(i, half) & 1, i & (cols - 1)))

    diagonal = lax.broadcasted_iota(jnp.int32, (pairs, pairs), 0) == lax.broadcasted_iota(
        jnp.int32, (pairs, pairs), 1)
    lane = lax.broadcasted_iota(jnp.int32, (pairs, LANES), 1)

    def column(i):
        line = jnp.broadcast_to(focal_ref[i:i + 1, :].astype(F32), (pairs, pairs))
        return jnp.broadcast_to(
            jnp.sum(jnp.where(diagonal, line, 0.0), 1, keepdims=True).astype(jnp.int32), (pairs, LANES))

    at_a, at_b = (column(i) - me * (rows * cols) for i in range(2))
    spot_a, spot_b = (lax.shift_right_arithmetic(x, 7) for x in (at_a, at_b))
    tile_a, tile_b = spot_a & (tiles - 1), spot_b & (tiles - 1)

    def within(spot, low, high):
        return jnp.logical_and(spot >= low * tiles, spot < high * tiles)

    for side, r in ends:
        msg_ref[side, 0:pairs, :] = jnp.where(within(spot_a, r, r + 1), near_a, 0.0)
        msg_ref[side, pairs:2 * pairs, :] = jnp.where(within(spot_b, r, r + 1), near_b, 0.0)

    def side_copy(src, dst, ssem, rsem, side):
        return pltpu.make_async_remote_copy(
            src_ref=src.at[side], dst_ref=dst.at[1 - side],
            send_sem=ssem.at[side], recv_sem=rsem.at[1 - side],
            device_id={"space": me - 1 if side == 0 else me + 1},
            device_id_type=pl.DeviceIdType.MESH,
        )

    def send(src, dst, ssem, rsem):
        for side in range(2):
            @pl.when(has[side])
            def _():
                side_copy(src, dst, ssem, rsem, side).start()

            @pl.when(jnp.logical_not(has[side]))
            def _():
                dst[side] = jnp.zeros(dst.shape[1:], F32)

    def done(src, dst, ssem, rsem):
        for side in range(2):
            @pl.when(has[side])
            def _():
                side_copy(src, dst, ssem, rsem, side).wait_send()
                pltpu.make_async_remote_copy(
                    src_ref=src.at[1 - side], dst_ref=dst.at[side],
                    send_sem=ssem.at[1 - side], recv_sem=rsem.at[side],
                    device_id={"space": me - 1 if side == 0 else me + 1},
                    device_id_type=pl.DeviceIdType.MESH,
                ).wait_recv()

    if few:
        greeted(barrier)
    else:
        pl.semaphore_wait(barrier, last)
    send(msg_ref, got_ref, send1, recv1)

    whole(reals_ref, 3).wait()
    whole(flags_ref, 4).wait()
    valid = (1 - flags_ref[0]).astype(F32)
    active = reals_ref[0] * valid
    background = flags_ref[2].astype(F32) * reals_ref[2]

    def tile_of(r, c):
        if r == 0 or r == rows - 1:
            return te_ref[min(r, 1), cuts[c], :]
        return ti_ref[r - 1, cuts[c], :]

    def product(x, r, c):
        number = x.shape[0]
        hi = x.astype(BF16).astype(F32)
        lhs = jnp.concatenate([hi, x - hi], 0).astype(BF16)
        o = jnp.dot(lhs, thl_ref[r, c], preferred_element_type=F32)
        return o[:number, :LANES] + (o[:number, LANES:] + (o[number:, :LANES] + o[number:, LANES:]))

    def shared_row(r):
        dot = jnp.zeros((EXTRA, LANES), F32)
        for c, cut in enumerate(cuts):
            t = tile_of(r, c)
            thi = t.astype(BF16)
            thl_ref[r, c, :, :LANES] = thi
            thl_ref[r, c, :, LANES:] = (t - thi.astype(F32)).astype(BF16)
            x = jnp.broadcast_to(background[r:r + 1, cut], (EXTRA, LANES))
            q = product(x, r, c)
            q_ref[r, pairs:ext, cut] = q
            dot = dot + x * q
        return dot

    shared = shared_row(0) + shared_row(rows - 1)
    for side, r in ends:
        for c, cut in enumerate(cuts):
            bmsg_ref[side, c:c + 1, :] = q_ref[r, pairs:pairs + 1, cut]
            bmsg_ref[side, tiles + c:tiles + c + 1, :] = active[r:r + 1, cut]
            bmsg_ref[side, 2 * tiles + c:2 * tiles + c + 1, :] = valid[r:r + 1, cut]
            tmsg_ref[side, c:c + 1, :] = te_ref[side, cut.start:cut.start + 1, :]
            tmsg_ref[side, tiles + c:tiles + c + 1, :] = te_ref[side, cut.stop - 1:cut.stop, :]
    send(bmsg_ref, bgot_ref, sendb, recvb)
    send(tmsg_ref, tgot_ref, sendt, recvt)

    def edge(a, b, v, u):
        return 0.5 * (a + b) * v * u

    row_at = lax.broadcasted_iota(jnp.int32, (rows, cols), 0)
    col_at = lax.broadcasted_iota(jnp.int32, (rows, cols), 1)

    def shifted(x, by, axis):
        length = x.shape[axis]
        at = (row_at, col_at)[axis][:x.shape[0], :]
        return jnp.where(at == (0 if by == 1 else length - 1), 0.0, pltpu.roll(x, by % length, axis))

    nw, sw, ww, ew = (
        edge(active, shifted(active, *how), valid, shifted(valid, *how))
        for how in ((1, 0), (-1, 0), (1, 1), (-1, 1))
    )
    dg = valid * (LEAKAGE + flags_ref[1].astype(F32) * reals_ref[1]) + (1.0 - valid) + nw + sw + ww + ew
    for r in range(rows):
        for i, x in enumerate((dg, nw, sw, ww, ew, 0.5 * dg, background)):
            wts_ref[r, i:i + 1, :] = x[r:r + 1, :]

    inner_load.wait()
    far_a, far_b = gather(
        ti_ref, lambda i: (
            jnp.clip((lax.shift_right_logical(i, high) & (rows - 1)) - 1, 0, rows - 3), i & (cols - 1)))
    for r in inner:
        shared = shared + shared_row(r)

    def dense_row(r, a, b, dot):
        for c, cut in enumerate(cuts):
            k = r * tiles + c
            x = jnp.where(spot_a == k, a, 0.0) + jnp.where(spot_b == k, b, 0.0)
            q_ref[r, 0:pairs, cut] = q_ref[r, pairs:pairs + 1, cut] + x
            dot = dot + background[r:r + 1, cut] * x
        return dot

    dot = jnp.zeros((pairs, LANES), F32)
    for r in range(rows):
        a, b = (far_a, far_b) if r in inner else (near_a, near_b)
        dot = dense_row(r, a, b, dot)
    in_a, in_b = (
        jnp.where(within(spot, 1, rows - 1), far, jnp.where(within(spot, 0, rows), near, 0.0))
        for spot, far, near in ((spot_a, far_a, near_a), (spot_b, far_b, near_b))
    )
    same = spot_a == spot_b
    own = jnp.where(lane == (at_a & (LANES - 1)), in_a + jnp.where(same, in_b, 0.0), 0.0) - jnp.where(
        lane == (at_b & (LANES - 1)), in_b + jnp.where(same, in_a, 0.0), 0.0)
    acc_ref[0] = 2.0 * dot + FOCAL_CURRENT * own + jnp.broadcast_to(shared[0:1, :], dot.shape)
    for i in range(1, 4):
        acc_ref[i] = jnp.zeros(acc_ref.shape[1:], F32)

    parts = [slice(p, p + 16) for p in range(0, pairs, 16)]
    extra = slice(pairs, ext)

    def stream(src, r, s, east=True):
        at = lane[:s.stop - s.start]
        x = src[r, s, cuts[0]]
        gone, west, ahead = None, pltpu.roll(x, 1, 1), east and pltpu.roll(x, LANES - 1, 1)
        for c in range(tiles):
            more = c + 1 < tiles
            if more:
                y = src[r, s, cuts[c + 1]]
                after = east and pltpu.roll(y, LANES - 1, 1)
            yield (
                c, cuts[c], x, west if gone is None else jnp.where(at == 0, gone, west),
                jnp.where(at == LANES - 1, after, ahead) if east and more else ahead,
            )
            if more:
                x, gone, west, ahead = y, west, pltpu.roll(y, 1, 1), after

    def apply_part(src, dst, r, s, north, south, acc=None):
        dots = None
        for c, cut, x, west, east in stream(src, r, s):
            out = wts_ref[r, 0:1, cut] * x - wts_ref[r, 3:4, cut] * west - wts_ref[r, 4:5, cut] * east
            if north is not None:
                out = out - wts_ref[r, 1:2, cut] * north[0][north[1], s, cut]
            if south is not None:
                out = out - wts_ref[r, 2:3, cut] * south[0][south[1], s, cut]
            dst[r, s, cut] = out
            dots = x * out if dots is None else dots + x * out
        if acc is not None:
            acc_ref[acc, s, :] += dots

    def apply_inner(src, dst):
        def body(r, carry):
            for s in parts:
                apply_part(src, dst, r, s, (src, r - 1), (src, r + 1))
            return carry
        lax.fori_loop(1, rows - 1, body, 0)

    for s in (*parts, extra):
        apply_part(q_ref, w_ref, 0, s, None, (q_ref, 1))
        apply_part(q_ref, w_ref, rows - 1, s, (q_ref, rows - 2), None)

    done(msg_ref, got_ref, send1, recv1)
    if few:
        greet(hello)
    done(bmsg_ref, bgot_ref, sendb, recvb)

    def row_of(side, base):
        return jnp.concatenate([bgot_ref[side, base + c:base + c + 1, :] for c in range(tiles)], 1)

    halo_a = [row_of(side, tiles) for side in range(2)]
    halo_v = [row_of(side, 2 * tiles) for side in range(2)]
    for side, r in ends:
        i = 1 + side
        h = edge(active[r:r + 1, :], halo_a[side], valid[r:r + 1, :], halo_v[side])
        wts_ref[r, i:i + 1, :] = h
        wts_ref[r, 0:1, :] += h
        wts_ref[r, 5:6, :] += 0.5 * h
        va = got_ref[side, 0:pairs, :]
        vb = got_ref[side, pairs:2 * pairs, :]
        dots = jnp.zeros((pairs, LANES), F32)
        for c, cut in enumerate(cuts):
            common = bgot_ref[side, c:c + 1, :]
            qh = jnp.where(tile_a == c, va, 0.0) + jnp.where(tile_b == c, vb, 0.0)
            qhalo_ref[side, :, cut] = qh
            q0 = q_ref[r, :pairs, cut]
            w0 = w_ref[r, :pairs, cut] + h[:, cut] * (q0 - (qh + common))
            w_ref[r, :pairs, cut] = w0
            w_ref[r, extra, cut] += h[:, cut] * (q_ref[r, extra, cut] - common)
            dots = dots + q0 * w0
        acc_ref[1] += dots

    def precond_row(r):
        for c, cut in enumerate(cuts):
            z_ref[r, :, cut] = product(w_ref[r, :, cut], r, c)

    def pack(src, r, dst, side):
        va = src[r, :pairs, 0:LANES]
        vb = va
        for c in range(1, tiles):
            x = src[r, :pairs, cuts[c]]
            va = jnp.where(tile_a == c, x, va)
            vb = jnp.where(tile_b == c, x, vb)
        dst[side, 0:pairs, :] = va
        dst[side, pairs:2 * pairs, :] = vb
        for c, cut in enumerate(cuts):
            dst[side, 2 * pairs + c:2 * pairs + c + 1, :] = src[r, pairs:pairs + 1, cut]

    precond_row(0)
    precond_row(rows - 1)
    for side, r in ends:
        pack(z_ref, r, zmsg_ref, side)
    send(zmsg_ref, zgot_ref, send2, recv2)


    def moment_part(r, s, north):
        mu = nu = None
        for c, cut, z, west, _ in stream(z_ref, r, s, False):
            t = wts_ref[r, 5:6, cut] * z - wts_ref[r, 3:4, cut] * west
            if north:
                t = t - wts_ref[r, 1:2, cut] * z_ref[r - 1, s, cut]
            one, two = w_ref[r, s, cut] * z, t * z
            mu, nu = (one, two) if mu is None else (mu + one, nu + two)
        acc_ref[2, s, :] += mu
        acc_ref[3, s, :] += nu

    def image_row(r):
        for s in parts:
            apply_part(q_ref, w_ref, r, s, (q_ref, r - 1), (q_ref, r + 1), 1)
        apply_part(q_ref, w_ref, r, extra, (q_ref, r - 1), (q_ref, r + 1))

    def moment_row(r):
        for s in parts:
            moment_part(r, s, r > 0)

    image_row(1)
    for r in inner:
        if r + 1 in inner:
            image_row(r + 1)
        precond_row(r)
        moment_row(r - 1)
    moment_row(rows - 2)
    moment_row(rows - 1)

    pad = jnp.zeros((8, LANES - pairs), F32)

    def lines(sums):
        table = jnp.zeros((pairs, LANES), F32)
        for i, x in enumerate(sums):
            table = jnp.where(lane == i, jnp.sum(x, 1, keepdims=True), table)
        return jnp.concatenate([table.T[0:8, :], pad], 1)

    def exchange(src, dst, ssem, rsem):
        for k in range(1, count):
            pltpu.make_async_remote_copy(
                src_ref=src, dst_ref=dst.at[k - 1], send_sem=ssem, recv_sem=rsem,
                device_id={"space": lax.rem(me + k, count)}, device_id_type=pl.DeviceIdType.MESH,
            ).start()

    def arrived(dst, ssem, rsem):
        for sem in (ssem, rsem):
            pltpu.make_async_copy(dst, dst, sem).wait()

    early = lines([acc_ref[i] for i in range(4)])
    stat_ref[...] = early
    if few:
        greeted(hello)
    exchange(stat_ref, all_ref, send3, recv3)

    done(tmsg_ref, tgot_ref, sendt, recvt)
    for side in range(2):
        halo_w, halo_e = (
            edge(halo_a[side], shifted(halo_a[side], by, 1), halo_v[side], shifted(halo_v[side], by, 1))
            for by in (1, -1)
        )
        near = [jnp.zeros((pairs, LANES), F32)] * tiles
        for c, cut in enumerate(cuts):
            qh = qhalo_ref[side, :, cut]
            if c > 0:
                gone = (halo_w[:, cut] * qh)[:, 0:1]
                near[c - 1] = near[c - 1] - gone * tgot_ref[side, tiles + c - 1:tiles + c, :]
            if c < tiles - 1:
                gone = (halo_e[:, cut] * qh)[:, LANES - 1:LANES]
                near[c + 1] = near[c + 1] - gone * tgot_ref[side, c + 1:c + 2, :]
        for c, cut in enumerate(cuts):
            zhalo_ref[side, :, cut] = near[c]

    done(zmsg_ref, zgot_ref, send2, recv2)
    coupling = []
    for side, r in ends:
        va = zgot_ref[side, 0:pairs, :]
        vb = zgot_ref[side, pairs:2 * pairs, :]
        total = jnp.zeros((pairs, LANES), F32)
        for c, cut in enumerate(cuts):
            other = zgot_ref[side, 2 * pairs + c:2 * pairs + c + 1, :] + zhalo_ref[side, :, cut]
            zh = jnp.where(tile_a == c, va, jnp.where(tile_b == c, vb, other))
            zhalo_ref[side, :, cut] = zh
            total = total + wts_ref[r, 1 + side:2 + side, cut] * z_ref[r, :pairs, cut] * zh
        coupling.append(total)
    late = lines(coupling)
    late_ref[...] = late
    def late_copy(k):
        return pltpu.make_async_remote_copy(
            src_ref=late_ref, dst_ref=lates_ref.at[k - 1], send_sem=send4.at[k - 1], recv_sem=recv4.at[k - 1],
            device_id={"space": lax.rem(me + k, count)}, device_id_type=pl.DeviceIdType.MESH,
        )

    def gives(who, k):
        up = who + k < count
        return jnp.logical_or(jnp.logical_and(up, who > 0), jnp.logical_and(jnp.logical_not(up), who < last))

    for k in range(1, count):
        @pl.when(gives(me, k))
        def _():
            late_copy(k).start()

    apply_inner(z_ref, y_ref)
    for s in parts:
        apply_part(z_ref, y_ref, 0, s, (zhalo_ref, 0), (z_ref, 1))
        apply_part(z_ref, y_ref, rows - 1, s, (z_ref, rows - 2), (zhalo_ref, 1))

    def right_side(r, carry):
        for c, cut in enumerate(cuts):
            local = r * cols + c * LANES + lane
            x = jnp.where(local == at_a, FOCAL_CURRENT, 0.0) - jnp.where(local == at_b, FOCAL_CURRENT, 0.0)
            r0_ref[r, 0:pairs, cut] = wts_ref[r, 6:7, cut] + x
        return carry

    lax.fori_loop(0, rows, right_side, 0)

    arrived(all_ref, send3, recv3)
    total = early
    for k in range(1, count):
        total = total + all_ref[k - 1]
    gamma0, kappa, mu, part = (total[i:i + 1, :] for i in range(4))
    a0 = gamma0 / kappa
    gamma1 = a0 * a0 * mu - gamma0
    beta = gamma1 / gamma0
    known = kappa - 2.0 * a0 * mu - beta * gamma1 / a0 + 2.0 * a0 * a0 * part
    scale = 2.0 * a0 * a0
    joint = late[0:1, :] + late[1:2, :]
    for k in range(1, count):
        @pl.when(gives(me, k))
        def _():
            late_copy(k).wait_send()

        @pl.when(gives(lax.rem(me - k + count, count), k))
        def _():
            late_copy(k).wait_recv()
    for k in range(1, count):
        joint = joint + jnp.where(k <= me, lates_ref[k - 1, 0:1, :], lates_ref[k - 1, 1:2, :])
    a1 = gamma1 / (known - scale * joint)
    first = a0 + a1 * (1.0 + beta)
    both = jnp.concatenate([first, a0 * a1, jnp.zeros((6, LANES), F32)], 0).T
    for i in range(2):
        coef_ref[i] = jnp.broadcast_to(both[:pairs, i:i + 1], (pairs, LANES))


def combine_kernel(coef_ref, r0_ref, q_ref, w_ref, z_ref, y_ref, sol_hbm, res_hbm, sol_ref, res_ref, sem):
    rows, pairs, cols = sol_ref.shape
    mine = pl.ds(0, pairs)

    def out(r, src, dst, k):
        return pltpu.make_async_copy(src.at[r], dst.at[mine, r], sem.at[k, r])

    def body(r, carry):
        one, two = coef_ref[0], coef_ref[1]
        for c in range(cols // LANES):
            cut = slice(c * LANES, (c + 1) * LANES)
            sol_ref[r, :, cut] = one * q_ref[r, mine, cut] - two * z_ref[r, mine, cut]
            res_ref[r, :, cut] = r0_ref[r, mine, cut] - one * w_ref[r, mine, cut] + two * y_ref[r, mine, cut]
        out(r, sol_ref, sol_hbm, 0).start()
        out(r, res_ref, res_hbm, 1).start()
        return carry

    lax.fori_loop(0, rows, body, 0)

    def finish(r, carry):
        out(r, sol_ref, sol_hbm, 0).wait()
        out(r, res_ref, res_hbm, 1).wait()
        return carry

    lax.fori_loop(0, rows, finish, 0)


def on_device(count, cond, nodata, gmask, gval, smask, scur, tinv, focal):
    rows, cols = cond.shape
    pairs = focal.shape[0]
    tiles = cols // LANES
    ext = pairs + EXTRA
    field = jax.ShapeDtypeStruct((rows, ext, cols), F32)
    vm = pl.BlockSpec(memory_space=pltpu.VMEM)
    hbm = pl.BlockSpec(memory_space=pltpu.HBM)
    msg = (2, 2 * pairs, LANES)
    bmsg = (2, 3 * tiles, LANES)
    tmsg = (2, 2 * tiles, LANES)
    zmsg = (2, 2 * pairs + tiles, LANES)
    others = count - 1
    r0, q, w, z, y, coef = pl.pallas_call(
        functools.partial(krylov_kernel, count),
        out_shape=[field] * 5 + [jax.ShapeDtypeStruct((2, pairs, LANES), F32)],
        in_specs=[hbm] * 8,
        out_specs=[vm] * 6,
        scratch_shapes=[
            pltpu.VMEM((3, rows, cols), F32),
            pltpu.VMEM((3, rows, cols), jnp.int32),
            pltpu.VMEM((2, pairs), jnp.int32),
            pltpu.SMEM((2, pairs), jnp.int32),
            pltpu.VMEM((2, cols, LANES), F32),
            pltpu.VMEM((rows - 2, cols, LANES), F32),
            pltpu.VMEM((rows, tiles, LANES, 2 * LANES), BF16),
            pltpu.VMEM((rows, 8, cols), F32),
            pltpu.VMEM((2, pairs, LANES), F32),
            pltpu.VMEM((2, pairs, cols), F32),
            pltpu.VMEM((2, pairs, cols), F32),
            *[pltpu.VMEM(shape, F32) for shape in (msg, bmsg, tmsg, zmsg) for _ in range(2)],
            pltpu.VMEM((4, pairs, LANES), F32),
            *[pltpu.VMEM(shape, F32) for _ in range(2) for shape in ((8, LANES), (others, 8, LANES))],
            *[pltpu.SemaphoreType.DMA((2,))] * 8,
            *[pltpu.SemaphoreType.DMA] * 2,
            *[pltpu.SemaphoreType.DMA((others,))] * 2,
            pltpu.SemaphoreType.DMA((6,)),
            pltpu.SemaphoreType.REGULAR,
        ],
        compiler_params=pltpu.CompilerParams(
            collective_id=0, has_side_effects=True, vmem_limit_bytes=36 * 1024 * 1024
        ),
        name="krylov",
    )(*(
        pltpu.with_memory_space_constraint(x, pltpu.HBM)
        for x in (cond, nodata, gmask, gval, smask, scur, tinv.reshape(rows, cols, LANES), focal.T)
    ))

    out = jax.ShapeDtypeStruct((pairs, rows, cols), F32)
    return tuple(pl.pallas_call(
        combine_kernel,
        out_shape=[out, out],
        in_specs=[vm] * 6,
        out_specs=[hbm, hbm],
        scratch_shapes=[
            pltpu.VMEM((rows, pairs, cols), F32),
            pltpu.VMEM((rows, pairs, cols), F32),
            pltpu.SemaphoreType.DMA((2, rows)),
        ],
        compiler_params=pltpu.CompilerParams(vmem_limit_bytes=20 * 1024 * 1024),
        name="combine",
    )(coef, r0, q, w, z, y))


def solution(mesh):
    return jax.shard_map(
        functools.partial(on_device, mesh.shape["space"]),
        mesh=mesh,
        in_specs=(
            P(("groups", "space"), None),
            P(("groups", "space"), None),
            P(("groups", "space"), None),
            P(("groups", "space"), None),
            P(("groups", "space"), None),
            P(("groups", "space"), None),
            P(("groups", "space"), None, None, None),
            P(("groups", "rhs"), None),
        ),
        out_specs=(P("rhs", ("groups", "space"), None), P("rhs", ("groups", "space"), None)),
        check_vma=False,
    )
```

```python
import functools

import jax
import jax.numpy as jnp
from jax import lax
from jax.experimental import pallas as pl
from jax.experimental.pallas import tpu as pltpu
from jax.sharding import PartitionSpec as P

LEAKAGE = 0.05
FOCAL_CURRENT = 16.0
LANES = 128
EXTRA = 8
F32 = jnp.float32
BF16 = jnp.bfloat16


def krylov_kernel(
    count, cond_hbm, nodata_hbm, gmask_hbm, gval_hbm, smask_hbm, scur_hbm, t_hbm, focal_hbm,
    r0_ref, q_ref, w_ref, z_ref, y_ref, coef_ref,
    reals_ref, flags_ref, focal_ref, ids_ref, te_ref, ti_ref,
    thl_ref, wts_ref, spot_ref, qhalo_ref, zhalo_ref, msg_ref, got_ref, bmsg_ref, bgot_ref, tmsg_ref, tgot_ref,
    zmsg_ref, zgot_ref, acc_ref, stat_ref, all_ref, late_ref, lates_ref,
    send1, recv1, sendb, recvb, sendt, recvt, send2, recv2, send3, recv3, send4, recv4, sem_in, hello,
):
    rows, cols = reals_ref.shape[1:]
    tiles = cols // LANES
    pairs = focal_ref.shape[1]
    ext = pairs + EXTRA
    me = lax.axis_index("space")
    last = count - 1
    ends = ((0, 0), (1, rows - 1))
    inner = range(1, rows - 1)
    cuts = [slice(c * LANES, (c + 1) * LANES) for c in range(tiles)]

    has = (me > 0, me < last)
    few = count <= 4
    barrier = pltpu.get_barrier_semaphore()
    lates_ref[...] = jnp.zeros(lates_ref.shape, F32)

    def greet(sem):
        for side in range(2):
            @pl.when(has[side])
            def _():
                pl.semaphore_signal(
                    sem, inc=1, device_id={"space": me - 1 if side == 0 else me + 1},
                    device_id_type=pl.DeviceIdType.MESH,
                )

    def greeted(sem):
        pl.semaphore_wait(sem, jnp.minimum(me, 1) + jnp.minimum(last - me, 1))

    if few:
        greet(barrier)
    else:
        for off in range(1, count):
            pl.semaphore_signal(
                barrier, inc=1, device_id={"space": lax.rem(me + off, count)},
                device_id_type=pl.DeviceIdType.MESH,
            )

    def whole(ref, i):
        return pltpu.make_async_copy(ref, ref, sem_in.at[i])

    ids_load = pltpu.make_async_copy(focal_hbm, ids_ref, sem_in.at[0])
    focal_load = pltpu.make_async_copy(focal_hbm, focal_ref, sem_in.at[1])
    inner_load = pltpu.make_async_copy(t_hbm.at[pl.ds(1, rows - 2)], ti_ref, sem_in.at[5])
    ids_load.start()
    focal_load.start()
    for side, r in ends:
        for cut in cuts:
            pltpu.make_async_copy(
                t_hbm.at[r, pl.ds(cut.start, LANES)], te_ref.at[side, pl.ds(cut.start, LANES)], sem_in.at[2]).start()
    for i, group in ((3, (cond_hbm, gval_hbm, scur_hbm)), (4, (nodata_hbm, gmask_hbm, smask_hbm))):
        for k, src in enumerate(group):
            pltpu.make_async_copy(src, (reals_ref, flags_ref)[i - 3].at[k], sem_in.at[i]).start()
    inner_load.start()
    ids_load.wait()
    focal_load.wait()
    whole(te_ref, 2).wait()

    def gather(src, at):
        for p in range(pairs):
            for i in range(2):
                r, k = at(ids_ref[i, p])
                spot_ref[i, p:p + 1, :] = src[r, pl.ds(k, 1), :]
        return FOCAL_CURRENT * spot_ref[0], -FOCAL_CURRENT * spot_ref[1]

    half, high = (rows * cols // 2).bit_length() - 1, cols.bit_length() - 1
    near_a, near_b = gather(
        te_ref, lambda i: (lax.shift_right_logical(i, half) & 1, i & (cols - 1)))

    diagonal = lax.broadcasted_iota(jnp.int32, (pairs, pairs), 0) == lax.broadcasted_iota(
        jnp.int32, (pairs, pairs), 1)
    lane = lax.broadcasted_iota(jnp.int32, (pairs, LANES), 1)

    def column(i):
        line = jnp.broadcast_to(focal_ref[i:i + 1, :].astype(F32), (pairs, pairs))
        return jnp.broadcast_to(
            jnp.sum(jnp.where(diagonal, line, 0.0), 1, keepdims=True).astype(jnp.int32), (pairs, LANES))

    at_a, at_b = (column(i) - me * (rows * cols) for i in range(2))
    spot_a, spot_b = (lax.shift_right_arithmetic(x, 7) for x in (at_a, at_b))
    tile_a, tile_b = spot_a & (tiles - 1), spot_b & (tiles - 1)

    def within(spot, low, high):
        return jnp.logical_and(spot >= low * tiles, spot < high * tiles)

    piece = pairs // 2
    halves = tuple(enumerate((slice(0, piece), slice(piece, pairs))))
    for side, r in ends:
        here_a = jnp.where(within(spot_a, r, r + 1), near_a, 0.0)
        here_b = jnp.where(within(spot_b, r, r + 1), near_b, 0.0)
        for h, s in halves:
            msg_ref[h, side, 0:piece, :] = here_a[s]
            msg_ref[h, side, piece:pairs, :] = here_b[s]

    def side_copy(src, dst, ssem, rsem, side, number):
        return pltpu.make_async_remote_copy(
            src_ref=src.at[side, pl.ds(0, number)], dst_ref=dst.at[1 - side, pl.ds(0, number)],
            send_sem=ssem.at[side], recv_sem=rsem.at[1 - side],
            device_id={"space": me - 1 if side == 0 else me + 1},
            device_id_type=pl.DeviceIdType.MESH,
        )

    def send(src, dst, ssem, rsem, number=None):
        number = number or src.shape[1]
        for side in range(2):
            @pl.when(has[side])
            def _():
                side_copy(src, dst, ssem, rsem, side, number).start()

            @pl.when(jnp.logical_not(has[side]))
            def _():
                dst[side] = jnp.zeros(dst.shape[1:], F32)

    def done(src, dst, ssem, rsem, number=None):
        number = number or src.shape[1]
        for side in range(2):
            @pl.when(has[side])
            def _():
                side_copy(src, dst, ssem, rsem, side, number).wait_send()
                pltpu.make_async_remote_copy(
                    src_ref=src.at[1 - side, pl.ds(0, number)], dst_ref=dst.at[side, pl.ds(0, number)],
                    send_sem=ssem.at[1 - side], recv_sem=rsem.at[side],
                    device_id={"space": me - 1 if side == 0 else me + 1},
                    device_id_type=pl.DeviceIdType.MESH,
                ).wait_recv()

    def ring(h):
        return msg_ref.at[h], got_ref.at[h], send1.at[h], recv1.at[h]

    def zring(h):
        return zmsg_ref.at[h], zgot_ref.at[h], send2.at[h], recv2.at[h], pairs + (0 if h else tiles)

    if few:
        greeted(barrier)
    else:
        pl.semaphore_wait(barrier, last)
    send(*ring(0))

    whole(reals_ref, 3).wait()
    whole(flags_ref, 4).wait()
    valid = (1 - flags_ref[0]).astype(F32)
    active = reals_ref[0] * valid
    background = flags_ref[2].astype(F32) * reals_ref[2]

    def tile_of(r, c):
        if r == 0 or r == rows - 1:
            return te_ref[min(r, 1), cuts[c], :]
        return ti_ref[r - 1, cuts[c], :]

    def product(x, r, c):
        number = x.shape[0]
        hi = x.astype(BF16).astype(F32)
        lhs = jnp.concatenate([hi, x - hi], 0).astype(BF16)
        o = jnp.dot(lhs, thl_ref[r, c], preferred_element_type=F32)
        return o[:number, :LANES] + (o[:number, LANES:] + (o[number:, :LANES] + o[number:, LANES:]))

    def shared_row(r):
        dot = jnp.zeros((EXTRA, LANES), F32)
        for c, cut in enumerate(cuts):
            t = tile_of(r, c)
            thi = t.astype(BF16)
            thl_ref[r, c, :, :LANES] = thi
            thl_ref[r, c, :, LANES:] = (t - thi.astype(F32)).astype(BF16)
            x = jnp.broadcast_to(background[r:r + 1, cut], (EXTRA, LANES))
            q = product(x, r, c)
            q_ref[r, pairs:ext, cut] = q
            dot = dot + x * q
        return dot

    shared = shared_row(0) + shared_row(rows - 1)
    for side, r in ends:
        for c, cut in enumerate(cuts):
            bmsg_ref[side, c:c + 1, :] = q_ref[r, pairs:pairs + 1, cut]
            bmsg_ref[side, tiles + c:tiles + c + 1, :] = active[r:r + 1, cut]
            bmsg_ref[side, 2 * tiles + c:2 * tiles + c + 1, :] = valid[r:r + 1, cut]
            tmsg_ref[side, c:c + 1, :] = te_ref[side, cut.start:cut.start + 1, :]
            tmsg_ref[side, tiles + c:tiles + c + 1, :] = te_ref[side, cut.stop - 1:cut.stop, :]
    send(bmsg_ref, bgot_ref, sendb, recvb)
    send(*ring(1))
    send(tmsg_ref, tgot_ref, sendt, recvt)

    def edge(a, b, v, u):
        return 0.5 * (a + b) * v * u

    row_at = lax.broadcasted_iota(jnp.int32, (rows, cols), 0)
    col_at = lax.broadcasted_iota(jnp.int32, (rows, cols), 1)

    def shifted(x, by, axis):
        length = x.shape[axis]
        at = (row_at, col_at)[axis][:x.shape[0], :]
        return jnp.where(at == (0 if by == 1 else length - 1), 0.0, pltpu.roll(x, by % length, axis))

    nw, sw, ww, ew = (
        edge(active, shifted(active, *how), valid, shifted(valid, *how))
        for how in ((1, 0), (-1, 0), (1, 1), (-1, 1))
    )
    dg = valid * (LEAKAGE + flags_ref[1].astype(F32) * reals_ref[1]) + (1.0 - valid) + nw + sw + ww + ew
    for r in range(rows):
        for i, x in enumerate((dg, nw, sw, ww, ew, 0.5 * dg, background)):
            wts_ref[r, i:i + 1, :] = x[r:r + 1, :]

    inner_load.wait()
    far_a, far_b = gather(
        ti_ref, lambda i: (
            jnp.clip((lax.shift_right_logical(i, high) & (rows - 1)) - 1, 0, rows - 3), i & (cols - 1)))
    for r in inner:
        shared = shared + shared_row(r)

    def dense_row(r, a, b, dot):
        for c, cut in enumerate(cuts):
            k = r * tiles + c
            x = jnp.where(spot_a == k, a, 0.0) + jnp.where(spot_b == k, b, 0.0)
            q_ref[r, 0:pairs, cut] = q_ref[r, pairs:pairs + 1, cut] + x
            dot = dot + background[r:r + 1, cut] * x
        return dot

    dot = jnp.zeros((pairs, LANES), F32)
    for r in range(rows):
        a, b = (far_a, far_b) if r in inner else (near_a, near_b)
        dot = dense_row(r, a, b, dot)
    in_a, in_b = (
        jnp.where(within(spot, 1, rows - 1), far, jnp.where(within(spot, 0, rows), near, 0.0))
        for spot, far, near in ((spot_a, far_a, near_a), (spot_b, far_b, near_b))
    )
    same = spot_a == spot_b
    own = jnp.where(lane == (at_a & (LANES - 1)), in_a + jnp.where(same, in_b, 0.0), 0.0) - jnp.where(
        lane == (at_b & (LANES - 1)), in_b + jnp.where(same, in_a, 0.0), 0.0)
    acc_ref[0] = 2.0 * dot + FOCAL_CURRENT * own + jnp.broadcast_to(shared[0:1, :], dot.shape)
    for i in range(1, 4):
        acc_ref[i] = jnp.zeros(acc_ref.shape[1:], F32)

    parts = [slice(p, p + 16) for p in range(0, pairs, 16)]
    extra = slice(pairs, ext)

    def stream(src, r, s, east=True):
        at = lane[:s.stop - s.start]
        x = src[r, s, cuts[0]]
        gone, west, ahead = None, pltpu.roll(x, 1, 1), east and pltpu.roll(x, LANES - 1, 1)
        for c in range(tiles):
            more = c + 1 < tiles
            if more:
                y = src[r, s, cuts[c + 1]]
                after = east and pltpu.roll(y, LANES - 1, 1)
            yield (
                c, cuts[c], x, west if gone is None else jnp.where(at == 0, gone, west),
                jnp.where(at == LANES - 1, after, ahead) if east and more else ahead,
            )
            if more:
                x, gone, west, ahead = y, west, pltpu.roll(y, 1, 1), after

    def apply_part(src, dst, r, s, north, south, acc=None):
        dots = None
        for c, cut, x, west, east in stream(src, r, s):
            out = wts_ref[r, 0:1, cut] * x - wts_ref[r, 3:4, cut] * west - wts_ref[r, 4:5, cut] * east
            if north is not None:
                out = out - wts_ref[r, 1:2, cut] * north[0][north[1], s, cut]
            if south is not None:
                out = out - wts_ref[r, 2:3, cut] * south[0][south[1], s, cut]
            dst[r, s, cut] = out
            dots = x * out if dots is None else dots + x * out
        if acc is not None:
            acc_ref[acc, s, :] += dots

    def apply_inner(src, dst):
        def body(r, carry):
            for s in parts:
                apply_part(src, dst, r, s, (src, r - 1), (src, r + 1))
            return carry
        lax.fori_loop(1, rows - 1, body, 0)

    for s in (*parts, extra):
        apply_part(q_ref, w_ref, 0, s, None, (q_ref, 1))
        apply_part(q_ref, w_ref, rows - 1, s, (q_ref, rows - 2), None)

    done(*ring(0))
    if few:
        greet(hello)
    done(bmsg_ref, bgot_ref, sendb, recvb)

    def row_of(side, base):
        return jnp.concatenate([bgot_ref[side, base + c:base + c + 1, :] for c in range(tiles)], 1)

    halo_a = [row_of(side, tiles) for side in range(2)]
    halo_v = [row_of(side, 2 * tiles) for side in range(2)]
    over = []
    for side, r in ends:
        i = 1 + side
        x = edge(active[r:r + 1, :], halo_a[side], valid[r:r + 1, :], halo_v[side])
        over.append(x)
        wts_ref[r, i:i + 1, :] = x
        wts_ref[r, 0:1, :] += x
        wts_ref[r, 5:6, :] += 0.5 * x

    def precond_row(r):
        for c, cut in enumerate(cuts):
            z_ref[r, :, cut] = product(w_ref[r, :, cut], r, c)

    for h, s in halves:
        if h:
            done(*ring(h))
        for side, r in ends:
            va = got_ref[h, side, 0:piece, :]
            vb = got_ref[h, side, piece:pairs, :]
            last_a = last_b = None
            dots = jnp.zeros((piece, LANES), F32)
            for c, cut in enumerate(cuts):
                common = bgot_ref[side, c:c + 1, :]
                qh = jnp.where(tile_a[s] == c, va, 0.0) + jnp.where(tile_b[s] == c, vb, 0.0)
                qhalo_ref[side, s, cut] = qh
                q0 = q_ref[r, s, cut]
                w0 = w_ref[r, s, cut] + over[side][:, cut] * (q0 - (qh + common))
                w_ref[r, s, cut] = w0
                dots = dots + q0 * w0
                if h == 0:
                    we = w_ref[r, extra, cut] + over[side][:, cut] * (q_ref[r, extra, cut] - common)
                    w_ref[r, extra, cut] = we
                    z = product(jnp.concatenate([w0, we], 0), r, c)
                    z_ref[r, extra, cut] = z[piece:]
                    zmsg_ref[h, side, pairs + c:pairs + c + 1, :] = z[piece:piece + 1]
                    z = z[:piece]
                else:
                    z = product(w0, r, c)
                z_ref[r, s, cut] = z
                last_a = z if c == 0 else jnp.where(tile_a[s] == c, z, last_a)
                last_b = z if c == 0 else jnp.where(tile_b[s] == c, z, last_b)
            acc_ref[1, s, :] += dots
            zmsg_ref[h, side, 0:piece, :] = last_a
            zmsg_ref[h, side, piece:pairs, :] = last_b
        send(*zring(h))

    def moment_part(r, s, north):
        mu = nu = None
        for c, cut, z, west, _ in stream(z_ref, r, s, False):
            t = wts_ref[r, 5:6, cut] * z - wts_ref[r, 3:4, cut] * west
            if north:
                t = t - wts_ref[r, 1:2, cut] * z_ref[r - 1, s, cut]
            one, two = w_ref[r, s, cut] * z, t * z
            mu, nu = (one, two) if mu is None else (mu + one, nu + two)
        acc_ref[2, s, :] += mu
        acc_ref[3, s, :] += nu

    def image_row(r):
        for s in parts:
            apply_part(q_ref, w_ref, r, s, (q_ref, r - 1), (q_ref, r + 1), 1)
        apply_part(q_ref, w_ref, r, extra, (q_ref, r - 1), (q_ref, r + 1))

    def moment_row(r):
        for s in parts:
            moment_part(r, s, r > 0)

    image_row(1)
    for r in inner:
        if r + 1 in inner:
            image_row(r + 1)
        precond_row(r)
        moment_row(r - 1)
    moment_row(rows - 2)
    moment_row(rows - 1)

    pad = jnp.zeros((8, LANES - pairs), F32)

    def lines(sums):
        table = jnp.zeros((pairs, LANES), F32)
        for i, x in enumerate(sums):
            table = jnp.where(lane == i, jnp.sum(x, 1, keepdims=True), table)
        return jnp.concatenate([table.T[0:8, :], pad], 1)

    def exchange(src, dst, ssem, rsem):
        for k in range(1, count):
            pltpu.make_async_remote_copy(
                src_ref=src, dst_ref=dst.at[k - 1], send_sem=ssem, recv_sem=rsem,
                device_id={"space": lax.rem(me + k, count)}, device_id_type=pl.DeviceIdType.MESH,
            ).start()

    def arrived(dst, ssem, rsem):
        for sem in (ssem, rsem):
            pltpu.make_async_copy(dst, dst, sem).wait()

    early = lines([acc_ref[i] for i in range(4)])
    stat_ref[...] = early
    if few:
        greeted(hello)
    exchange(stat_ref, all_ref, send3, recv3)

    done(tmsg_ref, tgot_ref, sendt, recvt)
    for side in range(2):
        halo_w, halo_e = (
            edge(halo_a[side], shifted(halo_a[side], by, 1), halo_v[side], shifted(halo_v[side], by, 1))
            for by in (1, -1)
        )
        near = [jnp.zeros((pairs, LANES), F32)] * tiles
        for c, cut in enumerate(cuts):
            qh = qhalo_ref[side, :, cut]
            if c > 0:
                gone = (halo_w[:, cut] * qh)[:, 0:1]
                near[c - 1] = near[c - 1] - gone * tgot_ref[side, tiles + c - 1:tiles + c, :]
            if c < tiles - 1:
                gone = (halo_e[:, cut] * qh)[:, LANES - 1:LANES]
                near[c + 1] = near[c + 1] - gone * tgot_ref[side, c + 1:c + 2, :]
        for c, cut in enumerate(cuts):
            zhalo_ref[side, :, cut] = near[c]

    coupling = [[], []]
    for h, s in halves:
        done(*zring(h))
        for side, r in ends:
            va = zgot_ref[h, side, 0:piece, :]
            vb = zgot_ref[h, side, piece:pairs, :]
            joined = jnp.zeros((piece, LANES), F32)
            for c, cut in enumerate(cuts):
                other = zgot_ref[0, side, pairs + c:pairs + c + 1, :] + zhalo_ref[side, s, cut]
                zh = jnp.where(tile_a[s] == c, va, jnp.where(tile_b[s] == c, vb, other))
                zhalo_ref[side, s, cut] = zh
                joined = joined + over[side][:, cut] * z_ref[r, s, cut] * zh
            coupling[side].append(joined)
    late = lines([jnp.concatenate(x, 0) for x in coupling])
    late_ref[...] = late
    def late_copy(k):
        return pltpu.make_async_remote_copy(
            src_ref=late_ref, dst_ref=lates_ref.at[k - 1], send_sem=send4.at[k - 1], recv_sem=recv4.at[k - 1],
            device_id={"space": lax.rem(me + k, count)}, device_id_type=pl.DeviceIdType.MESH,
        )

    def gives(who, k):
        up = who + k < count
        return jnp.logical_or(jnp.logical_and(up, who > 0), jnp.logical_and(jnp.logical_not(up), who < last))

    for k in range(1, count):
        @pl.when(gives(me, k))
        def _():
            late_copy(k).start()

    apply_inner(z_ref, y_ref)
    for s in parts:
        apply_part(z_ref, y_ref, 0, s, (zhalo_ref, 0), (z_ref, 1))
        apply_part(z_ref, y_ref, rows - 1, s, (z_ref, rows - 2), (zhalo_ref, 1))

    def right_side(r, carry):
        for c, cut in enumerate(cuts):
            local = r * cols + c * LANES + lane
            x = jnp.where(local == at_a, FOCAL_CURRENT, 0.0) - jnp.where(local == at_b, FOCAL_CURRENT, 0.0)
            r0_ref[r, 0:pairs, cut] = wts_ref[r, 6:7, cut] + x
        return carry

    lax.fori_loop(0, rows, right_side, 0)

    arrived(all_ref, send3, recv3)
    total = early
    for k in range(1, count):
        total = total + all_ref[k - 1]
    gamma0, kappa, mu, part = (total[i:i + 1, :] for i in range(4))
    a0 = gamma0 / kappa
    gamma1 = a0 * a0 * mu - gamma0
    beta = gamma1 / gamma0
    known = kappa - 2.0 * a0 * mu - beta * gamma1 / a0 + 2.0 * a0 * a0 * part
    scale = 2.0 * a0 * a0
    joint = late[0:1, :] + late[1:2, :]
    for k in range(1, count):
        @pl.when(gives(me, k))
        def _():
            late_copy(k).wait_send()

        @pl.when(gives(lax.rem(me - k + count, count), k))
        def _():
            late_copy(k).wait_recv()
    for k in range(1, count):
        joint = joint + jnp.where(k <= me, lates_ref[k - 1, 0:1, :], lates_ref[k - 1, 1:2, :])
    a1 = gamma1 / (known - scale * joint)
    first = a0 + a1 * (1.0 + beta)
    both = jnp.concatenate([first, a0 * a1, jnp.zeros((6, LANES), F32)], 0).T
    for i in range(2):
        coef_ref[i] = jnp.broadcast_to(both[:pairs, i:i + 1], (pairs, LANES))


def combine_kernel(coef_ref, r0_ref, q_ref, w_ref, z_ref, y_ref, sol_hbm, res_hbm, sol_ref, res_ref, sem):
    rows, pairs, cols = sol_ref.shape
    mine = pl.ds(0, pairs)

    def out(r, src, dst, k):
        return pltpu.make_async_copy(src.at[r], dst.at[mine, r], sem.at[k, r])

    def body(r, carry):
        one, two = coef_ref[0], coef_ref[1]
        for c in range(cols // LANES):
            cut = slice(c * LANES, (c + 1) * LANES)
            sol_ref[r, :, cut] = one * q_ref[r, mine, cut] - two * z_ref[r, mine, cut]
            res_ref[r, :, cut] = r0_ref[r, mine, cut] - one * w_ref[r, mine, cut] + two * y_ref[r, mine, cut]
        out(r, sol_ref, sol_hbm, 0).start()
        out(r, res_ref, res_hbm, 1).start()
        return carry

    lax.fori_loop(0, rows, body, 0)

    def finish(r, carry):
        out(r, sol_ref, sol_hbm, 0).wait()
        out(r, res_ref, res_hbm, 1).wait()
        return carry

    lax.fori_loop(0, rows, finish, 0)


def on_device(count, cond, nodata, gmask, gval, smask, scur, tinv, focal):
    rows, cols = cond.shape
    pairs = focal.shape[0]
    tiles = cols // LANES
    ext = pairs + EXTRA
    field = jax.ShapeDtypeStruct((rows, ext, cols), F32)
    vm = pl.BlockSpec(memory_space=pltpu.VMEM)
    hbm = pl.BlockSpec(memory_space=pltpu.HBM)
    msg = (2, 2, pairs, LANES)
    bmsg = (2, 3 * tiles, LANES)
    tmsg = (2, 2 * tiles, LANES)
    zmsg = (2, 2, pairs + tiles, LANES)
    others = count - 1
    r0, q, w, z, y, coef = pl.pallas_call(
        functools.partial(krylov_kernel, count),
        out_shape=[field] * 5 + [jax.ShapeDtypeStruct((2, pairs, LANES), F32)],
        in_specs=[hbm] * 8,
        out_specs=[vm] * 6,
        scratch_shapes=[
            pltpu.VMEM((3, rows, cols), F32),
            pltpu.VMEM((3, rows, cols), jnp.int32),
            pltpu.VMEM((2, pairs), jnp.int32),
            pltpu.SMEM((2, pairs), jnp.int32),
            pltpu.VMEM((2, cols, LANES), F32),
            pltpu.VMEM((rows - 2, cols, LANES), F32),
            pltpu.VMEM((rows, tiles, LANES, 2 * LANES), BF16),
            pltpu.VMEM((rows, 8, cols), F32),
            pltpu.VMEM((2, pairs, LANES), F32),
            pltpu.VMEM((2, pairs, cols), F32),
            pltpu.VMEM((2, pairs, cols), F32),
            *[pltpu.VMEM(shape, F32) for shape in (msg, bmsg, tmsg, zmsg) for _ in range(2)],
            pltpu.VMEM((4, pairs, LANES), F32),
            *[pltpu.VMEM(shape, F32) for _ in range(2) for shape in ((8, LANES), (others, 8, LANES))],
            *[pltpu.SemaphoreType.DMA((2, 2))] * 2,
            *[pltpu.SemaphoreType.DMA((2,))] * 4,
            *[pltpu.SemaphoreType.DMA((2, 2))] * 2,
            *[pltpu.SemaphoreType.DMA] * 2,
            *[pltpu.SemaphoreType.DMA((others,))] * 2,
            pltpu.SemaphoreType.DMA((6,)),
            pltpu.SemaphoreType.REGULAR,
        ],
        compiler_params=pltpu.CompilerParams(
            collective_id=0, has_side_effects=True, vmem_limit_bytes=36 * 1024 * 1024
        ),
        name="krylov",
    )(*(
        pltpu.with_memory_space_constraint(x, pltpu.HBM)
        for x in (cond, nodata, gmask, gval, smask, scur, tinv.reshape(rows, cols, LANES), focal.T)
    ))

    out = jax.ShapeDtypeStruct((pairs, rows, cols), F32)
    return tuple(pl.pallas_call(
        combine_kernel,
        out_shape=[out, out],
        in_specs=[vm] * 6,
        out_specs=[hbm, hbm],
        scratch_shapes=[
            pltpu.VMEM((rows, pairs, cols), F32),
            pltpu.VMEM((rows, pairs, cols), F32),
            pltpu.SemaphoreType.DMA((2, rows)),
        ],
        compiler_params=pltpu.CompilerParams(vmem_limit_bytes=20 * 1024 * 1024),
        name="combine",
    )(coef, r0, q, w, z, y))


def solution(mesh):
    return jax.shard_map(
        functools.partial(on_device, mesh.shape["space"]),
        mesh=mesh,
        in_specs=(
            P(("groups", "space"), None),
            P(("groups", "space"), None),
            P(("groups", "space"), None),
            P(("groups", "space"), None),
            P(("groups", "space"), None),
            P(("groups", "space"), None),
            P(("groups", "space"), None, None, None),
            P(("groups", "rhs"), None),
        ),
        out_specs=(P("rhs", ("groups", "space"), None), P("rhs", ("groups", "space"), None)),
        check_vma=False,
    )
```

```python
import functools

import jax
import jax.numpy as jnp
from jax import lax
from jax.experimental import pallas as pl
from jax.experimental.pallas import tpu as pltpu
from jax.sharding import PartitionSpec as P

LEAKAGE = 0.05
FOCAL_CURRENT = 16.0
LANES = 128
EXTRA = 8
F32 = jnp.float32
BF16 = jnp.bfloat16


def krylov_kernel(
    count, cond_hbm, nodata_hbm, gmask_hbm, gval_hbm, smask_hbm, scur_hbm, t_hbm, focal_hbm,
    r0_ref, q_ref, w_ref, z_ref, y_ref, coef_ref,
    reals_ref, flags_ref, focal_ref, ids_ref, te_ref, ti_ref,
    thl_ref, wts_ref, spot_ref, qhalo_ref, zhalo_ref, msg_ref, got_ref, bmsg_ref, bgot_ref, tmsg_ref, tgot_ref,
    zmsg_ref, zgot_ref, acc_ref, stat_ref, all_ref, late_ref, lates_ref,
    send1, recv1, sendb, recvb, sendt, recvt, send2, recv2, send3, recv3, send4, recv4, sem_in, hello,
):
    rows, cols = reals_ref.shape[1:]
    tiles = cols // LANES
    pairs = focal_ref.shape[1]
    ext = pairs + EXTRA
    me = lax.axis_index("space")
    last = count - 1
    ends = ((0, 0), (1, rows - 1))
    inner = range(1, rows - 1)
    cuts = [slice(c * LANES, (c + 1) * LANES) for c in range(tiles)]

    has = (me > 0, me < last)
    few = count <= 4
    barrier = pltpu.get_barrier_semaphore()
    lates_ref[...] = jnp.zeros(lates_ref.shape, F32)

    def greet(sem):
        for side in range(2):
            @pl.when(has[side])
            def _():
                pl.semaphore_signal(
                    sem, inc=1, device_id={"space": me - 1 if side == 0 else me + 1},
                    device_id_type=pl.DeviceIdType.MESH,
                )

    def greeted(sem):
        pl.semaphore_wait(sem, jnp.minimum(me, 1) + jnp.minimum(last - me, 1))

    if few:
        greet(barrier)
    else:
        for off in range(1, count):
            pl.semaphore_signal(
                barrier, inc=1, device_id={"space": lax.rem(me + off, count)},
                device_id_type=pl.DeviceIdType.MESH,
            )

    def whole(ref, i):
        return pltpu.make_async_copy(ref, ref, sem_in.at[i])

    ids_load = pltpu.make_async_copy(focal_hbm, ids_ref, sem_in.at[0])
    focal_load = pltpu.make_async_copy(focal_hbm, focal_ref, sem_in.at[1])
    inner_load = pltpu.make_async_copy(t_hbm.at[pl.ds(1, rows - 2)], ti_ref, sem_in.at[5])
    ids_load.start()
    focal_load.start()
    for side, r in ends:
        for cut in cuts:
            pltpu.make_async_copy(
                t_hbm.at[r, pl.ds(cut.start, LANES)], te_ref.at[side, pl.ds(cut.start, LANES)], sem_in.at[2]).start()
    for i, group in ((3, (cond_hbm, gval_hbm, scur_hbm)), (4, (nodata_hbm, gmask_hbm, smask_hbm))):
        for k, src in enumerate(group):
            pltpu.make_async_copy(src, (reals_ref, flags_ref)[i - 3].at[k], sem_in.at[i]).start()
    inner_load.start()
    ids_load.wait()
    focal_load.wait()
    whole(te_ref, 2).wait()

    def gather(src, at):
        for p in range(pairs):
            for i in range(2):
                r, k = at(ids_ref[i, p])
                spot_ref[i, p:p + 1, :] = src[r, pl.ds(k, 1), :]
        return FOCAL_CURRENT * spot_ref[0], -FOCAL_CURRENT * spot_ref[1]

    half, high = (rows * cols // 2).bit_length() - 1, cols.bit_length() - 1
    near_a, near_b = gather(
        te_ref, lambda i: (lax.shift_right_logical(i, half) & 1, i & (cols - 1)))

    diagonal = lax.broadcasted_iota(jnp.int32, (pairs, pairs), 0) == lax.broadcasted_iota(
        jnp.int32, (pairs, pairs), 1)
    lane = lax.broadcasted_iota(jnp.int32, (pairs, LANES), 1)

    def column(i):
        line = jnp.broadcast_to(focal_ref[i:i + 1, :].astype(F32), (pairs, pairs))
        return jnp.broadcast_to(
            jnp.sum(jnp.where(diagonal, line, 0.0), 1, keepdims=True).astype(jnp.int32), (pairs, LANES))

    at_a, at_b = (column(i) - me * (rows * cols) for i in range(2))
    spot_a, spot_b = (lax.shift_right_arithmetic(x, 7) for x in (at_a, at_b))
    tile_a, tile_b = spot_a & (tiles - 1), spot_b & (tiles - 1)

    def within(spot, low, high):
        return jnp.logical_and(spot >= low * tiles, spot < high * tiles)

    piece = pairs // 2
    halves = tuple(enumerate((slice(0, piece), slice(piece, pairs))))
    for side, r in ends:
        here_a = jnp.where(within(spot_a, r, r + 1), near_a, 0.0)
        here_b = jnp.where(within(spot_b, r, r + 1), near_b, 0.0)
        for h, s in halves:
            msg_ref[h, side, 0:piece, :] = here_a[s]
            msg_ref[h, side, piece:pairs, :] = here_b[s]

    def side_copy(src, dst, ssem, rsem, side, number):
        return pltpu.make_async_remote_copy(
            src_ref=src.at[side, pl.ds(0, number)], dst_ref=dst.at[1 - side, pl.ds(0, number)],
            send_sem=ssem.at[side], recv_sem=rsem.at[1 - side],
            device_id={"space": me - 1 if side == 0 else me + 1},
            device_id_type=pl.DeviceIdType.MESH,
        )

    def send(src, dst, ssem, rsem, number=None):
        number = number or src.shape[1]
        for side in range(2):
            @pl.when(has[side])
            def _():
                side_copy(src, dst, ssem, rsem, side, number).start()

            @pl.when(jnp.logical_not(has[side]))
            def _():
                dst[side] = jnp.zeros(dst.shape[1:], F32)

    def done(src, dst, ssem, rsem, number=None):
        number = number or src.shape[1]
        for side in range(2):
            @pl.when(has[side])
            def _():
                side_copy(src, dst, ssem, rsem, side, number).wait_send()
                pltpu.make_async_remote_copy(
                    src_ref=src.at[1 - side, pl.ds(0, number)], dst_ref=dst.at[side, pl.ds(0, number)],
                    send_sem=ssem.at[1 - side], recv_sem=rsem.at[side],
                    device_id={"space": me - 1 if side == 0 else me + 1},
                    device_id_type=pl.DeviceIdType.MESH,
                ).wait_recv()

    def ring(h):
        return msg_ref.at[h], got_ref.at[h], send1.at[h], recv1.at[h]

    def zring(h):
        return zmsg_ref.at[h], zgot_ref.at[h], send2.at[h], recv2.at[h], pairs + (0 if h else tiles)

    if few:
        greeted(barrier)
    else:
        pl.semaphore_wait(barrier, last)
    send(*ring(0))

    whole(reals_ref, 3).wait()
    whole(flags_ref, 4).wait()
    valid = (1 - flags_ref[0]).astype(F32)
    active = reals_ref[0] * valid
    background = flags_ref[2].astype(F32) * reals_ref[2]

    def tile_of(r, c):
        if r == 0 or r == rows - 1:
            return te_ref[min(r, 1), cuts[c], :]
        return ti_ref[r - 1, cuts[c], :]

    def product(x, r, c):
        number = x.shape[0]
        hi = x.astype(BF16).astype(F32)
        lhs = jnp.concatenate([hi, x - hi], 0).astype(BF16)
        o = jnp.dot(lhs, thl_ref[r, c], preferred_element_type=F32)
        return o[:number, :LANES] + (o[:number, LANES:] + (o[number:, :LANES] + o[number:, LANES:]))

    def shared_row(r):
        dot = jnp.zeros((EXTRA, LANES), F32)
        for c, cut in enumerate(cuts):
            t = tile_of(r, c)
            thi = t.astype(BF16)
            thl_ref[r, c, :, :LANES] = thi
            thl_ref[r, c, :, LANES:] = (t - thi.astype(F32)).astype(BF16)
            x = jnp.broadcast_to(background[r:r + 1, cut], (EXTRA, LANES))
            q = product(x, r, c)
            q_ref[r, pairs:ext, cut] = q
            dot = dot + x * q
        return dot

    shared = shared_row(0) + shared_row(rows - 1)
    for side, r in ends:
        for c, cut in enumerate(cuts):
            bmsg_ref[side, c:c + 1, :] = q_ref[r, pairs:pairs + 1, cut]
            bmsg_ref[side, tiles + c:tiles + c + 1, :] = active[r:r + 1, cut]
            bmsg_ref[side, 2 * tiles + c:2 * tiles + c + 1, :] = valid[r:r + 1, cut]
            tmsg_ref[side, c:c + 1, :] = te_ref[side, cut.start:cut.start + 1, :]
            tmsg_ref[side, tiles + c:tiles + c + 1, :] = te_ref[side, cut.stop - 1:cut.stop, :]
    send(bmsg_ref, bgot_ref, sendb, recvb)
    send(*ring(1))
    send(tmsg_ref, tgot_ref, sendt, recvt)

    def edge(a, b, v, u):
        return 0.5 * (a + b) * v * u

    row_at = lax.broadcasted_iota(jnp.int32, (rows, cols), 0)
    col_at = lax.broadcasted_iota(jnp.int32, (rows, cols), 1)

    def shifted(x, by, axis):
        length = x.shape[axis]
        at = (row_at, col_at)[axis][:x.shape[0], :]
        return jnp.where(at == (0 if by == 1 else length - 1), 0.0, pltpu.roll(x, by % length, axis))

    nw, sw, ww, ew = (
        edge(active, shifted(active, *how), valid, shifted(valid, *how))
        for how in ((1, 0), (-1, 0), (1, 1), (-1, 1))
    )
    dg = valid * (LEAKAGE + flags_ref[1].astype(F32) * reals_ref[1]) + (1.0 - valid) + nw + sw + ww + ew
    for r in range(rows):
        for i, x in enumerate((dg, nw, sw, ww, ew, 0.5 * dg, background)):
            wts_ref[r, i:i + 1, :] = x[r:r + 1, :]

    inner_load.wait()
    far_a, far_b = gather(
        ti_ref, lambda i: (
            jnp.clip((lax.shift_right_logical(i, high) & (rows - 1)) - 1, 0, rows - 3), i & (cols - 1)))
    for r in inner:
        shared = shared + shared_row(r)

    def dense_row(r, a, b, dot):
        for c, cut in enumerate(cuts):
            k = r * tiles + c
            x = jnp.where(spot_a == k, a, 0.0) + jnp.where(spot_b == k, b, 0.0)
            q_ref[r, 0:pairs, cut] = q_ref[r, pairs:pairs + 1, cut] + x
            dot = dot + background[r:r + 1, cut] * x
        return dot

    dot = jnp.zeros((pairs, LANES), F32)
    for r in range(rows):
        a, b = (far_a, far_b) if r in inner else (near_a, near_b)
        dot = dense_row(r, a, b, dot)
    in_a, in_b = (
        jnp.where(within(spot, 1, rows - 1), far, jnp.where(within(spot, 0, rows), near, 0.0))
        for spot, far, near in ((spot_a, far_a, near_a), (spot_b, far_b, near_b))
    )
    same = spot_a == spot_b
    own = jnp.where(lane == (at_a & (LANES - 1)), in_a + jnp.where(same, in_b, 0.0), 0.0) - jnp.where(
        lane == (at_b & (LANES - 1)), in_b + jnp.where(same, in_a, 0.0), 0.0)
    acc_ref[0] = 2.0 * dot + FOCAL_CURRENT * own + jnp.broadcast_to(shared[0:1, :], dot.shape)
    for i in range(1, 4):
        acc_ref[i] = jnp.zeros(acc_ref.shape[1:], F32)

    parts = [slice(p, p + 16) for p in range(0, pairs, 16)]
    extra = slice(pairs, ext)

    def stream(src, r, s, east=True):
        at = lane[:s.stop - s.start]
        x = src[r, s, cuts[0]]
        gone, west, ahead = None, pltpu.roll(x, 1, 1), east and pltpu.roll(x, LANES - 1, 1)
        for c in range(tiles):
            more = c + 1 < tiles
            if more:
                y = src[r, s, cuts[c + 1]]
                after = east and pltpu.roll(y, LANES - 1, 1)
            yield (
                c, cuts[c], x, west if gone is None else jnp.where(at == 0, gone, west),
                jnp.where(at == LANES - 1, after, ahead) if east and more else ahead,
            )
            if more:
                x, gone, west, ahead = y, west, pltpu.roll(y, 1, 1), after

    def apply_part(src, dst, r, s, north, south, acc=None):
        dots = None
        for c, cut, x, west, east in stream(src, r, s):
            out = wts_ref[r, 0:1, cut] * x - wts_ref[r, 3:4, cut] * west - wts_ref[r, 4:5, cut] * east
            if north is not None:
                out = out - wts_ref[r, 1:2, cut] * north[0][north[1], s, cut]
            if south is not None:
                out = out - wts_ref[r, 2:3, cut] * south[0][south[1], s, cut]
            dst[r, s, cut] = out
            dots = x * out if dots is None else dots + x * out
        if acc is not None:
            acc_ref[acc, s, :] += dots

    def apply_inner(src, dst):
        def body(r, carry):
            for s in parts:
                apply_part(src, dst, r, s, (src, r - 1), (src, r + 1))
            return carry
        lax.fori_loop(1, rows - 1, body, 0)

    for s in (*parts, extra):
        apply_part(q_ref, w_ref, 0, s, None, (q_ref, 1))
        apply_part(q_ref, w_ref, rows - 1, s, (q_ref, rows - 2), None)

    def image_row(r):
        for s in parts:
            apply_part(q_ref, w_ref, r, s, (q_ref, r - 1), (q_ref, r + 1), 1)
        apply_part(q_ref, w_ref, r, extra, (q_ref, r - 1), (q_ref, r + 1))

    ready = rows - 2 - 3
    for r in range(ready + 1, rows - 1):
        image_row(r)

    done(*ring(0))
    if few:
        greet(hello)
    done(bmsg_ref, bgot_ref, sendb, recvb)

    def row_of(side, base):
        return jnp.concatenate([bgot_ref[side, base + c:base + c + 1, :] for c in range(tiles)], 1)

    halo_a = [row_of(side, tiles) for side in range(2)]
    halo_v = [row_of(side, 2 * tiles) for side in range(2)]
    over = []
    for side, r in ends:
        i = 1 + side
        x = edge(active[r:r + 1, :], halo_a[side], valid[r:r + 1, :], halo_v[side])
        over.append(x)
        wts_ref[r, i:i + 1, :] = x
        wts_ref[r, 0:1, :] += x
        wts_ref[r, 5:6, :] += 0.5 * x

    def precond_row(r):
        for c, cut in enumerate(cuts):
            z_ref[r, :, cut] = product(w_ref[r, :, cut], r, c)

    for h, s in halves:
        if h:
            done(*ring(h))
        for side, r in ends:
            va = got_ref[h, side, 0:piece, :]
            vb = got_ref[h, side, piece:pairs, :]
            last_a = last_b = None
            dots = jnp.zeros((piece, LANES), F32)
            for c, cut in enumerate(cuts):
                common = bgot_ref[side, c:c + 1, :]
                qh = jnp.where(tile_a[s] == c, va, 0.0) + jnp.where(tile_b[s] == c, vb, 0.0)
                qhalo_ref[side, s, cut] = qh
                q0 = q_ref[r, s, cut]
                w0 = w_ref[r, s, cut] + over[side][:, cut] * (q0 - (qh + common))
                w_ref[r, s, cut] = w0
                dots = dots + q0 * w0
                if h == 0:
                    we = w_ref[r, extra, cut] + over[side][:, cut] * (q_ref[r, extra, cut] - common)
                    w_ref[r, extra, cut] = we
                    z = product(jnp.concatenate([w0, we], 0), r, c)
                    z_ref[r, extra, cut] = z[piece:]
                    zmsg_ref[h, side, pairs + c:pairs + c + 1, :] = z[piece:piece + 1]
                    z = z[:piece]
                else:
                    z = product(w0, r, c)
                z_ref[r, s, cut] = z
                last_a = z if c == 0 else jnp.where(tile_a[s] == c, z, last_a)
                last_b = z if c == 0 else jnp.where(tile_b[s] == c, z, last_b)
            acc_ref[1, s, :] += dots
            zmsg_ref[h, side, 0:piece, :] = last_a
            zmsg_ref[h, side, piece:pairs, :] = last_b
        send(*zring(h))

    def moment_part(r, s, north):
        mu = nu = None
        for c, cut, z, west, _ in stream(z_ref, r, s, False):
            t = wts_ref[r, 5:6, cut] * z - wts_ref[r, 3:4, cut] * west
            if north:
                t = t - wts_ref[r, 1:2, cut] * z_ref[r - 1, s, cut]
            one, two = w_ref[r, s, cut] * z, t * z
            mu, nu = (one, two) if mu is None else (mu + one, nu + two)
        acc_ref[2, s, :] += mu
        acc_ref[3, s, :] += nu

    def moment_row(r):
        for s in parts:
            moment_part(r, s, r > 0)

    image_row(1)
    for r in inner:
        if r + 1 <= ready:
            image_row(r + 1)
        precond_row(r)
        moment_row(r - 1)
    moment_row(rows - 2)
    moment_row(rows - 1)

    pad = jnp.zeros((8, LANES - pairs), F32)

    def lines(sums):
        table = jnp.zeros((pairs, LANES), F32)
        for i, x in enumerate(sums):
            table = jnp.where(lane == i, jnp.sum(x, 1, keepdims=True), table)
        return jnp.concatenate([table.T[0:8, :], pad], 1)

    def exchange(src, dst, ssem, rsem):
        for k in range(1, count):
            pltpu.make_async_remote_copy(
                src_ref=src, dst_ref=dst.at[k - 1], send_sem=ssem, recv_sem=rsem,
                device_id={"space": lax.rem(me + k, count)}, device_id_type=pl.DeviceIdType.MESH,
            ).start()

    def arrived(dst, ssem, rsem):
        for sem in (ssem, rsem):
            pltpu.make_async_copy(dst, dst, sem).wait()

    early = lines([acc_ref[i] for i in range(4)])
    stat_ref[...] = early
    if few:
        greeted(hello)
    exchange(stat_ref, all_ref, send3, recv3)

    done(tmsg_ref, tgot_ref, sendt, recvt)
    for side in range(2):
        halo_w, halo_e = (
            edge(halo_a[side], shifted(halo_a[side], by, 1), halo_v[side], shifted(halo_v[side], by, 1))
            for by in (1, -1)
        )
        near = [jnp.zeros((pairs, LANES), F32)] * tiles
        for c, cut in enumerate(cuts):
            qh = qhalo_ref[side, :, cut]
            if c > 0:
                gone = (halo_w[:, cut] * qh)[:, 0:1]
                near[c - 1] = near[c - 1] - gone * tgot_ref[side, tiles + c - 1:tiles + c, :]
            if c < tiles - 1:
                gone = (halo_e[:, cut] * qh)[:, LANES - 1:LANES]
                near[c + 1] = near[c + 1] - gone * tgot_ref[side, c + 1:c + 2, :]
        for c, cut in enumerate(cuts):
            zhalo_ref[side, :, cut] = near[c]

    coupling = [[], []]
    for h, s in halves:
        done(*zring(h))
        for side, r in ends:
            va = zgot_ref[h, side, 0:piece, :]
            vb = zgot_ref[h, side, piece:pairs, :]
            joined = jnp.zeros((piece, LANES), F32)
            for c, cut in enumerate(cuts):
                other = zgot_ref[0, side, pairs + c:pairs + c + 1, :] + zhalo_ref[side, s, cut]
                zh = jnp.where(tile_a[s] == c, va, jnp.where(tile_b[s] == c, vb, other))
                zhalo_ref[side, s, cut] = zh
                joined = joined + over[side][:, cut] * z_ref[r, s, cut] * zh
            coupling[side].append(joined)
    late = lines([jnp.concatenate(x, 0) for x in coupling])
    late_ref[...] = late
    def late_copy(k):
        return pltpu.make_async_remote_copy(
            src_ref=late_ref, dst_ref=lates_ref.at[k - 1], send_sem=send4.at[k - 1], recv_sem=recv4.at[k - 1],
            device_id={"space": lax.rem(me + k, count)}, device_id_type=pl.DeviceIdType.MESH,
        )

    def gives(who, k):
        up = who + k < count
        return jnp.logical_or(jnp.logical_and(up, who > 0), jnp.logical_and(jnp.logical_not(up), who < last))

    for k in range(1, count):
        @pl.when(gives(me, k))
        def _():
            late_copy(k).start()

    apply_inner(z_ref, y_ref)
    for s in parts:
        apply_part(z_ref, y_ref, 0, s, (zhalo_ref, 0), (z_ref, 1))
        apply_part(z_ref, y_ref, rows - 1, s, (z_ref, rows - 2), (zhalo_ref, 1))

    def right_side(r, carry):
        for c, cut in enumerate(cuts):
            local = r * cols + c * LANES + lane
            x = jnp.where(local == at_a, FOCAL_CURRENT, 0.0) - jnp.where(local == at_b, FOCAL_CURRENT, 0.0)
            r0_ref[r, 0:pairs, cut] = wts_ref[r, 6:7, cut] + x
        return carry

    lax.fori_loop(0, rows, right_side, 0)

    arrived(all_ref, send3, recv3)
    total = early
    for k in range(1, count):
        total = total + all_ref[k - 1]
    gamma0, kappa, mu, part = (total[i:i + 1, :] for i in range(4))
    a0 = gamma0 / kappa
    gamma1 = a0 * a0 * mu - gamma0
    beta = gamma1 / gamma0
    known = kappa - 2.0 * a0 * mu - beta * gamma1 / a0 + 2.0 * a0 * a0 * part
    scale = 2.0 * a0 * a0
    joint = late[0:1, :] + late[1:2, :]
    for k in range(1, count):
        @pl.when(gives(me, k))
        def _():
            late_copy(k).wait_send()

        @pl.when(gives(lax.rem(me - k + count, count), k))
        def _():
            late_copy(k).wait_recv()
    for k in range(1, count):
        joint = joint + jnp.where(k <= me, lates_ref[k - 1, 0:1, :], lates_ref[k - 1, 1:2, :])
    a1 = gamma1 / (known - scale * joint)
    first = a0 + a1 * (1.0 + beta)
    both = jnp.concatenate([first, a0 * a1, jnp.zeros((6, LANES), F32)], 0).T
    for i in range(2):
        coef_ref[i] = jnp.broadcast_to(both[:pairs, i:i + 1], (pairs, LANES))


def combine_kernel(coef_ref, r0_ref, q_ref, w_ref, z_ref, y_ref, sol_hbm, res_hbm, sol_ref, res_ref, sem):
    rows, pairs, cols = sol_ref.shape
    mine = pl.ds(0, pairs)

    def out(r, src, dst, k):
        return pltpu.make_async_copy(src.at[r], dst.at[mine, r], sem.at[k, r])

    def body(r, carry):
        one, two = coef_ref[0], coef_ref[1]
        for c in range(cols // LANES):
            cut = slice(c * LANES, (c + 1) * LANES)
            sol_ref[r, :, cut] = one * q_ref[r, mine, cut] - two * z_ref[r, mine, cut]
            res_ref[r, :, cut] = r0_ref[r, mine, cut] - one * w_ref[r, mine, cut] + two * y_ref[r, mine, cut]
        out(r, sol_ref, sol_hbm, 0).start()
        out(r, res_ref, res_hbm, 1).start()
        return carry

    lax.fori_loop(0, rows, body, 0)

    def finish(r, carry):
        out(r, sol_ref, sol_hbm, 0).wait()
        out(r, res_ref, res_hbm, 1).wait()
        return carry

    lax.fori_loop(0, rows, finish, 0)


def on_device(count, cond, nodata, gmask, gval, smask, scur, tinv, focal):
    rows, cols = cond.shape
    pairs = focal.shape[0]
    tiles = cols // LANES
    ext = pairs + EXTRA
    field = jax.ShapeDtypeStruct((rows, ext, cols), F32)
    vm = pl.BlockSpec(memory_space=pltpu.VMEM)
    hbm = pl.BlockSpec(memory_space=pltpu.HBM)
    msg = (2, 2, pairs, LANES)
    bmsg = (2, 3 * tiles, LANES)
    tmsg = (2, 2 * tiles, LANES)
    zmsg = (2, 2, pairs + tiles, LANES)
    others = count - 1
    r0, q, w, z, y, coef = pl.pallas_call(
        functools.partial(krylov_kernel, count),
        out_shape=[field] * 5 + [jax.ShapeDtypeStruct((2, pairs, LANES), F32)],
        in_specs=[hbm] * 8,
        out_specs=[vm] * 6,
        scratch_shapes=[
            pltpu.VMEM((3, rows, cols), F32),
            pltpu.VMEM((3, rows, cols), jnp.int32),
            pltpu.VMEM((2, pairs), jnp.int32),
            pltpu.SMEM((2, pairs), jnp.int32),
            pltpu.VMEM((2, cols, LANES), F32),
            pltpu.VMEM((rows - 2, cols, LANES), F32),
            pltpu.VMEM((rows, tiles, LANES, 2 * LANES), BF16),
            pltpu.VMEM((rows, 8, cols), F32),
            pltpu.VMEM((2, pairs, LANES), F32),
            pltpu.VMEM((2, pairs, cols), F32),
            pltpu.VMEM((2, pairs, cols), F32),
            *[pltpu.VMEM(shape, F32) for shape in (msg, bmsg, tmsg, zmsg) for _ in range(2)],
            pltpu.VMEM((4, pairs, LANES), F32),
            *[pltpu.VMEM(shape, F32) for _ in range(2) for shape in ((8, LANES), (others, 8, LANES))],
            *[pltpu.SemaphoreType.DMA((2, 2))] * 2,
            *[pltpu.SemaphoreType.DMA((2,))] * 4,
            *[pltpu.SemaphoreType.DMA((2, 2))] * 2,
            *[pltpu.SemaphoreType.DMA] * 2,
            *[pltpu.SemaphoreType.DMA((others,))] * 2,
            pltpu.SemaphoreType.DMA((6,)),
            pltpu.SemaphoreType.REGULAR,
        ],
        compiler_params=pltpu.CompilerParams(
            collective_id=0, has_side_effects=True, vmem_limit_bytes=36 * 1024 * 1024
        ),
        name="krylov",
    )(*(
        pltpu.with_memory_space_constraint(x, pltpu.HBM)
        for x in (cond, nodata, gmask, gval, smask, scur, tinv.reshape(rows, cols, LANES), focal.T)
    ))

    out = jax.ShapeDtypeStruct((pairs, rows, cols), F32)
    return tuple(pl.pallas_call(
        combine_kernel,
        out_shape=[out, out],
        in_specs=[vm] * 6,
        out_specs=[hbm, hbm],
        scratch_shapes=[
            pltpu.VMEM((rows, pairs, cols), F32),
            pltpu.VMEM((rows, pairs, cols), F32),
            pltpu.SemaphoreType.DMA((2, rows)),
        ],
        compiler_params=pltpu.CompilerParams(vmem_limit_bytes=20 * 1024 * 1024),
        name="combine",
    )(coef, r0, q, w, z, y))


def solution(mesh):
    return jax.shard_map(
        functools.partial(on_device, mesh.shape["space"]),
        mesh=mesh,
        in_specs=(
            P(("groups", "space"), None),
            P(("groups", "space"), None),
            P(("groups", "space"), None),
            P(("groups", "space"), None),
            P(("groups", "space"), None),
            P(("groups", "space"), None),
            P(("groups", "space"), None, None, None),
            P(("groups", "rhs"), None),
        ),
        out_specs=(P("rhs", ("groups", "space"), None), P("rhs", ("groups", "space"), None)),
        check_vma=False,
    )
```

```python
import functools

import jax
import jax.numpy as jnp
from jax import lax
from jax.experimental import pallas as pl
from jax.experimental.pallas import tpu as pltpu
from jax.sharding import PartitionSpec as P

LEAKAGE = 0.05
FOCAL_CURRENT = 16.0
LANES = 128
EXTRA = 8
F32 = jnp.float32
BF16 = jnp.bfloat16


def krylov_kernel(
    count, cond_hbm, nodata_hbm, gmask_hbm, gval_hbm, smask_hbm, scur_hbm, t_hbm, focal_hbm,
    r0_ref, q_ref, w_ref, z_ref, y_ref, coef_ref,
    reals_ref, flags_ref, focal_ref, ids_ref, te_ref, ti_ref,
    thl_ref, wts_ref, spot_ref, qhalo_ref, zhalo_ref, msg_ref, got_ref, bmsg_ref, bgot_ref, tmsg_ref, tgot_ref,
    zmsg_ref, zgot_ref, acc_ref, stat_ref, all_ref, late_ref, lates_ref,
    send1, recv1, sendb, recvb, sendt, recvt, send2, recv2, send3, recv3, send4, recv4, sem_in, hello,
):
    rows, cols = reals_ref.shape[1:]
    tiles = cols // LANES
    pairs = focal_ref.shape[1]
    ext = pairs + EXTRA
    me = lax.axis_index("space")
    last = count - 1
    ends = ((0, 0), (1, rows - 1))
    inner = range(1, rows - 1)
    cuts = [slice(c * LANES, (c + 1) * LANES) for c in range(tiles)]

    has = (me > 0, me < last)
    few = count <= 4
    barrier = pltpu.get_barrier_semaphore()
    lates_ref[...] = jnp.zeros(lates_ref.shape, F32)

    def greet(sem):
        for side in range(2):
            @pl.when(has[side])
            def _():
                pl.semaphore_signal(
                    sem, inc=1, device_id={"space": me - 1 if side == 0 else me + 1},
                    device_id_type=pl.DeviceIdType.MESH,
                )

    def greeted(sem):
        pl.semaphore_wait(sem, jnp.minimum(me, 1) + jnp.minimum(last - me, 1))

    if few:
        greet(barrier)
    else:
        for off in range(1, count):
            pl.semaphore_signal(
                barrier, inc=1, device_id={"space": lax.rem(me + off, count)},
                device_id_type=pl.DeviceIdType.MESH,
            )

    def whole(ref, i):
        return pltpu.make_async_copy(ref, ref, sem_in.at[i])

    ids_load = pltpu.make_async_copy(focal_hbm, ids_ref, sem_in.at[0])
    focal_load = pltpu.make_async_copy(focal_hbm, focal_ref, sem_in.at[1])
    inner_load = pltpu.make_async_copy(t_hbm.at[pl.ds(1, rows - 2)], ti_ref, sem_in.at[5])
    ids_load.start()
    focal_load.start()
    for side, r in ends:
        for cut in cuts:
            pltpu.make_async_copy(
                t_hbm.at[r, pl.ds(cut.start, LANES)], te_ref.at[side, pl.ds(cut.start, LANES)], sem_in.at[2]).start()
    for i, group in ((3, (cond_hbm, gval_hbm, scur_hbm)), (4, (nodata_hbm, gmask_hbm, smask_hbm))):
        for k, src in enumerate(group):
            pltpu.make_async_copy(src, (reals_ref, flags_ref)[i - 3].at[k], sem_in.at[i]).start()
    inner_load.start()
    ids_load.wait()
    focal_load.wait()
    whole(te_ref, 2).wait()

    def gather(src, at):
        for p in range(pairs):
            for i in range(2):
                r, k = at(ids_ref[i, p])
                spot_ref[i, p:p + 1, :] = src[r, pl.ds(k, 1), :]
        return FOCAL_CURRENT * spot_ref[0], -FOCAL_CURRENT * spot_ref[1]

    half, high = (rows * cols // 2).bit_length() - 1, cols.bit_length() - 1
    near_a, near_b = gather(
        te_ref, lambda i: (lax.shift_right_logical(i, half) & 1, i & (cols - 1)))

    diagonal = lax.broadcasted_iota(jnp.int32, (pairs, pairs), 0) == lax.broadcasted_iota(
        jnp.int32, (pairs, pairs), 1)
    lane = lax.broadcasted_iota(jnp.int32, (pairs, LANES), 1)

    def column(i):
        line = jnp.broadcast_to(focal_ref[i:i + 1, :].astype(F32), (pairs, pairs))
        return jnp.broadcast_to(
            jnp.sum(jnp.where(diagonal, line, 0.0), 1, keepdims=True).astype(jnp.int32), (pairs, LANES))

    at_a, at_b = (column(i) - me * (rows * cols) for i in range(2))
    spot_a, spot_b = (lax.shift_right_arithmetic(x, 7) for x in (at_a, at_b))
    tile_a, tile_b = spot_a & (tiles - 1), spot_b & (tiles - 1)

    def within(spot, low, high):
        return jnp.logical_and(spot >= low * tiles, spot < high * tiles)

    piece = pairs // 2
    halves = tuple(enumerate((slice(0, piece), slice(piece, pairs))))
    for side, r in ends:
        here_a = jnp.where(within(spot_a, r, r + 1), near_a, 0.0)
        here_b = jnp.where(within(spot_b, r, r + 1), near_b, 0.0)
        for h, s in halves:
            msg_ref[h, side, 0:piece, :] = here_a[s]
            msg_ref[h, side, piece:pairs, :] = here_b[s]

    def side_copy(src, dst, ssem, rsem, side, number):
        return pltpu.make_async_remote_copy(
            src_ref=src.at[side, pl.ds(0, number)], dst_ref=dst.at[1 - side, pl.ds(0, number)],
            send_sem=ssem.at[side], recv_sem=rsem.at[1 - side],
            device_id={"space": me - 1 if side == 0 else me + 1},
            device_id_type=pl.DeviceIdType.MESH,
        )

    def send(src, dst, ssem, rsem, number=None):
        number = number or src.shape[1]
        for side in range(2):
            @pl.when(has[side])
            def _():
                side_copy(src, dst, ssem, rsem, side, number).start()

            @pl.when(jnp.logical_not(has[side]))
            def _():
                dst[side] = jnp.zeros(dst.shape[1:], F32)

    def done(src, dst, ssem, rsem, number=None):
        number = number or src.shape[1]
        for side in range(2):
            @pl.when(has[side])
            def _():
                side_copy(src, dst, ssem, rsem, side, number).wait_send()
                pltpu.make_async_remote_copy(
                    src_ref=src.at[1 - side, pl.ds(0, number)], dst_ref=dst.at[side, pl.ds(0, number)],
                    send_sem=ssem.at[1 - side], recv_sem=rsem.at[side],
                    device_id={"space": me - 1 if side == 0 else me + 1},
                    device_id_type=pl.DeviceIdType.MESH,
                ).wait_recv()

    def ring(h):
        return msg_ref.at[h], got_ref.at[h], send1.at[h], recv1.at[h]

    def zring(h):
        return zmsg_ref.at[h], zgot_ref.at[h], send2.at[h], recv2.at[h], pairs + (0 if h else tiles)

    if few:
        greeted(barrier)
    else:
        pl.semaphore_wait(barrier, last)
    send(*ring(0))

    whole(reals_ref, 3).wait()
    whole(flags_ref, 4).wait()
    valid = (1 - flags_ref[0]).astype(F32)
    active = reals_ref[0] * valid
    background = flags_ref[2].astype(F32) * reals_ref[2]

    def tile_of(r, c):
        if r == 0 or r == rows - 1:
            return te_ref[min(r, 1), cuts[c], :]
        return ti_ref[r - 1, cuts[c], :]

    def product(x, r, c):
        number = x.shape[0]
        hi = x.astype(BF16).astype(F32)
        lhs = jnp.concatenate([hi, x - hi], 0).astype(BF16)
        o = jnp.dot(lhs, thl_ref[r, c], preferred_element_type=F32)
        return o[:number, :LANES] + (o[:number, LANES:] + (o[number:, :LANES] + o[number:, LANES:]))

    def shared_row(r):
        dot = jnp.zeros((EXTRA, LANES), F32)
        for c, cut in enumerate(cuts):
            t = tile_of(r, c)
            thi = t.astype(BF16)
            thl_ref[r, c, :, :LANES] = thi
            thl_ref[r, c, :, LANES:] = (t - thi.astype(F32)).astype(BF16)
            x = jnp.broadcast_to(background[r:r + 1, cut], (EXTRA, LANES))
            q = product(x, r, c)
            q_ref[r, pairs:ext, cut] = q
            dot = dot + x * q
        return dot

    shared = shared_row(0) + shared_row(rows - 1)
    for side, r in ends:
        for c, cut in enumerate(cuts):
            bmsg_ref[side, c:c + 1, :] = q_ref[r, pairs:pairs + 1, cut]
            bmsg_ref[side, tiles + c:tiles + c + 1, :] = active[r:r + 1, cut]
            bmsg_ref[side, 2 * tiles + c:2 * tiles + c + 1, :] = valid[r:r + 1, cut]
            tmsg_ref[side, c:c + 1, :] = te_ref[side, cut.start:cut.start + 1, :]
            tmsg_ref[side, tiles + c:tiles + c + 1, :] = te_ref[side, cut.stop - 1:cut.stop, :]
    send(bmsg_ref, bgot_ref, sendb, recvb)
    send(*ring(1))
    send(tmsg_ref, tgot_ref, sendt, recvt)

    def edge(a, b, v, u):
        return 0.5 * (a + b) * v * u

    row_at = lax.broadcasted_iota(jnp.int32, (rows, cols), 0)
    col_at = lax.broadcasted_iota(jnp.int32, (rows, cols), 1)

    def shifted(x, by, axis):
        length = x.shape[axis]
        at = (row_at, col_at)[axis][:x.shape[0], :]
        return jnp.where(at == (0 if by == 1 else length - 1), 0.0, pltpu.roll(x, by % length, axis))

    nw, sw, ww, ew = (
        edge(active, shifted(active, *how), valid, shifted(valid, *how))
        for how in ((1, 0), (-1, 0), (1, 1), (-1, 1))
    )
    dg = valid * (LEAKAGE + flags_ref[1].astype(F32) * reals_ref[1]) + (1.0 - valid) + nw + sw + ww + ew
    for r in range(rows):
        for i, x in enumerate((dg, nw, sw, ww, ew, 0.5 * dg, background)):
            wts_ref[r, i:i + 1, :] = x[r:r + 1, :]

    inner_load.wait()
    far_a, far_b = gather(
        ti_ref, lambda i: (
            jnp.clip((lax.shift_right_logical(i, high) & (rows - 1)) - 1, 0, rows - 3), i & (cols - 1)))
    for r in inner:
        shared = shared + shared_row(r)

    def dense_row(r, a, b, dot):
        for c, cut in enumerate(cuts):
            k = r * tiles + c
            x = jnp.where(spot_a == k, a, 0.0) + jnp.where(spot_b == k, b, 0.0)
            q_ref[r, 0:pairs, cut] = q_ref[r, pairs:pairs + 1, cut] + x
            dot = dot + background[r:r + 1, cut] * x
        return dot

    dot = jnp.zeros((pairs, LANES), F32)
    for r in range(rows):
        a, b = (far_a, far_b) if r in inner else (near_a, near_b)
        dot = dense_row(r, a, b, dot)
    in_a, in_b = (
        jnp.where(within(spot, 1, rows - 1), far, jnp.where(within(spot, 0, rows), near, 0.0))
        for spot, far, near in ((spot_a, far_a, near_a), (spot_b, far_b, near_b))
    )
    same = spot_a == spot_b
    own = jnp.where(lane == (at_a & (LANES - 1)), in_a + jnp.where(same, in_b, 0.0), 0.0) - jnp.where(
        lane == (at_b & (LANES - 1)), in_b + jnp.where(same, in_a, 0.0), 0.0)
    acc_ref[0] = 2.0 * dot + FOCAL_CURRENT * own + jnp.broadcast_to(shared[0:1, :], dot.shape)
    for i in range(1, 4):
        acc_ref[i] = jnp.zeros(acc_ref.shape[1:], F32)

    parts = [slice(p, p + 16) for p in range(0, pairs, 16)]
    extra = slice(pairs, ext)

    def stream(src, r, s, east=True):
        at = lane[:s.stop - s.start]
        x = src[r, s, cuts[0]]
        gone, west, ahead = None, pltpu.roll(x, 1, 1), east and pltpu.roll(x, LANES - 1, 1)
        for c in range(tiles):
            more = c + 1 < tiles
            if more:
                y = src[r, s, cuts[c + 1]]
                after = east and pltpu.roll(y, LANES - 1, 1)
            yield (
                c, cuts[c], x, west if gone is None else jnp.where(at == 0, gone, west),
                jnp.where(at == LANES - 1, after, ahead) if east and more else ahead,
            )
            if more:
                x, gone, west, ahead = y, west, pltpu.roll(y, 1, 1), after

    def apply_part(src, dst, r, s, north, south, acc=None):
        dots = None
        for c, cut, x, west, east in stream(src, r, s):
            out = wts_ref[r, 0:1, cut] * x - wts_ref[r, 3:4, cut] * west - wts_ref[r, 4:5, cut] * east
            if north is not None:
                out = out - wts_ref[r, 1:2, cut] * north[0][north[1], s, cut]
            if south is not None:
                out = out - wts_ref[r, 2:3, cut] * south[0][south[1], s, cut]
            dst[r, s, cut] = out
            dots = x * out if dots is None else dots + x * out
        if acc is not None:
            acc_ref[acc, s, :] += dots

    def apply_inner(src, dst):
        def body(r, carry):
            for s in parts:
                apply_part(src, dst, r, s, (src, r - 1), (src, r + 1))
            return carry
        lax.fori_loop(1, rows - 1, body, 0)

    for s in (*parts, extra):
        apply_part(q_ref, w_ref, 0, s, None, (q_ref, 1))
        apply_part(q_ref, w_ref, rows - 1, s, (q_ref, rows - 2), None)

    def image_row(r):
        for s in parts:
            apply_part(q_ref, w_ref, r, s, (q_ref, r - 1), (q_ref, r + 1), 1)
        apply_part(q_ref, w_ref, r, extra, (q_ref, r - 1), (q_ref, r + 1))

    ready = rows - 2 - 3
    for r in range(ready + 1, rows - 1):
        image_row(r)

    done(*ring(0))
    if few:
        greet(hello)
    done(bmsg_ref, bgot_ref, sendb, recvb)

    def row_of(side, base):
        return jnp.concatenate([bgot_ref[side, base + c:base + c + 1, :] for c in range(tiles)], 1)

    halo_a = [row_of(side, tiles) for side in range(2)]
    halo_v = [row_of(side, 2 * tiles) for side in range(2)]
    over = []
    for side, r in ends:
        i = 1 + side
        x = edge(active[r:r + 1, :], halo_a[side], valid[r:r + 1, :], halo_v[side])
        over.append(x)
        wts_ref[r, i:i + 1, :] = x
        wts_ref[r, 0:1, :] += x
        wts_ref[r, 5:6, :] += 0.5 * x

    def precond_row(r):
        for c, cut in enumerate(cuts):
            z_ref[r, :, cut] = product(w_ref[r, :, cut], r, c)

    for h, s in halves:
        if h:
            done(*ring(h))
        for side, r in ends:
            va = got_ref[h, side, 0:piece, :]
            vb = got_ref[h, side, piece:pairs, :]
            last_a = last_b = None
            dots = jnp.zeros((piece, LANES), F32)
            for c, cut in enumerate(cuts):
                common = bgot_ref[side, c:c + 1, :]
                qh = jnp.where(tile_a[s] == c, va, 0.0) + jnp.where(tile_b[s] == c, vb, 0.0)
                qhalo_ref[side, s, cut] = qh
                q0 = q_ref[r, s, cut]
                w0 = w_ref[r, s, cut] + over[side][:, cut] * (q0 - (qh + common))
                w_ref[r, s, cut] = w0
                dots = dots + q0 * w0
                if h == 0:
                    we = w_ref[r, extra, cut] + over[side][:, cut] * (q_ref[r, extra, cut] - common)
                    w_ref[r, extra, cut] = we
                    z = product(jnp.concatenate([w0, we], 0), r, c)
                    z_ref[r, extra, cut] = z[piece:]
                    zmsg_ref[h, side, pairs + c:pairs + c + 1, :] = z[piece:piece + 1]
                    z = z[:piece]
                else:
                    z = product(w0, r, c)
                z_ref[r, s, cut] = z
                last_a = z if c == 0 else jnp.where(tile_a[s] == c, z, last_a)
                last_b = z if c == 0 else jnp.where(tile_b[s] == c, z, last_b)
            acc_ref[1, s, :] += dots
            zmsg_ref[h, side, 0:piece, :] = last_a
            zmsg_ref[h, side, piece:pairs, :] = last_b
        send(*zring(h))

    def moment_part(r, s, north):
        mu = nu = None
        for c, cut, z, west, _ in stream(z_ref, r, s, False):
            t = wts_ref[r, 5:6, cut] * z - wts_ref[r, 3:4, cut] * west
            if north:
                t = t - wts_ref[r, 1:2, cut] * z_ref[r - 1, s, cut]
            one, two = w_ref[r, s, cut] * z, t * z
            mu, nu = (one, two) if mu is None else (mu + one, nu + two)
        acc_ref[2, s, :] += mu
        acc_ref[3, s, :] += nu

    def moment_row(r):
        for s in parts:
            moment_part(r, s, r > 0)

    image_row(1)
    for r in inner:
        if r + 1 <= ready:
            image_row(r + 1)
        precond_row(r)
        moment_row(r - 1)
    moment_row(rows - 2)
    moment_row(rows - 1)

    pad = jnp.zeros((8, LANES - pairs), F32)

    def lines(sums):
        table = jnp.zeros((pairs, LANES), F32)
        for i, x in enumerate(sums):
            table = jnp.where(lane == i, jnp.sum(x, 1, keepdims=True), table)
        return jnp.concatenate([table.T[0:8, :], pad], 1)

    def exchange(src, dst, ssem, rsem):
        for k in range(1, count):
            pltpu.make_async_remote_copy(
                src_ref=src, dst_ref=dst.at[k - 1], send_sem=ssem, recv_sem=rsem,
                device_id={"space": lax.rem(me + k, count)}, device_id_type=pl.DeviceIdType.MESH,
            ).start()

    def arrived(dst, ssem, rsem):
        for sem in (ssem, rsem):
            pltpu.make_async_copy(dst, dst, sem).wait()

    early = lines([acc_ref[i] for i in range(4)])
    stat_ref[...] = early
    if few:
        greeted(hello)
    exchange(stat_ref, all_ref, send3, recv3)

    done(tmsg_ref, tgot_ref, sendt, recvt)
    for side in range(2):
        halo_w, halo_e = (
            edge(halo_a[side], shifted(halo_a[side], by, 1), halo_v[side], shifted(halo_v[side], by, 1))
            for by in (1, -1)
        )
        near = [jnp.zeros((pairs, LANES), F32)] * tiles
        for c, cut in enumerate(cuts):
            qh = qhalo_ref[side, :, cut]
            if c > 0:
                gone = (halo_w[:, cut] * qh)[:, 0:1]
                near[c - 1] = near[c - 1] - gone * tgot_ref[side, tiles + c - 1:tiles + c, :]
            if c < tiles - 1:
                gone = (halo_e[:, cut] * qh)[:, LANES - 1:LANES]
                near[c + 1] = near[c + 1] - gone * tgot_ref[side, c + 1:c + 2, :]
        for c, cut in enumerate(cuts):
            zhalo_ref[side, :, cut] = near[c]

    coupling = [[], []]
    for h, s in halves:
        done(*zring(h))
        for side, r in ends:
            va = zgot_ref[h, side, 0:piece, :]
            vb = zgot_ref[h, side, piece:pairs, :]
            joined = jnp.zeros((piece, LANES), F32)
            for c, cut in enumerate(cuts):
                other = zgot_ref[0, side, pairs + c:pairs + c + 1, :] + zhalo_ref[side, s, cut]
                zh = jnp.where(tile_a[s] == c, va, jnp.where(tile_b[s] == c, vb, other))
                zhalo_ref[side, s, cut] = zh
                joined = joined + over[side][:, cut] * z_ref[r, s, cut] * zh
            coupling[side].append(joined)
    late = lines([jnp.concatenate(x, 0) for x in coupling])
    for i in range(2):
        late_ref[i] = late[i:i + 1, :]
    def late_copy(k):
        row = jnp.where(me + k < count, 0, 1)
        return pltpu.make_async_remote_copy(
            src_ref=late_ref.at[row], dst_ref=lates_ref.at[k - 1], send_sem=send4.at[k - 1], recv_sem=recv4.at[k - 1],
            device_id={"space": lax.rem(me + k, count)}, device_id_type=pl.DeviceIdType.MESH,
        )

    def gives(who, k):
        up = who + k < count
        return jnp.logical_or(jnp.logical_and(up, who > 0), jnp.logical_and(jnp.logical_not(up), who < last))

    for k in range(1, count):
        @pl.when(gives(me, k))
        def _():
            late_copy(k).start()

    apply_inner(z_ref, y_ref)
    for s in parts:
        apply_part(z_ref, y_ref, 0, s, (zhalo_ref, 0), (z_ref, 1))
        apply_part(z_ref, y_ref, rows - 1, s, (z_ref, rows - 2), (zhalo_ref, 1))

    def right_side(r, carry):
        for c, cut in enumerate(cuts):
            local = r * cols + c * LANES + lane
            x = jnp.where(local == at_a, FOCAL_CURRENT, 0.0) - jnp.where(local == at_b, FOCAL_CURRENT, 0.0)
            r0_ref[r, 0:pairs, cut] = wts_ref[r, 6:7, cut] + x
        return carry

    lax.fori_loop(0, rows, right_side, 0)

    arrived(all_ref, send3, recv3)
    total = early
    for k in range(1, count):
        total = total + all_ref[k - 1]
    gamma0, kappa, mu, part = (total[i:i + 1, :] for i in range(4))
    a0 = gamma0 / kappa
    gamma1 = a0 * a0 * mu - gamma0
    beta = gamma1 / gamma0
    known = kappa - 2.0 * a0 * mu - beta * gamma1 / a0 + 2.0 * a0 * a0 * part
    scale = 2.0 * a0 * a0
    joint = late[0:1, :] + late[1:2, :]
    for k in range(1, count):
        @pl.when(gives(me, k))
        def _():
            late_copy(k).wait_send()

        @pl.when(gives(lax.rem(me - k + count, count), k))
        def _():
            late_copy(k).wait_recv()
    for k in range(1, count):
        joint = joint + lates_ref[k - 1]
    a1 = gamma1 / (known - scale * joint)
    first = a0 + a1 * (1.0 + beta)
    both = jnp.concatenate([first, a0 * a1, jnp.zeros((6, LANES), F32)], 0).T
    for i in range(2):
        coef_ref[i] = jnp.broadcast_to(both[:pairs, i:i + 1], (pairs, LANES))


def combine_kernel(coef_ref, r0_ref, q_ref, w_ref, z_ref, y_ref, sol_hbm, res_hbm, sol_ref, res_ref, sem):
    rows, pairs, cols = sol_ref.shape
    mine = pl.ds(0, pairs)

    def out(r, src, dst, k):
        return pltpu.make_async_copy(src.at[r], dst.at[mine, r], sem.at[k, r])

    def body(r, carry):
        one, two = coef_ref[0], coef_ref[1]
        for c in range(cols // LANES):
            cut = slice(c * LANES, (c + 1) * LANES)
            sol_ref[r, :, cut] = one * q_ref[r, mine, cut] - two * z_ref[r, mine, cut]
            res_ref[r, :, cut] = r0_ref[r, mine, cut] - one * w_ref[r, mine, cut] + two * y_ref[r, mine, cut]
        out(r, sol_ref, sol_hbm, 0).start()
        out(r, res_ref, res_hbm, 1).start()
        return carry

    lax.fori_loop(0, rows, body, 0)

    def finish(r, carry):
        out(r, sol_ref, sol_hbm, 0).wait()
        out(r, res_ref, res_hbm, 1).wait()
        return carry

    lax.fori_loop(0, rows, finish, 0)


def on_device(count, cond, nodata, gmask, gval, smask, scur, tinv, focal):
    rows, cols = cond.shape
    pairs = focal.shape[0]
    tiles = cols // LANES
    ext = pairs + EXTRA
    field = jax.ShapeDtypeStruct((rows, ext, cols), F32)
    vm = pl.BlockSpec(memory_space=pltpu.VMEM)
    hbm = pl.BlockSpec(memory_space=pltpu.HBM)
    msg = (2, 2, pairs, LANES)
    bmsg = (2, 3 * tiles, LANES)
    tmsg = (2, 2 * tiles, LANES)
    zmsg = (2, 2, pairs + tiles, LANES)
    others = count - 1
    r0, q, w, z, y, coef = pl.pallas_call(
        functools.partial(krylov_kernel, count),
        out_shape=[field] * 5 + [jax.ShapeDtypeStruct((2, pairs, LANES), F32)],
        in_specs=[hbm] * 8,
        out_specs=[vm] * 6,
        scratch_shapes=[
            pltpu.VMEM((3, rows, cols), F32),
            pltpu.VMEM((3, rows, cols), jnp.int32),
            pltpu.VMEM((2, pairs), jnp.int32),
            pltpu.SMEM((2, pairs), jnp.int32),
            pltpu.VMEM((2, cols, LANES), F32),
            pltpu.VMEM((rows - 2, cols, LANES), F32),
            pltpu.VMEM((rows, tiles, LANES, 2 * LANES), BF16),
            pltpu.VMEM((rows, 8, cols), F32),
            pltpu.VMEM((2, pairs, LANES), F32),
            pltpu.VMEM((2, pairs, cols), F32),
            pltpu.VMEM((2, pairs, cols), F32),
            *[pltpu.VMEM(shape, F32) for shape in (msg, bmsg, tmsg, zmsg) for _ in range(2)],
            pltpu.VMEM((4, pairs, LANES), F32),
            *[pltpu.VMEM(shape, F32) for shape in ((8, LANES), (others, 8, LANES), (2, 1, LANES), (others, 1, LANES))],
            *[pltpu.SemaphoreType.DMA((2, 2))] * 2,
            *[pltpu.SemaphoreType.DMA((2,))] * 4,
            *[pltpu.SemaphoreType.DMA((2, 2))] * 2,
            *[pltpu.SemaphoreType.DMA] * 2,
            *[pltpu.SemaphoreType.DMA((others,))] * 2,
            pltpu.SemaphoreType.DMA((6,)),
            pltpu.SemaphoreType.REGULAR,
        ],
        compiler_params=pltpu.CompilerParams(
            collective_id=0, has_side_effects=True, vmem_limit_bytes=36 * 1024 * 1024
        ),
        name="krylov",
    )(*(
        pltpu.with_memory_space_constraint(x, pltpu.HBM)
        for x in (cond, nodata, gmask, gval, smask, scur, tinv.reshape(rows, cols, LANES), focal.T)
    ))

    out = jax.ShapeDtypeStruct((pairs, rows, cols), F32)
    return tuple(pl.pallas_call(
        combine_kernel,
        out_shape=[out, out],
        in_specs=[vm] * 6,
        out_specs=[hbm, hbm],
        scratch_shapes=[
            pltpu.VMEM((rows, pairs, cols), F32),
            pltpu.VMEM((rows, pairs, cols), F32),
            pltpu.SemaphoreType.DMA((2, rows)),
        ],
        compiler_params=pltpu.CompilerParams(vmem_limit_bytes=20 * 1024 * 1024),
        name="combine",
    )(coef, r0, q, w, z, y))


def solution(mesh):
    return jax.shard_map(
        functools.partial(on_device, mesh.shape["space"]),
        mesh=mesh,
        in_specs=(
            P(("groups", "space"), None),
            P(("groups", "space"), None),
            P(("groups", "space"), None),
            P(("groups", "space"), None),
            P(("groups", "space"), None),
            P(("groups", "space"), None),
            P(("groups", "space"), None, None, None),
            P(("groups", "rhs"), None),
        ),
        out_specs=(P("rhs", ("groups", "space"), None), P("rhs", ("groups", "space"), None)),
        check_vma=False,
    )
```
